32 devices in a mesh: row: 4 (over z), col: 8 (over y, x, core).
Axes of the slice: x: 2, y: 2, z: 4, core: 2. Of those that a mesh axis runs over, the one named last changes fastest.
Arguments:
- tokens: bfloat16 [24576, 256], P(('row', 'col'))
- codebook: bfloat16 [16384, 256], P(('row', 'col')), may hold values from -6 to 6
- codes: int32 [24576], P(('row', 'col')), may hold values from 0 to 16383
Outputs:
- quantized: bfloat16 [24576, 256], P(('row', 'col'))
- token_loss: float32 [24576], P(('row', 'col'))
- code_counts: int32 [16384], P(('row', 'col'))
- code_loss: float32 [16384], P(('row', 'col'))
- commitment: float32 [], replicated
- perplexity: float32 [], replicated
The draws below stay inside these ranges and needn't reach their ends.
All inputs are finite; a program needn't handle non-finite values.
Results may differ from the reference program's by a relative error of at most 0.0004.
Values may be sent and summed in bfloat16 or wider, within the bound.
A program may use at most 64 MiB of HBM per device.

```python
import math
import jax
import jax.numpy as jnp
import numpy as np

DIM = 256
CODES = 16384
TOKENS = 24576


def draw_tokens(key, part):
    key_norm = jax.random.fold_in(key, 11)
    key_scale = jax.random.fold_in(key, 12)
    values = jax.random.normal(key_norm, (TOKENS, DIM), jnp.float32)
    spread = jnp.exp(jax.random.uniform(key_scale, (TOKENS, 1), jnp.float32, jnp.log(0.2), jnp.log(2.0)))
    rising = 1.0 + 2.0 * jnp.arange(TOKENS, dtype=jnp.float32)[:, None] / TOKENS
    return (values * spread * rising).astype(jnp.bfloat16)


def touch_ends(drawn, own_key, smallest, top_value):
    index_at = [jax.random.randint(jax.random.fold_in(own_key, axis), (), 0, length) for axis, length in enumerate(drawn.shape)]
    main_axis = drawn.shape.index(max(drawn.shape))
    next_to = index_at[:main_axis] + [(index_at[main_axis] + 1) % drawn.shape[main_axis]] + index_at[main_axis + 1:]
    return drawn.at[tuple(index_at)].set(smallest).at[tuple(next_to)].set(top_value)


def levels(rng, extent, cuts, low, top_value):
    def one(position, shards_of):
        draws = jax.random.uniform(jax.random.fold_in(jax.random.fold_in(rng, 6), position), (shards_of,), jnp.float32, low / len(cuts), top_value / len(cuts))
        return jnp.repeat(jnp.exp(draws), extent[position] // shards_of).reshape((-1,) + (1,) * (len(extent) - position - 1))

    level = one(*cuts[0])
    for cut in cuts[1:]:
        level = level * one(*cut)
    return level


def rank_bounds(amount, lean):
    portions = [(1 << 20) // math.isqrt(rank ** lean) + 1 for rank in range(1, amount + 1)]
    scale = 1 + sum(portions) // (1 << 30)
    return np.cumsum(np.array([max(1, weight // scale) for weight in portions]))


def ranked(own_key, extent, count, lean):
    listing = rank_bounds(count, lean)
    lot = jax.random.randint(jax.random.fold_in(own_key, 1), extent, 0, int(listing[count - 1]))
    rank = jnp.searchsorted(jnp.asarray(listing, jnp.int32), lot, side="right")
    return jax.random.permutation(jax.random.fold_in(own_key, 2), count)[rank].astype(jnp.int32)


def normal_values(stream_key, shape, scale, most, cuts=(), kind=jnp.bfloat16):
    loudness = levels(stream_key, shape, cuts, -0.22, 0.18) if cuts else 1.0
    entries = jax.random.normal(stream_key, shape, jnp.float32) * scale * loudness
    return jnp.minimum(jnp.maximum(entries, -most), most).astype(kind)


def setup_inputs(seed: int = 0) -> dict:
    seeds = jax.random.split(jax.random.key(seed), 4)
    tokens = draw_tokens(jax.random.fold_in(seeds[3], 71), 0)
    codebook = normal_values(seeds[1], (CODES, DIM), 1.0, 6.0, ((0, 32),))
    codes = touch_ends(ranked(seeds[2], (TOKENS,), CODES, 2), jax.random.fold_in(seeds[2], 3), 0, CODES - 1).astype(jnp.int32)
    return dict(tokens=tokens, codebook=codebook, codes=codes)


def reference(tokens, codebook, codes):
    quantized = jnp.take(codebook, codes, axis=0)
    diff = tokens.astype(jnp.float32) - quantized.astype(jnp.float32)
    token_loss = jnp.sum(diff * diff, axis=1) / DIM
    code_counts = jnp.zeros((CODES,), jnp.int32).at[codes].add(1)
    code_loss = jax.ops.segment_sum(token_loss, codes, num_segments=CODES)
    commitment = 0.25 * jnp.sum(token_loss) / TOKENS
    probs = code_counts.astype(jnp.float32) / TOKENS
    floor_prob = jnp.float32(1.0 / TOKENS)
    terms = jnp.where(code_counts > 0, probs * jnp.log(jnp.maximum(probs, floor_prob)), jnp.float32(0.0))
    perplexity = jnp.exp(-jnp.sum(terms))
    return quantized, token_loss, code_counts, code_loss, commitment, perplexity
```

```python
import functools

import jax
import jax.numpy as jnp
from jax import lax
from jax.experimental import pallas as pl
from jax.experimental.pallas import tpu as pltpu
from jax.sharding import PartitionSpec as P

AXES = ("row", "col")
EXTRA = 128
GROUP = 4
F32 = jnp.float32
BF16 = jnp.bfloat16


def dense_plan(tokens, codebook, codes):
    tok_rows = tokens.shape[0]
    width = tokens.shape[1]
    per_dev = codebook.shape[0]
    devices = lax.axis_size("row") * lax.axis_size("col")
    total_codes = per_dev * devices
    total_tokens = tok_rows * devices
    full_book = lax.all_gather(codebook, AXES, axis=0, tiled=True)
    quantized = jnp.take(full_book, codes, axis=0)
    diff = tokens.astype(F32) - quantized.astype(F32)
    token_loss = jnp.sum(diff * diff, axis=1) / width
    loss_part = jnp.sum(token_loss)
    local_counts = jax.ops.segment_sum(
        jnp.ones((tok_rows,), F32), codes, num_segments=total_codes
    )
    local_loss = jax.ops.segment_sum(token_loss, codes, num_segments=total_codes)
    floor_prob = jnp.float32(1.0 / total_tokens)
    totals, loss_totals = lax.psum((local_counts, local_loss), AXES)
    loss_sum = lax.psum(loss_part, AXES)
    probs = totals / total_tokens
    terms = jnp.where(
        totals > 0.5, probs * jnp.log(jnp.maximum(probs, floor_prob)), jnp.float32(0.0)
    )
    offset = lax.axis_index(AXES) * per_dev
    owned_counts = lax.dynamic_slice_in_dim(totals, offset, per_dev, 0)
    code_loss = lax.dynamic_slice_in_dim(loss_totals, offset, per_dev, 0)
    commitment = 0.25 * loss_sum / total_tokens
    return (
        quantized,
        token_loss,
        owned_counts.astype(jnp.int32),
        code_loss,
        commitment,
        jnp.exp(-jnp.sum(terms)),
    )


def ring_plan(n, tokens, codebook, codes):
    rows, width = tokens.shape
    per_dev = codebook.shape[0]
    me = lax.axis_index(AXES)
    ring = [(i, (i + 1) % n) for i in range(n)]
    codes = jnp.where(me < n, codes, 0)
    codebook = jnp.where(me < n, codebook, 0)
    hi = codes // per_dev
    lo = codes % per_dev

    def pick(step, carry):
        block, got = carry
        owner = lax.rem(me - step + n, n)
        got = jnp.where((hi == owner)[:, None], jnp.take(block, lo, axis=0), got)
        return lax.ppermute(block, AXES, ring), got

    _, quantized = lax.fori_loop(0, n, pick, (codebook, jnp.zeros_like(tokens)))
    diff = tokens.astype(F32) - quantized.astype(F32)
    token_loss = jnp.sum(diff * diff, axis=1) / width

    def add(step, carry):
        c, t, total, hits, parts = carry
        owner = lax.rem(me - step + n, n)
        mine = (c // per_dev) == me
        total = total + jax.ops.segment_sum(
            jnp.where(mine, t, 0.0), c % per_dev, num_segments=per_dev
        )
        hits = hits + jax.ops.segment_sum(
            mine.astype(jnp.int32), c % per_dev, num_segments=per_dev
        )
        parts = lax.dynamic_update_slice(parts, jnp.sum(t)[None], (owner,))
        return lax.ppermute(c, AXES, ring), lax.ppermute(t, AXES, ring), total, hits, parts

    start = (
        codes, token_loss, jnp.zeros((per_dev,), F32),
        jnp.zeros((per_dev,), jnp.int32), jnp.zeros((n,), F32),
    )
    _, _, code_loss, counts, parts = lax.fori_loop(0, n, add, start)
    probs = counts.astype(F32) / (rows * n)
    floor_prob = jnp.float32(1.0 / (rows * n))
    terms = jnp.where(counts > 0, probs * jnp.log(jnp.maximum(probs, floor_prob)), 0.0)

    def collect(step, carry):
        entropy, parts = carry
        owner = lax.rem(me - step + n, n)
        parts = lax.dynamic_update_slice(parts, entropy, (owner,))
        return lax.ppermute(entropy, AXES, ring), parts

    _, entropies = lax.fori_loop(0, n, collect, (jnp.sum(terms)[None], jnp.zeros((n,), F32)))
    commitment = 0.25 * jnp.sum(parts) / (rows * n)
    return quantized, token_loss, counts, code_loss, commitment, jnp.exp(-jnp.sum(entropies))


def kernel(
    n, cols, cap, order_of,
    codes_hbm, tokens_hbm, book_hbm,
    quant_ref, tloss_ref, counts_ref, closs_ref, commit_ref, perp_ref, flag_ref,
    codes_ref, tokens_ref, book_ref, in_sem,
    csend, crecv, psend, precv, lsend, lrecv, ranks, low1h, sel,
    csem_s, csem_r, psem_s, psem_r, lsem_s, lsem_r,
):
    rows, width = tokens_hbm.shape
    per = book_hbm.shape[0]
    fetch_codes = pltpu.make_async_copy(codes_hbm, codes_ref, in_sem.at[0])
    fetch_book = pltpu.make_async_copy(book_hbm, book_ref, in_sem.at[1])
    fetch_tokens = pltpu.make_async_copy(tokens_hbm, tokens_ref, in_sem.at[2])
    fetch_codes.start()
    bits = per.bit_length() - 1
    total_tokens = rows * n
    my_row, my_col = lax.axis_index("row"), lax.axis_index("col")
    me = my_row * cols + my_col
    rows_at = [lax.rem(my_row + d, n // cols) for d in range(n // cols)]
    cols_at = [lax.rem(my_col + d, cols) for d in range(cols)]
    at = [(rows_at[k // cols], cols_at[k % cols]) for k in range(n)]
    peer = [r * cols + c for r, c in at]

    def copy(send, recv, ssem, rsem, k):
        return pltpu.make_async_remote_copy(
            src_ref=send.at[peer[k]],
            dst_ref=recv.at[me],
            send_sem=ssem.at[k],
            recv_sem=rsem.at[k],
            device_id=at[k],
            device_id_type=pl.DeviceIdType.MESH,
        )

    def start_all(*refs):
        for k in order_of:
            if k:
                copy(*refs, k).start()

    def wait_all(*refs):
        for k in order_of:
            if k:
                copy(*refs, k).wait_recv()

    def sent_all(*refs):
        for k in order_of:
            if k:
                copy(*refs, k).wait_send()

    barrier = pltpu.get_barrier_semaphore()
    for k in order_of:
        if k:
            pl.semaphore_signal(
                barrier, inc=1, device_id=at[k], device_id_type=pl.DeviceIdType.MESH
            )
    fetch_book.start()
    fetch_tokens.start()

    fetch_codes.wait()
    code_row = codes_ref[...].reshape(1, rows)
    hi_row = lax.shift_right_logical(code_row, bits)
    code_col = jnp.broadcast_to(code_row.astype(F32), (128, rows)).T.astype(jnp.int32)
    hi_col = lax.shift_right_logical(code_col, bits)
    lo_col = code_col & (per - 1)
    lane = lax.broadcasted_iota(jnp.int32, (rows, 128), 1)
    own_row = hi_row == lax.broadcasted_iota(jnp.int32, (n, rows), 0)
    for k in range(per // 128):
        low1h[:, k * 128 : (k + 1) * 128] = jnp.where(lo_col == lane + k * 128, 1.0, 0.0).astype(BF16)
    low = low1h[...]
    hist = jnp.dot(jnp.where(own_row, 1.0, 0.0).astype(BF16), low, preferred_element_type=F32)
    wanted = jnp.where(hist > 0.5, 1.0, 0.0)
    most = jnp.max(jnp.sum(wanted, axis=1, keepdims=True), axis=0, keepdims=True)
    most_wide = jnp.broadcast_to(most, (1, EXTRA))
    for p in range(n):
        csend[p, :, :per] = hist[p : p + 1, :]
        csend[p, :, per:] = most_wide
    crecv[pl.ds(me, 1)] = csend[pl.ds(me, 1)]

    pl.semaphore_wait(barrier, n - 1)
    start_all(csend, crecv, csem_s, csem_r)

    before = lax.broadcasted_iota(jnp.int32, (per, per), 0) < lax.broadcasted_iota(jnp.int32, (per, per), 1)
    before = jnp.where(before, 1.0, 0.0).astype(BF16)
    rank = jnp.dot(wanted.astype(BF16), before, preferred_element_type=F32)
    rank = jnp.minimum(rank, 255.0).astype(BF16)
    hi1h = jnp.where(hi_col[:, :n] == lane[:, :n], 1.0, 0.0).astype(BF16)
    looked = jnp.dot(hi1h, rank, preferred_element_type=F32).astype(BF16) * low
    found = jnp.dot(looked, jnp.ones((per, 128), BF16), preferred_element_type=F32)
    slot = hi_col * cap + found.astype(jnp.int32)
    for k in range(n * cap // 128):
        sel[:, k * 128 : (k + 1) * 128] = jnp.where(slot == lane + k * 128, 1.0, 0.0).astype(BF16)

    wait_all(csend, crecv, csem_s, csem_r)
    asked = crecv[:, 0, :per]
    present = asked > 0.5
    order = jnp.dot(jnp.where(present, 1.0, 0.0).astype(BF16), before, preferred_element_type=F32)
    order = jnp.where(present, order, -1.0)
    for p in range(n):
        ranks[p] = order[p : p + 1, :]

    place = lax.broadcasted_iota(jnp.int32, (cap, per), 0).astype(F32)
    fetch_book.wait()
    book = book_ref[...]
    ready = []
    for g in range(0, n, GROUP):
        group = order_of[g : g + GROUP]
        picks = [
            jnp.where(jnp.broadcast_to(ranks[peer[k]], (cap, per)) == place, 1.0, 0.0).astype(BF16)
            for k in group
        ]
        packed = jnp.dot(jnp.concatenate(picks, axis=0), book, preferred_element_type=F32)
        packed = packed.astype(BF16)
        for i, k in enumerate(group):
            out = psend if k else precv
            out[peer[k]] = packed[i * cap : (i + 1) * cap]
        for k in ready:
            copy(psend, precv, psem_s, psem_r, k).start()
        ready = [k for k in group if k]
    for k in ready:
        copy(psend, precv, psem_s, psem_r, k).start()

    counts = jnp.sum(asked, axis=0, keepdims=True)
    counts_ref[...] = counts.astype(jnp.int32)
    probs = counts / total_tokens
    terms = jnp.where(
        counts > 0.5, probs * jnp.log(jnp.maximum(probs, 1.0 / total_tokens)), 0.0
    )
    entropy = jnp.sum(terms, axis=1, keepdims=True)
    flag_ref[0, 0] = jnp.max(crecv[:, 0, per:]).astype(jnp.int32)

    wait_all(psend, precv, psem_s, psem_r)
    fetch_tokens.wait()
    packs = precv[...].reshape(n * cap, width)
    quant = jnp.dot(sel[...], packs, preferred_element_type=F32).astype(BF16)
    quant_ref[...] = quant
    diff = tokens_ref[...].astype(F32) - quant.astype(F32)
    square = diff * diff
    folded = square[:, :128]
    for k in range(1, width // 128):
        folded = folded + square[:, k * 128 : (k + 1) * 128]
    tloss = jnp.sum(folded.T, axis=0, keepdims=True) / width
    tloss_ref[...] = tloss
    part = jnp.sum(tloss, axis=1, keepdims=True)

    first = tloss.astype(BF16).astype(F32)
    second = (tloss - first).astype(BF16).astype(F32)
    third = tloss - first - second
    spread = jnp.concatenate(
        [jnp.where(own_row, x, 0.0).astype(BF16) for x in (first, second, third)], axis=0
    )
    sums = jnp.dot(spread, low1h[...], preferred_element_type=F32)
    sums = sums[:n] + sums[n : 2 * n] + sums[2 * n :]
    lane1 = lax.broadcasted_iota(jnp.int32, (1, EXTRA), 1)
    tail = jnp.where(lane1 == 0, part, jnp.where(lane1 == 1, entropy, 0.0))
    for p in range(n):
        lsend[p, :, :per] = sums[p : p + 1, :]
        lsend[p, :, per:] = tail
    lrecv[pl.ds(me, 1)] = lsend[pl.ds(me, 1)]
    start_all(lsend, lrecv, lsem_s, lsem_r)

    sent_all(csend, crecv, csem_s, csem_r)
    sent_all(psend, precv, psem_s, psem_r)
    wait_all(lsend, lrecv, lsem_s, lsem_r)
    added = jnp.sum(lrecv[:, 0, :], axis=0, keepdims=True)
    closs_ref[...] = added[:, :per]
    ends = added[:, per:]
    commit_ref[0, 0] = jnp.sum(jnp.where(lane1 == 0, ends, 0.0)) * (0.25 / total_tokens)
    perp = jnp.exp(-jnp.sum(jnp.where(lane1 == 1, ends, 0.0), axis=1, keepdims=True))
    perp_ref[0, 0] = jnp.max(jnp.broadcast_to(perp, (1, EXTRA)))
    sent_all(lsend, lrecv, lsem_s, lsem_r)


def send_order(n, cols):
    turns = sorted(range(n // cols), key=lambda d: (abs(2 * d - n // cols), d))
    turns = [d for d in turns if d] + [0]
    blocks = [(d, h) for d in turns for h in (0, 1)]
    half = cols // 2
    spread = sorted(blocks[2:-2], key=lambda b: b[1])
    blocks = blocks[:2] + spread + [(0, 1), (0, 0)]
    return [d * cols + h * half + c for d, h in blocks for c in range(half)]


def exchange(n, cols, cap, number, tokens, codebook, codes):
    rows, width = tokens.shape
    per = codebook.shape[0]
    vmem = pl.BlockSpec(memory_space=pltpu.VMEM)
    smem = pl.BlockSpec(memory_space=pltpu.SMEM)
    dma = pltpu.SemaphoreType.DMA((n,))
    message = pltpu.VMEM((n, 1, per + EXTRA), F32)
    return pl.pallas_call(
        functools.partial(kernel, n, cols, cap, send_order(n, cols)),
        out_shape=(
            jax.ShapeDtypeStruct((rows, width), BF16),
            jax.ShapeDtypeStruct((1, rows), F32),
            jax.ShapeDtypeStruct((1, per), jnp.int32),
            jax.ShapeDtypeStruct((1, per), F32),
            jax.ShapeDtypeStruct((1, 1), F32),
            jax.ShapeDtypeStruct((1, 1), F32),
            jax.ShapeDtypeStruct((1, 1), jnp.int32),
        ),
        in_specs=[pl.BlockSpec(memory_space=pltpu.HBM)] * 3,
        out_specs=(vmem, vmem, vmem, vmem, smem, smem, smem),
        scratch_shapes=[
            pltpu.VMEM(codes.shape, jnp.int32),
            pltpu.VMEM((rows, width), BF16),
            pltpu.VMEM((per, width), BF16),
            pltpu.SemaphoreType.DMA((3,)),
            message, message,
            pltpu.VMEM((n, cap, width), BF16),
            pltpu.VMEM((n, cap, width), BF16),
            message, message,
            pltpu.VMEM((n, 1, per), F32),
            pltpu.VMEM((rows, per), BF16),
            pltpu.VMEM((rows, n * cap), BF16),
            dma, dma, dma, dma, dma, dma,
        ],
        compiler_params=pltpu.CompilerParams(collective_id=number, has_side_effects=True),
    )(*[pltpu.with_memory_space_constraint(x, pltpu.HBM) for x in (codes, tokens, codebook)])


def finish_kernel(
    quant_ref, tloss_ref, counts_ref, closs_ref, commit_ref, perp_ref,
    quant_out, tloss_out, counts_out, closs_out, commit_out, perp_out, sem,
):
    put = pltpu.make_async_copy(quant_ref, quant_out, sem)
    put.start()
    tloss_out[...] = tloss_ref[...].reshape(tloss_out.shape)
    counts_out[...] = counts_ref[...].reshape(counts_out.shape)
    closs_out[...] = closs_ref[...].reshape(closs_out.shape)
    commit_out[0, 0] = commit_ref[0, 0]
    perp_out[0, 0] = perp_ref[0, 0]
    put.wait()


def finish(quantized, token_loss, counts, code_loss, commitment, perplexity):
    rows, per = token_loss.shape[1], counts.shape[1]
    vmem = pl.BlockSpec(memory_space=pltpu.VMEM)
    smem = pl.BlockSpec(memory_space=pltpu.SMEM)
    q, t, k, c, m, p = pl.pallas_call(
        finish_kernel,
        out_shape=(
            jax.ShapeDtypeStruct(quantized.shape, BF16),
            jax.ShapeDtypeStruct((rows,), F32),
            jax.ShapeDtypeStruct((per,), jnp.int32),
            jax.ShapeDtypeStruct((per,), F32),
            jax.ShapeDtypeStruct((1, 1), F32),
            jax.ShapeDtypeStruct((1, 1), F32),
        ),
        in_specs=[vmem] * 4 + [smem] * 2,
        out_specs=(pl.BlockSpec(memory_space=pltpu.HBM), vmem, vmem, vmem, smem, smem),
        scratch_shapes=[pltpu.SemaphoreType.DMA],
    )(quantized, token_loss, counts, code_loss, commitment, perplexity)
    return q, t, k, c, m[0, 0], p[0, 0]


def asked_plan(n, cols, cap, tokens, codebook, codes):
    rows = tokens.shape[0]
    per = codebook.shape[0]
    code_row = codes
    quantized, token_loss, counts, code_loss, commitment, perplexity, flag = exchange(
        n, cols, cap, 0, tokens, codebook, code_row
    )

    def kept():
        return finish(quantized, token_loss, counts, code_loss, commitment, perplexity)

    def wider():
        out = exchange(n, cols, 2 * cap, 1, tokens, codebook, code_row)
        return finish(*out[:6])

    def ringed():
        return ring_plan(n, tokens, codebook, codes)

    def any_codes():
        return lax.cond(flag[0, 0] > 2 * cap, ringed, wider)

    return lax.cond(flag[0, 0] > cap, any_codes, kept)


def on_device(n, cols, tokens, codebook, codes):
    rows, width = tokens.shape
    per = codebook.shape[0]
    cap = -(-rows // (n * 16)) * 16
    fits = (
        per % 128 == 0
        and per & (per - 1) == 0
        and rows % 128 == 0
        and width % 128 == 0
        and n * cap % 128 == 0
        and cols % 8 == 0
        and n // cols > 1
        and n <= 128
        and 2 * cap < min(per, 256)
    )
    if fits:
        return asked_plan(n, cols, cap, tokens, codebook, codes)
    return dense_plan(tokens, codebook, codes)


def solution(mesh):
    n = mesh.shape["row"] * mesh.shape["col"]
    return jax.shard_map(
        functools.partial(on_device, n, mesh.shape["col"]),
        mesh=mesh,
        in_specs=(P(AXES, None), P(AXES, None), P(AXES)),
        out_specs=(P(AXES, None), P(AXES), P(AXES), P(AXES), P(), P()),
        check_vma=False,
    )
```

```python
import functools

import jax
import jax.numpy as jnp
from jax import lax
from jax.experimental import pallas as pl
from jax.experimental.pallas import tpu as pltpu
from jax.sharding import PartitionSpec as P

AXES = ("row", "col")
EXTRA = 128
GROUP = 4
F32 = jnp.float32
BF16 = jnp.bfloat16


def dense_plan(tokens, codebook, codes):
    tok_rows = tokens.shape[0]
    width = tokens.shape[1]
    per_dev = codebook.shape[0]
    devices = lax.axis_size("row") * lax.axis_size("col")
    total_codes = per_dev * devices
    total_tokens = tok_rows * devices
    full_book = lax.all_gather(codebook, AXES, axis=0, tiled=True)
    quantized = jnp.take(full_book, codes, axis=0)
    diff = tokens.astype(F32) - quantized.astype(F32)
    token_loss = jnp.sum(diff * diff, axis=1) / width
    loss_part = jnp.sum(token_loss)
    local_counts = jax.ops.segment_sum(
        jnp.ones((tok_rows,), F32), codes, num_segments=total_codes
    )
    local_loss = jax.ops.segment_sum(token_loss, codes, num_segments=total_codes)
    floor_prob = jnp.float32(1.0 / total_tokens)
    totals, loss_totals = lax.psum((local_counts, local_loss), AXES)
    loss_sum = lax.psum(loss_part, AXES)
    probs = totals / total_tokens
    terms = jnp.where(
        totals > 0.5, probs * jnp.log(jnp.maximum(probs, floor_prob)), jnp.float32(0.0)
    )
    offset = lax.axis_index(AXES) * per_dev
    owned_counts = lax.dynamic_slice_in_dim(totals, offset, per_dev, 0)
    code_loss = lax.dynamic_slice_in_dim(loss_totals, offset, per_dev, 0)
    commitment = 0.25 * loss_sum / total_tokens
    return (
        quantized,
        token_loss,
        owned_counts.astype(jnp.int32),
        code_loss,
        commitment,
        jnp.exp(-jnp.sum(terms)),
    )


def ring_plan(n, tokens, codebook, codes):
    rows, width = tokens.shape
    per_dev = codebook.shape[0]
    me = lax.axis_index(AXES)
    ring = [(i, (i + 1) % n) for i in range(n)]
    codes = jnp.where(me < n, codes, 0)
    codebook = jnp.where(me < n, codebook, 0)
    hi = codes // per_dev
    lo = codes % per_dev

    def pick(step, carry):
        block, got = carry
        owner = lax.rem(me - step + n, n)
        got = jnp.where((hi == owner)[:, None], jnp.take(block, lo, axis=0), got)
        return lax.ppermute(block, AXES, ring), got

    _, quantized = lax.fori_loop(0, n, pick, (codebook, jnp.zeros_like(tokens)))
    diff = tokens.astype(F32) - quantized.astype(F32)
    token_loss = jnp.sum(diff * diff, axis=1) / width

    def add(step, carry):
        c, t, total, hits, parts = carry
        owner = lax.rem(me - step + n, n)
        mine = (c // per_dev) == me
        total = total + jax.ops.segment_sum(
            jnp.where(mine, t, 0.0), c % per_dev, num_segments=per_dev
        )
        hits = hits + jax.ops.segment_sum(
            mine.astype(jnp.int32), c % per_dev, num_segments=per_dev
        )
        parts = lax.dynamic_update_slice(parts, jnp.sum(t)[None], (owner,))
        return lax.ppermute(c, AXES, ring), lax.ppermute(t, AXES, ring), total, hits, parts

    start = (
        codes, token_loss, jnp.zeros((per_dev,), F32),
        jnp.zeros((per_dev,), jnp.int32), jnp.zeros((n,), F32),
    )
    _, _, code_loss, counts, parts = lax.fori_loop(0, n, add, start)
    probs = counts.astype(F32) / (rows * n)
    floor_prob = jnp.float32(1.0 / (rows * n))
    terms = jnp.where(counts > 0, probs * jnp.log(jnp.maximum(probs, floor_prob)), 0.0)

    def collect(step, carry):
        entropy, parts = carry
        owner = lax.rem(me - step + n, n)
        parts = lax.dynamic_update_slice(parts, entropy, (owner,))
        return lax.ppermute(entropy, AXES, ring), parts

    _, entropies = lax.fori_loop(0, n, collect, (jnp.sum(terms)[None], jnp.zeros((n,), F32)))
    commitment = 0.25 * jnp.sum(parts) / (rows * n)
    return quantized, token_loss, counts, code_loss, commitment, jnp.exp(-jnp.sum(entropies))


def kernel(
    n, cols, cap, order_of,
    codes_hbm, tokens_hbm, book_hbm,
    quant_ref, tloss_ref, counts_ref, closs_ref, scal_ref, flag_ref,
    codes_ref, tokens_ref, book_ref, csend, crecv, psend, precv, dsend, drecv, lsend, lrecv,
    ranks, low1h, sel, rank1h,
    in_sem, csem_s, csem_r, psem_s, psem_r, lsem_s, lsem_r, bsem, dsem,
):
    rows, width = tokens_hbm.shape
    per = book_hbm.shape[0]
    bits = per.bit_length() - 1
    total_tokens = rows * n
    chips, half = n // 2, cols // 2
    my_row, my_col = lax.axis_index("row"), lax.axis_index("col")
    core = lax.rem(my_col, 2)
    my_chip = lax.div(my_col, 2)
    me = my_row * half + my_chip
    rows_at = [lax.rem(my_row + d, chips // half) for d in range(chips // half)]
    chips_at = [lax.rem(my_chip + d, half) for d in range(half)]
    spots = [(rows_at[k // half], chips_at[k % half]) for k in range(chips)]
    at = [(r, 2 * c + core) for r, c in spots]
    mirror = [(r, 2 * c + 1 - core) for r, c in spots]
    peer = [r * half + c for r, c in spots]
    fetch_codes = pltpu.make_async_copy(codes_hbm, codes_ref, in_sem.at[0])
    own_book = book_ref.at[pl.ds(pl.multiple_of(core * per, per), per)]
    fetch_book = pltpu.make_async_copy(book_hbm, own_book, in_sem.at[1])
    fetch_tokens = pltpu.make_async_copy(tokens_hbm, tokens_ref, in_sem.at[2])
    fetch_codes.start()

    def remote(src, dst, ssem, rsem, to):
        return pltpu.make_async_remote_copy(
            src_ref=src,
            dst_ref=dst,
            send_sem=ssem,
            recv_sem=rsem,
            device_id=to,
            device_id_type=pl.DeviceIdType.MESH,
        )

    def copy(send, recv, ssem, rsem, k):
        return remote(send.at[peer[k]], recv.at[me], ssem.at[k], rsem.at[k], at[k])

    def loss_copy(k, other):
        s = other * chips + k
        to = mirror[k] if other else at[k]
        return remote(lsend.at[peer[k]], lrecv.at[other, me], lsem_s.at[s], lsem_r.at[s], to)

    asks = [copy(csend, crecv, csem_s, csem_r, k) for k in order_of if k]
    replies = {k: copy(psend, precv, psem_s, psem_r, k) for k in order_of if k}
    losses = [loss_copy(k, other) for k in order_of for other in (0, 1) if k or other]
    share_book = remote(own_book, own_book, bsem.at[0], bsem.at[1], mirror[0])
    share_asks = remote(dsend, drecv, dsem.at[0], dsem.at[1], mirror[0])

    barrier = pltpu.get_barrier_semaphore()
    for k in order_of:
        for to in (at[k], mirror[k]) if k else (mirror[k],):
            pl.semaphore_signal(
                barrier, inc=1, device_id=to, device_id_type=pl.DeviceIdType.MESH
            )
    fetch_book.start()
    fetch_tokens.start()

    fetch_codes.wait()
    code_row = codes_ref[...].reshape(1, rows)
    hi_row = lax.shift_right_logical(code_row, bits)
    code_col = jnp.broadcast_to(code_row.astype(F32), (128, rows)).T.astype(jnp.int32)
    hi_col = lax.shift_right_logical(code_col, bits)
    lo_col = code_col & (per - 1)
    lane = lax.broadcasted_iota(jnp.int32, (rows, 128), 1)
    own_row = hi_row == lax.broadcasted_iota(jnp.int32, (n, rows), 0)
    for k in range(per // 128):
        low1h[:, k * 128 : (k + 1) * 128] = jnp.where(lo_col == lane + k * 128, 1.0, 0.0).astype(BF16)
    low = low1h[...]
    hist = jnp.dot(jnp.where(own_row, 1.0, 0.0).astype(BF16), low, preferred_element_type=F32)
    odd = (lax.broadcasted_iota(jnp.int32, (n, 128), 0) & 1) == 1

    def first_half(found):
        total = jnp.broadcast_to(jnp.sum(found, axis=1, keepdims=True), (n, 128))
        return total, jnp.where(odd, pltpu.roll(total, 1, 0), 0.0)

    wanted = jnp.where(hist > 0.5, 1.0, 0.0)
    total, ahead = first_half(wanted)
    most = jnp.max(total + ahead, axis=0, keepdims=True)
    heavy = jnp.max(jnp.max(hist, axis=0, keepdims=True), axis=1, keepdims=True) > 256.0
    most = jnp.where(heavy, 256.0, jnp.minimum(most, 256.0))
    most_pair = jnp.broadcast_to(most, (2, EXTRA)).astype(BF16)
    hist16 = hist.astype(BF16)
    for q in range(chips):
        csend[q, :, :per] = hist16[2 * q : 2 * q + 2, :]
        csend[q, :, per:] = most_pair
    crecv[pl.ds(me, 1)] = csend[pl.ds(me, 1)]

    pl.semaphore_wait(barrier, n - 1)
    for ask in asks:
        ask.start()
    fetch_book.wait()
    share_book.start()

    before = lax.broadcasted_iota(jnp.int32, (per, per), 0) < lax.broadcasted_iota(jnp.int32, (per, per), 1)
    before = jnp.where(before, 1.0, 0.0).astype(BF16)
    rank = jnp.dot(wanted.astype(BF16), before, preferred_element_type=F32) + ahead[:, :1]
    rank = jnp.minimum(rank, 255.0).astype(BF16)
    hi1h = jnp.where(hi_col[:, :n] == lane[:, :n], 1.0, 0.0).astype(BF16)
    looked = jnp.dot(hi1h, rank, preferred_element_type=F32).astype(BF16) * low
    found = jnp.dot(looked, jnp.ones((per, 128), BF16), preferred_element_type=F32)
    found = found.astype(jnp.int32)
    rank1h[...] = jnp.where(found == lane, 1.0, 0.0).astype(BF16)
    slot = lax.shift_right_logical(hi_col, 1) * cap + found
    for k in range(chips * cap // 128):
        sel[:, k * 128 : (k + 1) * 128] = jnp.where(slot == lane + k * 128, 1.0, 0.0).astype(BF16)

    for ask in asks:
        ask.wait_recv()
    got = jnp.concatenate([crecv[q].astype(F32) for q in range(chips)], axis=0)
    asked = got[:, :per]
    present = asked > 0.5
    present_one = jnp.where(present, 1.0, 0.0)
    order = jnp.dot(present_one.astype(BF16), before, preferred_element_type=F32)
    order = jnp.where(present, order + first_half(present_one)[1][:, :1], -1.0)
    for q in range(chips):
        ranks[q] = order[2 * q : 2 * q + 2, :]

    share_book.wait_recv()
    place = lax.broadcasted_iota(jnp.int32, (cap, per), 0).astype(F32)
    book = book_ref[...]
    ready = []
    for g in range(0, chips, GROUP):
        group = order_of[g : g + GROUP]
        picks = []
        for k in group:
            pair = ranks[peer[k]]
            picks.append(jnp.concatenate(
                [
                    jnp.where(jnp.broadcast_to(pair[h : h + 1], (cap, per)) == place, 1.0, 0.0).astype(BF16)
                    for h in (0, 1)
                ],
                axis=1,
            ))
        packed = jnp.dot(jnp.concatenate(picks, axis=0), book, preferred_element_type=F32)
        packed = packed.astype(BF16)
        for i, k in enumerate(group):
            out = psend if k else precv
            out[peer[k]] = packed[i * cap : (i + 1) * cap]
        for k in ready:
            replies[k].start()
        ready = [k for k in group if k]
    for k in ready:
        replies[k].start()

    turn = lax.broadcasted_iota(jnp.int32, (n, n), 0)
    side = jnp.where(turn < chips, core, 1 - core)
    which = 2 * lax.rem(turn, chips) + side
    split = jnp.where(lax.broadcasted_iota(jnp.int32, (n, n), 1) == which, 1.0, 0.0).astype(BF16)
    both = jnp.concatenate([order.astype(BF16), jnp.minimum(asked, 256.0).astype(BF16)], axis=1)
    both = jnp.dot(split, both, preferred_element_type=F32)
    most_asked = jnp.max(got[:, per:], axis=0, keepdims=True)
    dsend[:, : 2 * per] = both[chips:]
    dsend[:, 2 * per :] = jnp.broadcast_to(most_asked, (chips, EXTRA))
    share_asks.start()
    share_asks.wait_recv()
    counts = jnp.sum(both[:chips, per:] + drecv[:, per : 2 * per], axis=0, keepdims=True)
    counts_ref[...] = counts.astype(jnp.int32)
    probs = counts / total_tokens
    terms = jnp.where(
        counts > 0.5, probs * jnp.log(jnp.maximum(probs, 1.0 / total_tokens)), 0.0
    )
    entropy = jnp.sum(terms, axis=1, keepdims=True)
    flag_ref[0, 0] = jnp.max(jnp.maximum(most_asked, drecv[:1, 2 * per :])).astype(jnp.int32)
    spots_of = [both[:chips, :per].astype(jnp.int32), drecv[:, :per].astype(jnp.int32)]

    for k in replies:
        replies[k].wait_recv()
    fetch_tokens.wait()
    packs = precv[...].reshape(chips * cap, width)
    quant = jnp.dot(sel[...], packs, preferred_element_type=F32).astype(BF16)
    quant_ref[...] = quant
    diff = tokens_ref[...].astype(F32) - quant.astype(F32)
    square = diff * diff
    folded = square[:, :128]
    for k in range(1, width // 128):
        folded = folded + square[:, k * 128 : (k + 1) * 128]
    tloss = jnp.sum(folded.T, axis=0, keepdims=True) / width
    tloss_ref[...] = tloss
    part = jnp.sum(tloss, axis=1, keepdims=True)

    first = tloss.astype(BF16).astype(F32)
    second = (tloss - first).astype(BF16).astype(F32)
    third = tloss - first - second
    own_chip = lax.shift_right_logical(hi_row, 1) == lax.broadcasted_iota(jnp.int32, (chips, rows), 0)
    spread = jnp.concatenate(
        [jnp.where(own_chip, x, 0.0).astype(BF16) for x in (first, second, third)], axis=0
    )
    sums = jnp.dot(spread, rank1h[...], preferred_element_type=F32)
    sums = sums[:chips] + sums[chips : 2 * chips] + sums[2 * chips :]
    lane1 = lax.broadcasted_iota(jnp.int32, (chips, EXTRA), 1)
    sums = jnp.where(lane1 == EXTRA - 2, part, jnp.where(lane1 == EXTRA - 1, entropy, sums))
    for q in range(chips):
        lsend[q] = sums[q : q + 1, :]
    lrecv[0, pl.ds(me, 1)] = lsend[pl.ds(me, 1)]
    for loss in losses:
        loss.start()

    for ask in asks:
        ask.wait_send()
    for k in replies:
        replies[k].wait_send()
    share_book.wait_send()
    share_asks.wait_send()
    for loss in losses:
        loss.wait_recv()
    added = jnp.zeros((chips, per), F32)
    ends = jnp.zeros((1, EXTRA), F32)
    for other in (0, 1):
        back = lrecv[other, :, 0, :]
        spot = spots_of[other]
        parts = [
            jnp.take_along_axis(back, jnp.maximum(spot[:, j : j + 128], 0), axis=1)
            for j in range(0, per, 128)
        ]
        added = added + jnp.where(spot >= 0, jnp.concatenate(parts, axis=1), 0.0)
        ends = ends + jnp.sum(back, axis=0, keepdims=True)
    closs_ref[...] = jnp.sum(added, axis=0, keepdims=True)
    lane1 = lane1[:1]
    perp = jnp.exp(-ends[:, EXTRA - 1 :])
    scal_ref[...] = jnp.where(lane1 == 0, ends[:, EXTRA - 2 : EXTRA - 1] * (0.25 / total_tokens), perp)
    for loss in losses:
        loss.wait_send()


def send_order(n, cols):
    turns = sorted(range(n // cols), key=lambda d: (abs(2 * d - n // cols), d))
    turns = [d for d in turns if d] + [0]
    blocks = [(d, h) for d in turns for h in (0, 1)]
    half = cols // 2
    spread = sorted(blocks[2:-2], key=lambda b: b[1])
    blocks = blocks[:2] + spread + [(0, 1), (0, 0)]
    return [d * cols + h * half + c for d, h in blocks for c in range(half)]


def exchange(n, cols, cap, number, tokens, codebook, codes):
    rows, width = tokens.shape
    per = codebook.shape[0]
    chips = n // 2
    vmem = pl.BlockSpec(memory_space=pltpu.VMEM)
    smem = pl.BlockSpec(memory_space=pltpu.SMEM)
    dma = pltpu.SemaphoreType.DMA
    return pl.pallas_call(
        functools.partial(kernel, n, cols, cap, send_order(chips, cols // 2)),
        out_shape=(
            jax.ShapeDtypeStruct((rows, width), BF16),
            jax.ShapeDtypeStruct((1, rows), F32),
            jax.ShapeDtypeStruct((1, per), jnp.int32),
            jax.ShapeDtypeStruct((1, per), F32),
            jax.ShapeDtypeStruct((1, EXTRA), F32),
            jax.ShapeDtypeStruct((1, 1), jnp.int32),
        ),
        in_specs=[pl.BlockSpec(memory_space=pltpu.HBM)] * 3,
        out_specs=(vmem, vmem, vmem, vmem, vmem, smem),
        scratch_shapes=[
            pltpu.VMEM(codes.shape, jnp.int32),
            pltpu.VMEM((rows, width), BF16),
            pltpu.VMEM((2 * per, width), BF16),
            pltpu.VMEM((chips, 2, per + EXTRA), BF16),
            pltpu.VMEM((chips, 2, per + EXTRA), BF16),
            pltpu.VMEM((chips, cap, width), BF16),
            pltpu.VMEM((chips, cap, width), BF16),
            pltpu.VMEM((chips, 2 * per + EXTRA), F32),
            pltpu.VMEM((chips, 2 * per + EXTRA), F32),
            pltpu.VMEM((chips, 1, EXTRA), F32),
            pltpu.VMEM((2, chips, 1, EXTRA), F32),
            pltpu.VMEM((chips, 2, per), F32),
            pltpu.VMEM((rows, per), BF16),
            pltpu.VMEM((rows, chips * cap), BF16),
            pltpu.VMEM((rows, 128), BF16),
            dma((3,)),
            dma((chips,)), dma((chips,)), dma((chips,)), dma((chips,)),
            dma((n,)), dma((n,)), dma((2,)), dma((2,)),
        ],
        compiler_params=pltpu.CompilerParams(collective_id=number, has_side_effects=True),
    )(*[pltpu.with_memory_space_constraint(x, pltpu.HBM) for x in (codes, tokens, codebook)])


def finish_kernel(
    quant_ref, tloss_ref, counts_ref, closs_ref, scal_ref,
    quant_out, tloss_out, counts_out, closs_out, commit_out, perp_out, sem,
):
    put = pltpu.make_async_copy(quant_ref, quant_out, sem)
    put.start()
    tloss_out[...] = tloss_ref[...].reshape(tloss_out.shape)
    counts_out[...] = counts_ref[...].reshape(counts_out.shape)
    closs_out[...] = closs_ref[...].reshape(closs_out.shape)
    commit_out[...] = scal_ref[:, :1]
    perp_out[...] = scal_ref[:, 1:2]
    put.wait()


def finish(quantized, token_loss, counts, code_loss, scalars):
    rows, per = token_loss.shape[1], counts.shape[1]
    vmem = pl.BlockSpec(memory_space=pltpu.VMEM)
    q, t, k, c, m, p = pl.pallas_call(
        finish_kernel,
        out_shape=(
            jax.ShapeDtypeStruct(quantized.shape, BF16),
            jax.ShapeDtypeStruct((rows,), F32),
            jax.ShapeDtypeStruct((per,), jnp.int32),
            jax.ShapeDtypeStruct((per,), F32),
            jax.ShapeDtypeStruct((1, 1), F32),
            jax.ShapeDtypeStruct((1, 1), F32),
        ),
        in_specs=[vmem] * 5,
        out_specs=(pl.BlockSpec(memory_space=pltpu.HBM), vmem, vmem, vmem, vmem, vmem),
        scratch_shapes=[pltpu.SemaphoreType.DMA],
    )(quantized, token_loss, counts, code_loss, scalars)
    return q, t, k, c, m[0, 0], p[0, 0]


def asked_plan(n, cols, cap, tokens, codebook, codes):
    *outs, flag = exchange(n, cols, cap, 0, tokens, codebook, codes)

    def kept():
        return finish(*outs)

    def wider():
        return finish(*exchange(n, cols, 2 * cap, 1, tokens, codebook, codes)[:-1])

    def ringed():
        return ring_plan(n, tokens, codebook, codes)

    def any_codes():
        return lax.cond(flag[0, 0] > 2 * cap, ringed, wider)

    return lax.cond(flag[0, 0] > cap, any_codes, kept)


def on_device(n, cols, tokens, codebook, codes):
    rows, width = tokens.shape
    per = codebook.shape[0]
    cap = -(-2 * rows // (n * 16)) * 16
    fits = (
        per % 128 == 0
        and per & (per - 1) == 0
        and rows % 128 == 0
        and width % 128 == 0
        and n // 2 * cap % 128 == 0
        and cols % 8 == 0
        and n // cols > 1
        and n <= 128
        and 2 * cap < EXTRA - 1
    )
    if fits:
        return asked_plan(n, cols, cap, tokens, codebook, codes)
    return dense_plan(tokens, codebook, codes)


def solution(mesh):
    n = mesh.shape["row"] * mesh.shape["col"]
    return jax.shard_map(
        functools.partial(on_device, n, mesh.shape["col"]),
        mesh=mesh,
        in_specs=(P(AXES, None), P(AXES, None), P(AXES)),
        out_specs=(P(AXES, None), P(AXES), P(AXES), P(AXES), P(), P()),
        check_vma=False,
    )
```

```python
import functools

import jax
import jax.numpy as jnp
from jax import lax
from jax.experimental import pallas as pl
from jax.experimental.pallas import tpu as pltpu
from jax.sharding import PartitionSpec as P

AXES = ("row", "col")
EXTRA = 128
ASK_ORDER = (3, 2, 1, 0)
REPLY_ORDER = (2, 3, 1, 0)
F32 = jnp.float32
BF16 = jnp.bfloat16


def dense_plan(tokens, codebook, codes):
    tok_rows = tokens.shape[0]
    width = tokens.shape[1]
    per_dev = codebook.shape[0]
    devices = lax.axis_size("row") * lax.axis_size("col")
    total_codes = per_dev * devices
    total_tokens = tok_rows * devices
    full_book = lax.all_gather(codebook, AXES, axis=0, tiled=True)
    quantized = jnp.take(full_book, codes, axis=0)
    diff = tokens.astype(F32) - quantized.astype(F32)
    token_loss = jnp.sum(diff * diff, axis=1) / width
    loss_part = jnp.sum(token_loss)
    local_counts = jax.ops.segment_sum(
        jnp.ones((tok_rows,), F32), codes, num_segments=total_codes
    )
    local_loss = jax.ops.segment_sum(token_loss, codes, num_segments=total_codes)
    floor_prob = jnp.float32(1.0 / total_tokens)
    totals, loss_totals = lax.psum((local_counts, local_loss), AXES)
    loss_sum = lax.psum(loss_part, AXES)
    probs = totals / total_tokens
    terms = jnp.where(
        totals > 0.5, probs * jnp.log(jnp.maximum(probs, floor_prob)), jnp.float32(0.0)
    )
    offset = lax.axis_index(AXES) * per_dev
    owned_counts = lax.dynamic_slice_in_dim(totals, offset, per_dev, 0)
    code_loss = lax.dynamic_slice_in_dim(loss_totals, offset, per_dev, 0)
    commitment = 0.25 * loss_sum / total_tokens
    return (
        quantized,
        token_loss,
        owned_counts.astype(jnp.int32),
        code_loss,
        commitment,
        jnp.exp(-jnp.sum(terms)),
    )


def ring_plan(n, tokens, codebook, codes):
    rows, width = tokens.shape
    per_dev = codebook.shape[0]
    me = lax.axis_index(AXES)
    ring = [(i, (i + 1) % n) for i in range(n)]
    codes = jnp.where(me < n, codes, 0)
    codebook = jnp.where(me < n, codebook, 0)
    hi = codes // per_dev
    lo = codes % per_dev

    def pick(step, carry):
        block, got = carry
        owner = lax.rem(me - step + n, n)
        got = jnp.where((hi == owner)[:, None], jnp.take(block, lo, axis=0), got)
        return lax.ppermute(block, AXES, ring), got

    _, quantized = lax.fori_loop(0, n, pick, (codebook, jnp.zeros_like(tokens)))
    diff = tokens.astype(F32) - quantized.astype(F32)
    token_loss = jnp.sum(diff * diff, axis=1) / width

    def add(step, carry):
        c, t, total, hits, parts = carry
        owner = lax.rem(me - step + n, n)
        mine = (c // per_dev) == me
        total = total + jax.ops.segment_sum(
            jnp.where(mine, t, 0.0), c % per_dev, num_segments=per_dev
        )
        hits = hits + jax.ops.segment_sum(
            mine.astype(jnp.int32), c % per_dev, num_segments=per_dev
        )
        parts = lax.dynamic_update_slice(parts, jnp.sum(t)[None], (owner,))
        return lax.ppermute(c, AXES, ring), lax.ppermute(t, AXES, ring), total, hits, parts

    start = (
        codes, token_loss, jnp.zeros((per_dev,), F32),
        jnp.zeros((per_dev,), jnp.int32), jnp.zeros((n,), F32),
    )
    _, _, code_loss, counts, parts = lax.fori_loop(0, n, add, start)
    probs = counts.astype(F32) / (rows * n)
    floor_prob = jnp.float32(1.0 / (rows * n))
    terms = jnp.where(counts > 0, probs * jnp.log(jnp.maximum(probs, floor_prob)), 0.0)

    def collect(step, carry):
        entropy, parts = carry
        owner = lax.rem(me - step + n, n)
        parts = lax.dynamic_update_slice(parts, entropy, (owner,))
        return lax.ppermute(entropy, AXES, ring), parts

    _, entropies = lax.fori_loop(0, n, collect, (jnp.sum(terms)[None], jnp.zeros((n,), F32)))
    commitment = 0.25 * jnp.sum(parts) / (rows * n)
    return quantized, token_loss, counts, code_loss, commitment, jnp.exp(-jnp.sum(entropies))


def kernel(
    n, cols, cap, spill, wide_spill,
    codes_hbm, tokens_hbm, book_hbm,
    quant_ref, tloss_ref, counts_ref, closs_ref, scal_ref, flag_ref,
    codes_ref, tokens_ref, book_ref, csend, crecv, hsend, hrecv, psend, precv, gsend, grecv, osend, orecv,
    dsend, drecv, lsend, lrecv, low1h, sel, spill1h, rank1h,
    in_sem, csem_s, csem_r, hsem_s, hsem_r, psem_s, psem_r,
    gsem_s, gsem_r, osem_s, osem_r, lsem_s, lsem_r, bsem, dsem,
):
    rows, width = tokens_hbm.shape
    per = book_hbm.shape[0]
    bits = per.bit_length() - 1
    total_tokens = rows * n
    chips, half = n // 2, cols // 2
    my_row, my_col = lax.axis_index("row"), lax.axis_index("col")
    core = lax.rem(my_col, 2)
    my_chip = lax.div(my_col, 2)
    me = my_row * half + my_chip
    inner = lax.rem(lax.div(my_row + 1, 2), 2)
    beside, across = my_row + 1 - 2 * lax.rem(my_row, 2), 3 - my_row
    near = inner * across + (1 - inner) * beside
    far = inner * beside + (1 - inner) * across
    rows_at = [my_row, near, lax.rem(my_row + 2, 4), far]
    chips_at = [
        my_chip, my_chip + 1 - 2 * lax.rem(my_chip, 2), lax.rem(my_chip + 2, 4), 3 - my_chip
    ]
    spots = [(rows_at[k // half], chips_at[k % half]) for k in range(chips)]
    at = [(r, 2 * c + core) for r, c in spots]
    mirror = [(r, 2 * c + 1 - core) for r, c in spots]
    peer = [r * half + c for r, c in spots]
    fetch_codes = pltpu.make_async_copy(codes_hbm, codes_ref, in_sem.at[0])
    own_book = book_ref.at[pl.ds(pl.multiple_of(core * per, per), per)]
    fetch_book = pltpu.make_async_copy(book_hbm, own_book, in_sem.at[1])
    fetch_tokens = pltpu.make_async_copy(tokens_hbm, tokens_ref, in_sem.at[2])
    fetch_codes.start()

    def remote(src, dst, ssem, rsem, to):
        return pltpu.make_async_remote_copy(
            src_ref=src,
            dst_ref=dst,
            send_sem=ssem,
            recv_sem=rsem,
            device_id=to,
            device_id_type=pl.DeviceIdType.MESH,
        )

    def put(send, recv, ssem, rsem, k):
        return remote(send.at[peer[k]], recv.at[me], ssem, rsem, at[k])

    def spill_put(d, c):
        r, to = rows_at[d], chips_at[c]
        return remote(gsend.at[r, to], grecv.at[r, my_chip], gsem_s, gsem_r.at[r], at[c])

    def joint_put(d):
        return remote(osend.at[rows_at[d]], orecv.at[my_row], osem_s, osem_r, at[d * half])

    def loss_put(k, other):
        to = mirror[k] if other else at[k]
        return remote(lsend.at[peer[k]], lrecv.at[other * chips + me], lsem_s, lsem_r, to)

    def all_in(ref, count, sem):
        part = ref.at[pl.ds(0, count)]
        remote(part, part, sem, sem, mirror[0]).wait_recv()

    def all_out(ref, count, sem):
        part = ref.at[pl.ds(0, count)]
        remote(part, part, sem, sem, mirror[0]).wait_send()

    ask_refs = (csend, crecv, csem_s, csem_r.at[my_row])
    count_refs = (hsend, hrecv, hsem_s, hsem_r)
    reply_refs = (psend, precv, psem_s, psem_r)
    partners = [k for d in ASK_ORDER for k in range(d * half, d * half + half) if k]
    everyone = [(k, other) for d in ASK_ORDER for k in range(d * half, d * half + half)
                for other in (0, 1) if k or other]
    share_book = remote(own_book, own_book, bsem.at[0], bsem.at[1], mirror[0])
    share_asks = remote(dsend, drecv, dsem.at[0], dsem.at[1], mirror[0])

    barrier = pltpu.get_barrier_semaphore()
    for k, other in everyone:
        pl.semaphore_signal(
            barrier, inc=1, device_id=mirror[k] if other else at[k],
            device_id_type=pl.DeviceIdType.MESH,
        )
    fetch_book.start()
    fetch_tokens.start()

    fetch_codes.wait()
    code_row = codes_ref[...].reshape(1, rows)
    hi_row = lax.shift_right_logical(code_row, bits)
    code_col = jnp.broadcast_to(code_row.astype(F32), (128, rows)).T.astype(jnp.int32)
    hi_col = lax.shift_right_logical(code_col, bits)
    lo_col = code_col & (per - 1)
    lane = lax.broadcasted_iota(jnp.int32, (rows, 128), 1)
    own_row = hi_row == lax.broadcasted_iota(jnp.int32, (n, rows), 0)
    for k in range(per // 128):
        low1h[:, k * 128 : (k + 1) * 128] = jnp.where(lo_col == lane + k * 128, 1.0, 0.0).astype(BF16)
    low = low1h[...]
    hist = jnp.dot(jnp.where(own_row, 1.0, 0.0).astype(BF16), low, preferred_element_type=F32)
    odd = (lax.broadcasted_iota(jnp.int32, (n, 128), 0) & 1) == 1

    def first_half(found):
        total = jnp.broadcast_to(jnp.sum(found, axis=1, keepdims=True), (n, 128))
        return total, jnp.where(odd, pltpu.roll(total, 1, 0), 0.0)

    wanted = jnp.where(hist > 0.5, 1.0, 0.0)
    total, ahead = first_half(wanted)
    both = total + ahead
    over = [jnp.where(odd, jnp.maximum(both - float(c), 0.0), 0.0) for c in (cap, 2 * cap)]
    over = jnp.minimum(jnp.concatenate(over, axis=1), 256.0).astype(BF16)
    line = lax.broadcasted_iota(jnp.int32, (2 * n, n), 0)
    source = lax.broadcasted_iota(jnp.int32, (2 * n, n), 1)
    line_of = lax.rem(line, n)
    same = lax.div(line_of, cols) == lax.div(source, cols)
    earlier = lax.div(source, 2) < lax.div(line_of, 2)
    reach = jnp.where(same & (earlier | (line >= n)), 1.0, 0.0).astype(BF16)
    over = jnp.dot(reach, over, preferred_element_type=F32)
    behind = over[:n, :1]
    worst = jnp.max(over[n:], axis=0, keepdims=True)
    heavy = jnp.max(jnp.max(hist, axis=0, keepdims=True), axis=1, keepdims=True) > 256.0
    most = jnp.where(worst[:, EXTRA:] > float(wide_spill), 2.0, 1.0)
    most = jnp.where(worst[:, :EXTRA] > float(spill), most, 0.0)
    most = jnp.where(heavy, 2.0, most)
    most_pair = jnp.broadcast_to(most, (2, EXTRA)).astype(BF16)
    before = lax.broadcasted_iota(jnp.int32, (per, per), 0) < lax.broadcasted_iota(jnp.int32, (per, per), 1)
    before = jnp.where(before, 1.0, 0.0).astype(BF16)
    rank = jnp.dot(wanted.astype(BF16), before, preferred_element_type=F32) + ahead[:, :1]
    rank = jnp.minimum(rank + jnp.where(rank > cap - 0.5, behind, 0.0), 255.0)
    order = jnp.where(wanted > 0.5, rank, -1.0).astype(BF16)
    for q in range(chips):
        csend[q, :, :per] = order[2 * q : 2 * q + 2, :]
        csend[q, :, per:] = most_pair
    crecv[pl.ds(me, 1)] = csend[pl.ds(me, 1)]

    pl.semaphore_wait(barrier, n - 1)
    for k in partners:
        put(*ask_refs, k).start()
    hist16 = jnp.minimum(hist, 256.0).astype(BF16)
    for q in range(chips):
        hsend[q] = hist16[2 * q : 2 * q + 2, :]
    hrecv[pl.ds(me, 1)] = hsend[pl.ds(me, 1)]
    fetch_book.wait()
    share_book.start()
    for k in partners:
        put(*count_refs, k).start()

    rank = rank.astype(BF16)
    hi1h = jnp.where(hi_col[:, :n] == lane[:, :n], 1.0, 0.0).astype(BF16)
    looked = jnp.dot(hi1h, rank, preferred_element_type=F32).astype(BF16) * low
    found = jnp.dot(looked, jnp.ones((per, 128), BF16), preferred_element_type=F32)
    found = found.astype(jnp.int32)
    rank1h[...] = jnp.where(found == lane, 1.0, 0.0).astype(BF16)
    chip_col = lax.shift_right_logical(hi_col, 1)
    slot = jnp.where(found < cap, chip_col * cap + found, -1)
    for k in range(chips * cap // 128):
        sel[:, k * 128 : (k + 1) * 128] = jnp.where(slot == lane + k * 128, 1.0, 0.0).astype(BF16)
    slot = jnp.where(found < cap, -1, lax.div(chip_col, half) * spill + (found - cap))
    planes = chips // half
    for k in range(0, planes * spill, 128):
        wide = min(128, planes * spill - k)
        spill1h[:, k : k + wide] = jnp.where(slot == lane + k, 1.0, 0.0).astype(BF16)[:, :wide]

    both_caps = cap + spill
    place = lax.broadcasted_iota(jnp.int32, (both_caps, per), 0).astype(F32)
    for i, d in enumerate(REPLY_ORDER):
        group = range(d * half, d * half + half)
        all_in(crecv, half if d else half - 1, csem_r.at[rows_at[d]])
        if i == 0:
            share_book.wait_recv()
        picks = []
        for k in group:
            pair = crecv[peer[k]][:, :per].astype(F32)
            picks.append(jnp.concatenate(
                [
                    jnp.where(jnp.broadcast_to(pair[h : h + 1], (both_caps, per)) == place, 1.0, 0.0).astype(BF16)
                    for h in (0, 1)
                ],
                axis=1,
            ))
        packed = jnp.dot(jnp.concatenate(picks, axis=0), book_ref[...], preferred_element_type=F32)
        packed = packed.astype(BF16)
        for j, k in enumerate(group):
            out = psend if k else precv
            start = j * both_caps
            out[peer[k]] = packed[start : start + cap]
            if j:
                gsend[rows_at[d], chips_at[j]] = packed[start + cap : start + both_caps]
            else:
                grecv[rows_at[d], my_chip] = packed[start + cap : start + both_caps]
        for c in range(1, half):
            spill_put(d, c).start()
        for k in group:
            if k:
                put(*reply_refs, k).start()

    for d in REPLY_ORDER:
        all_in(grecv.at[0], half - 1, gsem_r.at[rows_at[d]])
        joint = grecv[rows_at[d], 0].astype(F32)
        for c in range(1, half):
            joint = joint + grecv[rows_at[d], c].astype(F32)
        if d:
            osend[rows_at[d]] = joint.astype(BF16)
            joint_put(d).start()
        else:
            orecv[my_row] = joint.astype(BF16)

    all_in(hrecv, chips - 1, hsem_r)
    got = jnp.concatenate([crecv[q].astype(F32) for q in range(chips)], axis=0)
    asked = jnp.concatenate([hrecv[q].astype(F32) for q in range(chips)], axis=0)
    turn = lax.broadcasted_iota(jnp.int32, (n, n), 0)
    side = jnp.where(turn < chips, core, 1 - core)
    which = 2 * lax.rem(turn, chips) + side
    split = jnp.where(lax.broadcasted_iota(jnp.int32, (n, n), 1) == which, 1.0, 0.0).astype(BF16)
    both = jnp.concatenate([got[:, :per].astype(BF16), asked.astype(BF16)], axis=1)
    both = jnp.dot(split, both, preferred_element_type=F32)
    most_asked = jnp.max(got[:, per:], axis=0, keepdims=True)
    dsend[:, : 2 * per] = both[chips:]
    dsend[:, 2 * per :] = jnp.broadcast_to(most_asked, (chips, EXTRA))
    share_asks.start()
    share_asks.wait_recv()
    counts = jnp.sum(both[:chips, per:] + drecv[:, per : 2 * per], axis=0, keepdims=True)
    counts_ref[...] = counts.astype(jnp.int32)
    probs = counts / total_tokens
    terms = jnp.where(
        counts > 0.5, probs * jnp.log(jnp.maximum(probs, 1.0 / total_tokens)), 0.0
    )
    entropy = jnp.sum(terms, axis=1, keepdims=True)
    flag_ref[0, 0] = jnp.max(jnp.maximum(most_asked, drecv[:1, 2 * per :])).astype(jnp.int32)
    spots_of = [both[:chips, :per].astype(jnp.int32), drecv[:, :per].astype(jnp.int32)]

    all_in(precv, chips - 1, psem_r)
    fetch_tokens.wait()
    packs = precv[...].reshape(chips * cap, width)
    direct = jnp.dot(sel[...], packs, preferred_element_type=F32)
    all_in(orecv, planes - 1, osem_r)
    packs = orecv[...].reshape(planes * spill, width)
    quant = (direct + jnp.dot(spill1h[...], packs, preferred_element_type=F32)).astype(BF16)
    quant_ref[...] = quant
    diff = tokens_ref[...].astype(F32) - quant.astype(F32)
    square = diff * diff
    folded = square[:, :128]
    for k in range(1, width // 128):
        folded = folded + square[:, k * 128 : (k + 1) * 128]
    tloss = jnp.sum(folded.T, axis=0, keepdims=True) / width
    tloss_ref[...] = tloss
    part = jnp.sum(tloss, axis=1, keepdims=True)

    first = tloss.astype(BF16).astype(F32)
    second = (tloss - first).astype(BF16).astype(F32)
    third = tloss - first - second
    own_chip = lax.shift_right_logical(hi_row, 1) == lax.broadcasted_iota(jnp.int32, (chips, rows), 0)
    spread = jnp.concatenate(
        [jnp.where(own_chip, x, 0.0).astype(BF16) for x in (first, second, third)], axis=0
    )
    sums = jnp.dot(spread, rank1h[...], preferred_element_type=F32)
    sums = sums[:chips] + sums[chips : 2 * chips] + sums[2 * chips :]
    lane1 = lax.broadcasted_iota(jnp.int32, (chips, EXTRA), 1)
    sums = jnp.where(lane1 == EXTRA - 2, part, jnp.where(lane1 == EXTRA - 1, entropy, sums))
    for q in range(chips):
        lsend[q] = sums[q : q + 1, :]
    lrecv[pl.ds(me, 1)] = lsend[pl.ds(me, 1)]
    for k, other in everyone:
        loss_put(k, other).start()

    all_out(csend, chips - 1, csem_s)
    all_out(hsend, chips - 1, hsem_s)
    all_out(psend, chips - 1, psem_s)
    all_out(gsend, planes - 1, gsem_s)
    all_out(osend, planes - 1, osem_s)
    share_book.wait_send()
    share_asks.wait_send()
    all_in(lrecv, n - 1, lsem_r)
    added = jnp.zeros((chips, per), F32)
    ends = jnp.zeros((1, EXTRA), F32)
    for other in (0, 1):
        back = lrecv[other * chips : (other + 1) * chips, 0, :]
        spot = spots_of[other]
        parts = [
            jnp.take_along_axis(back, jnp.maximum(spot[:, j : j + 128], 0), axis=1)
            for j in range(0, per, 128)
        ]
        added = added + jnp.where(spot >= 0, jnp.concatenate(parts, axis=1), 0.0)
        ends = ends + jnp.sum(back, axis=0, keepdims=True)
    closs_ref[...] = jnp.sum(added, axis=0, keepdims=True)
    lane1 = lane1[:1]
    perp = jnp.exp(-ends[:, EXTRA - 1 :])
    scal_ref[...] = jnp.where(lane1 == 0, ends[:, EXTRA - 2 : EXTRA - 1] * (0.25 / total_tokens), perp)
    all_out(lrecv, n - 1, lsem_s)


def exchange(n, cols, cap, spill, wide_spill, number, tokens, codebook, codes):
    rows, width = tokens.shape
    per = codebook.shape[0]
    chips, planes = n // 2, n // cols
    vmem = pl.BlockSpec(memory_space=pltpu.VMEM)
    smem = pl.BlockSpec(memory_space=pltpu.SMEM)
    dma = pltpu.SemaphoreType.DMA
    return pl.pallas_call(
        functools.partial(kernel, n, cols, cap, spill, wide_spill),
        out_shape=(
            jax.ShapeDtypeStruct((rows, width), BF16),
            jax.ShapeDtypeStruct((1, rows), F32),
            jax.ShapeDtypeStruct((1, per), jnp.int32),
            jax.ShapeDtypeStruct((1, per), F32),
            jax.ShapeDtypeStruct((1, EXTRA), F32),
            jax.ShapeDtypeStruct((1, 1), jnp.int32),
        ),
        in_specs=[pl.BlockSpec(memory_space=pltpu.HBM)] * 3,
        out_specs=(vmem, vmem, vmem, vmem, vmem, smem),
        scratch_shapes=[
            pltpu.VMEM(codes.shape, jnp.int32),
            pltpu.VMEM((rows, width), BF16),
            pltpu.VMEM((2 * per, width), BF16),
            pltpu.VMEM((chips, 2, per + EXTRA), BF16),
            pltpu.VMEM((chips, 2, per + EXTRA), BF16),
            pltpu.VMEM((chips, 2, per), BF16),
            pltpu.VMEM((chips, 2, per), BF16),
            pltpu.VMEM((chips, cap, width), BF16),
            pltpu.VMEM((chips, cap, width), BF16),
            pltpu.VMEM((planes, cols // 2, spill, width), BF16),
            pltpu.VMEM((planes, cols // 2, spill, width), BF16),
            pltpu.VMEM((planes, spill, width), BF16),
            pltpu.VMEM((planes, spill, width), BF16),
            pltpu.VMEM((chips, 2 * per + EXTRA), F32),
            pltpu.VMEM((chips, 2 * per + EXTRA), F32),
            pltpu.VMEM((chips, 1, EXTRA), F32),
            pltpu.VMEM((n, 1, EXTRA), F32),
            pltpu.VMEM((rows, per), BF16),
            pltpu.VMEM((rows, chips * cap), BF16),
            pltpu.VMEM((rows, planes * spill), BF16),
            pltpu.VMEM((rows, 128), BF16),
            dma((3,)),
            dma, dma((planes,)), *[dma] * 4,
            dma, dma((planes,)), *[dma] * 4,
            dma((2,)), dma((2,)),
        ],
        compiler_params=pltpu.CompilerParams(collective_id=number, has_side_effects=True),
    )(*[pltpu.with_memory_space_constraint(x, pltpu.HBM) for x in (codes, tokens, codebook)])


def finish_kernel(
    quant_ref, tloss_ref, counts_ref, closs_ref, scal_ref,
    quant_out, tloss_out, counts_out, closs_out, commit_out, perp_out, sem,
):
    put = pltpu.make_async_copy(quant_ref, quant_out, sem)
    put.start()
    tloss_out[...] = tloss_ref[...].reshape(tloss_out.shape)
    counts_out[...] = counts_ref[...].reshape(counts_out.shape)
    closs_out[...] = closs_ref[...].reshape(closs_out.shape)
    commit_out[...] = scal_ref[:, :1]
    perp_out[...] = scal_ref[:, 1:2]
    put.wait()


def finish(quantized, token_loss, counts, code_loss, scalars):
    rows, per = token_loss.shape[1], counts.shape[1]
    vmem = pl.BlockSpec(memory_space=pltpu.VMEM)
    q, t, k, c, m, p = pl.pallas_call(
        finish_kernel,
        out_shape=(
            jax.ShapeDtypeStruct(quantized.shape, BF16),
            jax.ShapeDtypeStruct((rows,), F32),
            jax.ShapeDtypeStruct((per,), jnp.int32),
            jax.ShapeDtypeStruct((per,), F32),
            jax.ShapeDtypeStruct((1, 1), F32),
            jax.ShapeDtypeStruct((1, 1), F32),
        ),
        in_specs=[vmem] * 5,
        out_specs=(pl.BlockSpec(memory_space=pltpu.HBM), vmem, vmem, vmem, vmem, vmem),
        scratch_shapes=[pltpu.SemaphoreType.DMA],
    )(quantized, token_loss, counts, code_loss, scalars)
    return q, t, k, c, m[0, 0], p[0, 0]


def asked_plan(n, cols, cap, spill, tokens, codebook, codes):
    wide = spill * 3 // 2
    *outs, flag = exchange(n, cols, cap, spill, wide, 0, tokens, codebook, codes)

    def kept():
        return finish(*outs)

    def wider():
        return finish(*exchange(n, cols, 2 * cap, wide, wide, 1, tokens, codebook, codes)[:-1])

    def ringed():
        return ring_plan(n, tokens, codebook, codes)

    def any_codes():
        return lax.cond(flag[0, 0] > 1, ringed, wider)

    return lax.cond(flag[0, 0] > 0, any_codes, kept)


def on_device(n, cols, tokens, codebook, codes):
    rows, width = tokens.shape
    per = codebook.shape[0]
    cap = -(-rows // (n * 16)) * 16
    spill = cap
    fits = (
        per % 128 == 0
        and per & (per - 1) == 0
        and rows % 128 == 0
        and width % 128 == 0
        and n // 2 * cap % 128 == 0
        and n // cols * spill % 128 == 0
        and n // cols * (spill * 3 // 2) % 64 == 0
        and cols == 8
        and n == 4 * cols
        and n <= 128
        and 2 * cap + spill * 3 // 2 < EXTRA - 1
    )
    if fits:
        return asked_plan(n, cols, cap, spill, tokens, codebook, codes)
    return dense_plan(tokens, codebook, codes)


def solution(mesh):
    n = mesh.shape["row"] * mesh.shape["col"]
    return jax.shard_map(
        functools.partial(on_device, n, mesh.shape["col"]),
        mesh=mesh,
        in_specs=(P(AXES, None), P(AXES, None), P(AXES)),
        out_specs=(P(AXES, None), P(AXES), P(AXES), P(AXES), P(), P()),
        check_vma=False,
    )
```

```python
import functools

import jax
import jax.numpy as jnp
from jax import lax
from jax.experimental import pallas as pl
from jax.experimental.pallas import tpu as pltpu
from jax.sharding import PartitionSpec as P

AXES = ("row", "col")
EXTRA = 128
ASK_ORDER = (3, 2, 1, 0)
REPLY_ORDER = (2, 3, 1, 0)
F32 = jnp.float32
BF16 = jnp.bfloat16


def dense_plan(tokens, codebook, codes):
    tok_rows = tokens.shape[0]
    width = tokens.shape[1]
    per_dev = codebook.shape[0]
    devices = lax.axis_size("row") * lax.axis_size("col")
    total_codes = per_dev * devices
    total_tokens = tok_rows * devices
    full_book = lax.all_gather(codebook, AXES, axis=0, tiled=True)
    quantized = jnp.take(full_book, codes, axis=0)
    diff = tokens.astype(F32) - quantized.astype(F32)
    token_loss = jnp.sum(diff * diff, axis=1) / width
    loss_part = jnp.sum(token_loss)
    local_counts = jax.ops.segment_sum(
        jnp.ones((tok_rows,), F32), codes, num_segments=total_codes
    )
    local_loss = jax.ops.segment_sum(token_loss, codes, num_segments=total_codes)
    floor_prob = jnp.float32(1.0 / total_tokens)
    totals, loss_totals = lax.psum((local_counts, local_loss), AXES)
    loss_sum = lax.psum(loss_part, AXES)
    probs = totals / total_tokens
    terms = jnp.where(
        totals > 0.5, probs * jnp.log(jnp.maximum(probs, floor_prob)), jnp.float32(0.0)
    )
    offset = lax.axis_index(AXES) * per_dev
    owned_counts = lax.dynamic_slice_in_dim(totals, offset, per_dev, 0)
    code_loss = lax.dynamic_slice_in_dim(loss_totals, offset, per_dev, 0)
    commitment = 0.25 * loss_sum / total_tokens
    return (
        quantized,
        token_loss,
        owned_counts.astype(jnp.int32),
        code_loss,
        commitment,
        jnp.exp(-jnp.sum(terms)),
    )


def ring_plan(n, tokens, codebook, codes):
    rows, width = tokens.shape
    per_dev = codebook.shape[0]
    me = lax.axis_index(AXES)
    ring = [(i, (i + 1) % n) for i in range(n)]
    codes = jnp.where(me < n, codes, 0)
    codebook = jnp.where(me < n, codebook, 0)
    hi = codes // per_dev
    lo = codes % per_dev

    def pick(step, carry):
        block, got = carry
        owner = lax.rem(me - step + n, n)
        got = jnp.where((hi == owner)[:, None], jnp.take(block, lo, axis=0), got)
        return lax.ppermute(block, AXES, ring), got

    _, quantized = lax.fori_loop(0, n, pick, (codebook, jnp.zeros_like(tokens)))
    diff = tokens.astype(F32) - quantized.astype(F32)
    token_loss = jnp.sum(diff * diff, axis=1) / width

    def add(step, carry):
        c, t, total, hits, parts = carry
        owner = lax.rem(me - step + n, n)
        mine = (c // per_dev) == me
        total = total + jax.ops.segment_sum(
            jnp.where(mine, t, 0.0), c % per_dev, num_segments=per_dev
        )
        hits = hits + jax.ops.segment_sum(
            mine.astype(jnp.int32), c % per_dev, num_segments=per_dev
        )
        parts = lax.dynamic_update_slice(parts, jnp.sum(t)[None], (owner,))
        return lax.ppermute(c, AXES, ring), lax.ppermute(t, AXES, ring), total, hits, parts

    start = (
        codes, token_loss, jnp.zeros((per_dev,), F32),
        jnp.zeros((per_dev,), jnp.int32), jnp.zeros((n,), F32),
    )
    _, _, code_loss, counts, parts = lax.fori_loop(0, n, add, start)
    probs = counts.astype(F32) / (rows * n)
    floor_prob = jnp.float32(1.0 / (rows * n))
    terms = jnp.where(counts > 0, probs * jnp.log(jnp.maximum(probs, floor_prob)), 0.0)

    def collect(step, carry):
        entropy, parts = carry
        owner = lax.rem(me - step + n, n)
        parts = lax.dynamic_update_slice(parts, entropy, (owner,))
        return lax.ppermute(entropy, AXES, ring), parts

    _, entropies = lax.fori_loop(0, n, collect, (jnp.sum(terms)[None], jnp.zeros((n,), F32)))
    commitment = 0.25 * jnp.sum(parts) / (rows * n)
    return quantized, token_loss, counts, code_loss, commitment, jnp.exp(-jnp.sum(entropies))


def kernel(
    n, cols, cap, spill, wide_spill,
    codes_hbm, tokens_hbm, book_hbm,
    quant_ref, tloss_ref, counts_ref, closs_ref, scal_ref,
    codes_ref, tokens_ref, book_ref, csend, crecv, hsend, hrecv, psend, precv, gsend, grecv, osend, orecv,
    dsend, drecv, lsend, lrecv, low1h, sel, spill1h, rank1h,
    in_sem, csem_s, csem_r, hsem_s, hsem_r, psem_s, psem_r,
    gsem_s, gsem_r, osem_s, osem_r, lsem_s, lsem_r, bsem, dsem,
):
    rows, width = tokens_hbm.shape
    per = book_hbm.shape[0]
    bits = per.bit_length() - 1
    total_tokens = rows * n
    chips, half = n // 2, cols // 2
    my_row, my_col = lax.axis_index("row"), lax.axis_index("col")
    core = lax.rem(my_col, 2)
    my_chip = lax.div(my_col, 2)
    me = my_row * half + my_chip
    inner = lax.rem(lax.div(my_row + 1, 2), 2)
    beside, across = my_row + 1 - 2 * lax.rem(my_row, 2), 3 - my_row
    near = inner * across + (1 - inner) * beside
    far = inner * beside + (1 - inner) * across
    rows_at = [my_row, near, lax.rem(my_row + 2, 4), far]
    chips_at = [
        my_chip, my_chip + 1 - 2 * lax.rem(my_chip, 2), lax.rem(my_chip + 2, 4), 3 - my_chip
    ]
    spots = [(rows_at[k // half], chips_at[k % half]) for k in range(chips)]
    at = [(r, 2 * c + core) for r, c in spots]
    mirror = [(r, 2 * c + 1 - core) for r, c in spots]
    peer = [r * half + c for r, c in spots]
    fetch_codes = pltpu.make_async_copy(codes_hbm, codes_ref, in_sem.at[0])
    own_book = book_ref.at[pl.ds(pl.multiple_of(core * per, per), per)]
    fetch_book = pltpu.make_async_copy(book_hbm, own_book, in_sem.at[1])
    fetch_tokens = pltpu.make_async_copy(tokens_hbm, tokens_ref, in_sem.at[2])
    fetch_codes.start()

    def remote(src, dst, ssem, rsem, to):
        return pltpu.make_async_remote_copy(
            src_ref=src,
            dst_ref=dst,
            send_sem=ssem,
            recv_sem=rsem,
            device_id=to,
            device_id_type=pl.DeviceIdType.MESH,
        )

    def put(send, recv, ssem, rsem, k):
        return remote(send.at[peer[k]], recv.at[me], ssem, rsem, at[k])

    def spill_put(d, c):
        r, to = rows_at[d], chips_at[c]
        return remote(gsend.at[r, to], grecv.at[r, my_chip], gsem_s, gsem_r.at[r], at[c])

    def joint_put(d):
        return remote(osend.at[rows_at[d]], orecv.at[my_row], osem_s, osem_r, at[d * half])

    def loss_put(k, other):
        to = mirror[k] if other else at[k]
        return remote(lsend.at[peer[k]], lrecv.at[other * chips + me], lsem_s, lsem_r, to)

    def all_in(ref, count, sem):
        part = ref.at[pl.ds(0, count)]
        remote(part, part, sem, sem, mirror[0]).wait_recv()

    def all_out(ref, count, sem):
        part = ref.at[pl.ds(0, count)]
        remote(part, part, sem, sem, mirror[0]).wait_send()

    ask_refs = (csend, crecv, csem_s, csem_r.at[my_row])
    count_refs = (hsend, hrecv, hsem_s, hsem_r)
    reply_refs = (psend, precv, psem_s, psem_r)
    partners = [k for d in ASK_ORDER for k in range(d * half, d * half + half) if k]
    everyone = [(k, other) for d in ASK_ORDER for k in range(d * half, d * half + half)
                for other in (0, 1) if k or other]
    share_book = remote(own_book, own_book, bsem.at[0], bsem.at[1], mirror[0])
    share_asks = remote(dsend, drecv, dsem.at[0], dsem.at[1], mirror[0])

    barrier = pltpu.get_barrier_semaphore()
    for k, other in everyone:
        pl.semaphore_signal(
            barrier, inc=1, device_id=mirror[k] if other else at[k],
            device_id_type=pl.DeviceIdType.MESH,
        )
    fetch_book.start()
    fetch_tokens.start()

    fetch_codes.wait()
    code_row = codes_ref[...].reshape(1, rows)
    hi_row = lax.shift_right_logical(code_row, bits)
    code_col = jnp.broadcast_to(code_row.astype(F32), (128, rows)).T.astype(jnp.int32)
    hi_col = lax.shift_right_logical(code_col, bits)
    lo_col = code_col & (per - 1)
    lane = lax.broadcasted_iota(jnp.int32, (rows, 128), 1)
    own_row = hi_row == lax.broadcasted_iota(jnp.int32, (n, rows), 0)
    for k in range(per // 128):
        low1h[:, k * 128 : (k + 1) * 128] = jnp.where(lo_col == lane + k * 128, 1.0, 0.0).astype(BF16)
    low = low1h[...]
    hist = jnp.dot(jnp.where(own_row, 1.0, 0.0).astype(BF16), low, preferred_element_type=F32)
    odd = (lax.broadcasted_iota(jnp.int32, (n, 128), 0) & 1) == 1

    def first_half(found):
        total = jnp.broadcast_to(jnp.sum(found, axis=1, keepdims=True), (n, 128))
        return total, jnp.where(odd, pltpu.roll(total, 1, 0), 0.0)

    wanted = jnp.where(hist > 0.5, 1.0, 0.0)
    total, ahead = first_half(wanted)
    both = total + ahead
    over = [jnp.where(odd, jnp.maximum(both - float(c), 0.0), 0.0) for c in (cap, 2 * cap)]
    over = jnp.minimum(jnp.concatenate(over, axis=1), 256.0).astype(BF16)
    line = lax.broadcasted_iota(jnp.int32, (2 * n, n), 0)
    source = lax.broadcasted_iota(jnp.int32, (2 * n, n), 1)
    line_of = lax.rem(line, n)
    same = lax.div(line_of, cols) == lax.div(source, cols)
    earlier = lax.div(source, 2) < lax.div(line_of, 2)
    reach = jnp.where(same & (earlier | (line >= n)), 1.0, 0.0).astype(BF16)
    over = jnp.dot(reach, over, preferred_element_type=F32)
    behind = over[:n, :1]
    worst = jnp.max(over[n:], axis=0, keepdims=True)
    heavy = jnp.max(jnp.max(hist, axis=0, keepdims=True), axis=1, keepdims=True) > 256.0
    most = jnp.where(worst[:, EXTRA:] > float(wide_spill), 2.0, 1.0)
    most = jnp.where(worst[:, :EXTRA] > float(spill), most, 0.0)
    most = jnp.where(heavy, 2.0, most)
    most_pair = jnp.broadcast_to(most, (2, EXTRA)).astype(BF16)
    before = lax.broadcasted_iota(jnp.int32, (per, per), 0) < lax.broadcasted_iota(jnp.int32, (per, per), 1)
    before = jnp.where(before, 1.0, 0.0).astype(BF16)
    rank = jnp.dot(wanted.astype(BF16), before, preferred_element_type=F32) + ahead[:, :1]
    rank = jnp.minimum(rank + jnp.where(rank > cap - 0.5, behind, 0.0), 255.0)
    order = jnp.where(wanted > 0.5, rank, -1.0).astype(BF16)
    for q in range(chips):
        csend[q, :, :per] = order[2 * q : 2 * q + 2, :]
        csend[q, :, per:] = most_pair
    crecv[pl.ds(me, 1)] = csend[pl.ds(me, 1)]

    pl.semaphore_wait(barrier, n - 1)
    for k in partners:
        put(*ask_refs, k).start()
    hist16 = jnp.minimum(hist, 256.0).astype(BF16)
    for q in range(chips):
        hsend[q] = hist16[2 * q : 2 * q + 2, :]
    hrecv[pl.ds(me, 1)] = hsend[pl.ds(me, 1)]
    fetch_book.wait()
    share_book.start()
    for k in partners:
        put(*count_refs, k).start()

    rank = rank.astype(BF16)
    hi1h = jnp.where(hi_col[:, :n] == lane[:, :n], 1.0, 0.0).astype(BF16)
    looked = jnp.dot(hi1h, rank, preferred_element_type=F32).astype(BF16) * low
    found = jnp.dot(looked, jnp.ones((per, 128), BF16), preferred_element_type=F32)
    found = found.astype(jnp.int32)
    rank1h[...] = jnp.where(found == lane, 1.0, 0.0).astype(BF16)
    chip_col = lax.shift_right_logical(hi_col, 1)
    slot = jnp.where(found < cap, chip_col * cap + found, -1)
    for k in range(chips * cap // 128):
        sel[:, k * 128 : (k + 1) * 128] = jnp.where(slot == lane + k * 128, 1.0, 0.0).astype(BF16)
    slot = jnp.where(found < cap, -1, lax.div(chip_col, half) * spill + (found - cap))
    planes = chips // half
    for k in range(0, planes * spill, 128):
        wide = min(128, planes * spill - k)
        spill1h[:, k : k + wide] = jnp.where(slot == lane + k, 1.0, 0.0).astype(BF16)[:, :wide]

    both_caps = cap + -(-spill // 16) * 16
    place = lax.broadcasted_iota(jnp.int32, (both_caps, per), 0).astype(F32)
    for i, d in enumerate(REPLY_ORDER):
        group = range(d * half, d * half + half)
        all_in(crecv, half if d else half - 1, csem_r.at[rows_at[d]])
        if i == 0:
            share_book.wait_recv()
        picks = []
        for k in group:
            pair = crecv[peer[k]][:, :per].astype(F32)
            picks.append(jnp.concatenate(
                [
                    jnp.where(jnp.broadcast_to(pair[h : h + 1], (both_caps, per)) == place, 1.0, 0.0).astype(BF16)
                    for h in (0, 1)
                ],
                axis=1,
            ))
        packed = jnp.dot(jnp.concatenate(picks, axis=0), book_ref[...], preferred_element_type=F32)
        packed = packed.astype(BF16)
        for j, k in enumerate(group):
            out = psend if k else precv
            start = j * both_caps
            out[peer[k]] = packed[start : start + cap]
            if j:
                gsend[rows_at[d], chips_at[j]] = packed[start + cap : start + cap + spill]
            else:
                grecv[rows_at[d], my_chip] = packed[start + cap : start + cap + spill]
        for c in range(1, half):
            spill_put(d, c).start()
        for k in group:
            if k:
                put(*reply_refs, k).start()

    for d in REPLY_ORDER:
        all_in(grecv.at[0], half - 1, gsem_r.at[rows_at[d]])
        joint = grecv[rows_at[d], 0].astype(F32)
        for c in range(1, half):
            joint = joint + grecv[rows_at[d], c].astype(F32)
        if d:
            osend[rows_at[d]] = joint.astype(BF16)
            joint_put(d).start()
        else:
            orecv[my_row] = joint.astype(BF16)

    all_in(hrecv, chips - 1, hsem_r)
    got = jnp.concatenate([crecv[q].astype(F32) for q in range(chips)], axis=0)
    asked = jnp.concatenate([hrecv[q].astype(F32) for q in range(chips)], axis=0)
    turn = lax.broadcasted_iota(jnp.int32, (n, n), 0)
    side = jnp.where(turn < chips, core, 1 - core)
    which = 2 * lax.rem(turn, chips) + side
    split = jnp.where(lax.broadcasted_iota(jnp.int32, (n, n), 1) == which, 1.0, 0.0).astype(BF16)
    both = jnp.concatenate([got[:, :per].astype(BF16), asked.astype(BF16)], axis=1)
    both = jnp.dot(split, both, preferred_element_type=F32)
    most_asked = jnp.max(got[:, per:], axis=0, keepdims=True)
    dsend[:, : 2 * per] = both[chips:]
    dsend[:, 2 * per :] = jnp.broadcast_to(most_asked, (chips, EXTRA))
    share_asks.start()
    share_asks.wait_recv()
    counts = jnp.sum(both[:chips, per:] + drecv[:, per : 2 * per], axis=0, keepdims=True)
    counts_ref[...] = counts.astype(jnp.int32)
    probs = counts / total_tokens
    terms = jnp.where(
        counts > 0.5, probs * jnp.log(jnp.maximum(probs, 1.0 / total_tokens)), 0.0
    )
    entropy = jnp.sum(terms, axis=1, keepdims=True)
    flag = jnp.maximum(most_asked, drecv[:1, 2 * per :])
    spots_of = [both[:chips, :per].astype(jnp.int32), drecv[:, :per].astype(jnp.int32)]

    all_in(precv, chips - 1, psem_r)
    fetch_tokens.wait()
    packs = precv[...].reshape(chips * cap, width)
    direct = jnp.dot(sel[...], packs, preferred_element_type=F32)
    all_in(orecv, planes - 1, osem_r)
    packs = orecv[...].reshape(planes * spill, width)
    quant = (direct + jnp.dot(spill1h[...], packs, preferred_element_type=F32)).astype(BF16)
    quant_ref[...] = quant
    diff = tokens_ref[...].astype(F32) - quant.astype(F32)
    square = diff * diff
    folded = square[:, :128]
    for k in range(1, width // 128):
        folded = folded + square[:, k * 128 : (k + 1) * 128]
    tloss = jnp.sum(folded.T, axis=0, keepdims=True) / width
    tloss_ref[...] = tloss
    part = jnp.sum(tloss, axis=1, keepdims=True)

    first = tloss.astype(BF16).astype(F32)
    second = (tloss - first).astype(BF16).astype(F32)
    third = tloss - first - second
    own_chip = lax.shift_right_logical(hi_row, 1) == lax.broadcasted_iota(jnp.int32, (chips, rows), 0)
    spread = jnp.concatenate(
        [jnp.where(own_chip, x, 0.0).astype(BF16) for x in (first, second, third)], axis=0
    )
    sums = jnp.dot(spread, rank1h[...], preferred_element_type=F32)
    sums = sums[:chips] + sums[chips : 2 * chips] + sums[2 * chips :]
    lane1 = lax.broadcasted_iota(jnp.int32, (chips, EXTRA), 1)
    sums = jnp.where(lane1 == EXTRA - 2, part, jnp.where(lane1 == EXTRA - 1, entropy, sums))
    for q in range(chips):
        lsend[q] = sums[q : q + 1, :]
    lrecv[pl.ds(me, 1)] = lsend[pl.ds(me, 1)]
    for k, other in everyone:
        loss_put(k, other).start()

    all_out(csend, chips - 1, csem_s)
    all_out(hsend, chips - 1, hsem_s)
    all_out(psend, chips - 1, psem_s)
    all_out(gsend, planes - 1, gsem_s)
    all_out(osend, planes - 1, osem_s)
    share_book.wait_send()
    share_asks.wait_send()
    all_in(lrecv, n - 1, lsem_r)
    added = jnp.zeros((chips, per), F32)
    ends = jnp.zeros((1, EXTRA), F32)
    for other in (0, 1):
        back = lrecv[other * chips : (other + 1) * chips, 0, :]
        spot = spots_of[other]
        parts = [
            jnp.take_along_axis(back, jnp.maximum(spot[:, j : j + 128], 0), axis=1)
            for j in range(0, per, 128)
        ]
        added = added + jnp.where(spot >= 0, jnp.concatenate(parts, axis=1), 0.0)
        ends = ends + jnp.sum(back, axis=0, keepdims=True)
    closs_ref[...] = jnp.sum(added, axis=0, keepdims=True)
    lane1 = lane1[:1]
    perp = jnp.exp(-ends[:, EXTRA - 1 :])
    commit = ends[:, EXTRA - 2 : EXTRA - 1] * (0.25 / total_tokens)
    scal_ref[...] = jnp.where(lane1 == 0, commit, jnp.where(lane1 == 1, perp, flag))
    all_out(lrecv, n - 1, lsem_s)


def exchange(n, cols, cap, spill, wide_spill, number, tokens, codebook, codes):
    rows, width = tokens.shape
    per = codebook.shape[0]
    chips, planes = n // 2, n // cols
    vmem = pl.BlockSpec(memory_space=pltpu.VMEM)
    dma = pltpu.SemaphoreType.DMA
    return pl.pallas_call(
        functools.partial(kernel, n, cols, cap, spill, wide_spill),
        out_shape=(
            pltpu.VMEM((rows, width), BF16),
            pltpu.VMEM((1, rows), F32),
            pltpu.VMEM((1, per), jnp.int32),
            pltpu.VMEM((1, per), F32),
            pltpu.VMEM((1, EXTRA), F32),
        ),
        in_specs=[pl.BlockSpec(memory_space=pltpu.HBM)] * 3,
        out_specs=(vmem,) * 5,
        scratch_shapes=[
            pltpu.VMEM(codes.shape, jnp.int32),
            pltpu.VMEM((rows, width), BF16),
            pltpu.VMEM((2 * per, width), BF16),
            pltpu.VMEM((chips, 2, per + EXTRA), BF16),
            pltpu.VMEM((chips, 2, per + EXTRA), BF16),
            pltpu.VMEM((chips, 2, per), BF16),
            pltpu.VMEM((chips, 2, per), BF16),
            pltpu.VMEM((chips, cap, width), BF16),
            pltpu.VMEM((chips, cap, width), BF16),
            pltpu.VMEM((planes, cols // 2, spill, width), BF16),
            pltpu.VMEM((planes, cols // 2, spill, width), BF16),
            pltpu.VMEM((planes, spill, width), BF16),
            pltpu.VMEM((planes, spill, width), BF16),
            pltpu.VMEM((chips, 2 * per + EXTRA), F32),
            pltpu.VMEM((chips, 2 * per + EXTRA), F32),
            pltpu.VMEM((chips, 1, EXTRA), F32),
            pltpu.VMEM((n, 1, EXTRA), F32),
            pltpu.VMEM((rows, per), BF16),
            pltpu.VMEM((rows, chips * cap), BF16),
            pltpu.VMEM((rows, planes * spill), BF16),
            pltpu.VMEM((rows, 128), BF16),
            dma((3,)),
            dma, dma((planes,)), *[dma] * 4,
            dma, dma((planes,)), *[dma] * 4,
            dma((2,)), dma((2,)),
        ],
        compiler_params=pltpu.CompilerParams(collective_id=number, has_side_effects=True),
    )(*[pltpu.with_memory_space_constraint(x, pltpu.HBM) for x in (codes, tokens, codebook)])


def finish_kernel(
    quant_ref, tloss_ref, counts_ref, closs_ref, scal_ref,
    quant_out, tloss_out, counts_out, closs_out, commit_out, perp_out, flag_out, sem,
):
    put = pltpu.make_async_copy(quant_ref, quant_out, sem)
    put.start()
    tloss_out[...] = tloss_ref[...].reshape(tloss_out.shape)
    counts_out[...] = counts_ref[...].reshape(counts_out.shape)
    closs_out[...] = closs_ref[...].reshape(closs_out.shape)
    commit_out[...] = scal_ref[:, :1]
    perp_out[...] = scal_ref[:, 1:2]
    flag_out[...] = scal_ref[:, 2:3].astype(jnp.int32)
    put.wait()


def finish(quantized, token_loss, counts, code_loss, scalars):
    rows, per = token_loss.shape[1], counts.shape[1]
    vmem = pl.BlockSpec(memory_space=pltpu.VMEM)
    q, t, k, c, m, p, f = pl.pallas_call(
        finish_kernel,
        out_shape=(
            jax.ShapeDtypeStruct(quantized.shape, BF16),
            jax.ShapeDtypeStruct((rows,), F32),
            jax.ShapeDtypeStruct((per,), jnp.int32),
            jax.ShapeDtypeStruct((per,), F32),
            jax.ShapeDtypeStruct((1, 1), F32),
            jax.ShapeDtypeStruct((1, 1), F32),
            jax.ShapeDtypeStruct((1, 1), jnp.int32),
        ),
        in_specs=[vmem] * 5,
        out_specs=(pl.BlockSpec(memory_space=pltpu.HBM), vmem, vmem, vmem, vmem, vmem, vmem),
        scratch_shapes=[pltpu.SemaphoreType.DMA],
        compiler_params=pltpu.CompilerParams(vmem_limit_bytes=4 << 20),
    )(quantized, token_loss, counts, code_loss, scalars)
    return q, t, k, c, m[0, 0], p[0, 0], f


def asked_plan(n, cols, cap, spill, tokens, codebook, codes):
    wide = spill * 2
    outs = exchange(n, cols, cap, spill, wide, 0, tokens, codebook, codes)

    *done, flag = finish(*outs)

    def kept():
        return tuple(done)

    def wider():
        return finish(*exchange(n, cols, 2 * cap, wide, wide, 1, tokens, codebook, codes))[:-1]

    def ringed():
        return ring_plan(n, tokens, codebook, codes)

    def any_codes():
        return lax.cond(flag[0, 0] > 1, ringed, wider)

    return lax.cond(flag[0, 0] > 0, any_codes, kept)


def on_device(n, cols, tokens, codebook, codes):
    rows, width = tokens.shape
    per = codebook.shape[0]
    cap = -(-rows // (n * 16)) * 16
    spill = cap * 3 // 4
    fits = (
        per % 128 == 0
        and per & (per - 1) == 0
        and rows % 128 == 0
        and width % 128 == 0
        and n // 2 * cap % 128 == 0
        and spill % 8 == 0
        and cols == 8
        and n == 4 * cols
        and n <= 128
        and 2 * cap + 2 * spill < EXTRA - 1
    )
    if fits:
        return asked_plan(n, cols, cap, spill, tokens, codebook, codes)
    return dense_plan(tokens, codebook, codes)


def solution(mesh):
    n = mesh.shape["row"] * mesh.shape["col"]
    return jax.shard_map(
        functools.partial(on_device, n, mesh.shape["col"]),
        mesh=mesh,
        in_specs=(P(AXES, None), P(AXES, None), P(AXES)),
        out_specs=(P(AXES, None), P(AXES), P(AXES), P(AXES), P(), P()),
        check_vma=False,
    )
```

```python
import functools

import jax
import jax.numpy as jnp
from jax import lax
from jax.experimental import pallas as pl
from jax.experimental.pallas import tpu as pltpu
from jax.sharding import PartitionSpec as P

AXES = ("row", "col")
EXTRA = 128
ASK_ORDER = (3, 2, 1, 0)
REPLY_ORDER = (2, 3, 1, 0)
F32 = jnp.float32
BF16 = jnp.bfloat16


def dense_plan(tokens, codebook, codes):
    tok_rows = tokens.shape[0]
    width = tokens.shape[1]
    per_dev = codebook.shape[0]
    devices = lax.axis_size("row") * lax.axis_size("col")
    total_codes = per_dev * devices
    total_tokens = tok_rows * devices
    full_book = lax.all_gather(codebook, AXES, axis=0, tiled=True)
    quantized = jnp.take(full_book, codes, axis=0)
    diff = tokens.astype(F32) - quantized.astype(F32)
    token_loss = jnp.sum(diff * diff, axis=1) / width
    loss_part = jnp.sum(token_loss)
    local_counts = jax.ops.segment_sum(
        jnp.ones((tok_rows,), F32), codes, num_segments=total_codes
    )
    local_loss = jax.ops.segment_sum(token_loss, codes, num_segments=total_codes)
    floor_prob = jnp.float32(1.0 / total_tokens)
    totals, loss_totals = lax.psum((local_counts, local_loss), AXES)
    loss_sum = lax.psum(loss_part, AXES)
    probs = totals / total_tokens
    terms = jnp.where(
        totals > 0.5, probs * jnp.log(jnp.maximum(probs, floor_prob)), jnp.float32(0.0)
    )
    offset = lax.axis_index(AXES) * per_dev
    owned_counts = lax.dynamic_slice_in_dim(totals, offset, per_dev, 0)
    code_loss = lax.dynamic_slice_in_dim(loss_totals, offset, per_dev, 0)
    commitment = 0.25 * loss_sum / total_tokens
    return (
        quantized,
        token_loss,
        owned_counts.astype(jnp.int32),
        code_loss,
        commitment,
        jnp.exp(-jnp.sum(terms)),
    )


def ring_plan(n, tokens, codebook, codes):
    rows, width = tokens.shape
    per_dev = codebook.shape[0]
    me = lax.axis_index(AXES)
    ring = [(i, (i + 1) % n) for i in range(n)]
    hi = codes // per_dev
    lo = codes % per_dev

    def pick(step, carry):
        block, got = carry
        owner = lax.rem(me - step + n, n)
        got = jnp.where((hi == owner)[:, None], jnp.take(block, lo, axis=0), got)
        return lax.ppermute(block, AXES, ring), got

    _, quantized = lax.fori_loop(0, n, pick, (codebook, jnp.zeros_like(tokens)))
    diff = tokens.astype(F32) - quantized.astype(F32)
    token_loss = jnp.sum(diff * diff, axis=1) / width

    def add(step, carry):
        c, t, total, hits, parts = carry
        owner = lax.rem(me - step + n, n)
        mine = (c // per_dev) == me
        total = total + jax.ops.segment_sum(
            jnp.where(mine, t, 0.0), c % per_dev, num_segments=per_dev
        )
        hits = hits + jax.ops.segment_sum(
            mine.astype(jnp.int32), c % per_dev, num_segments=per_dev
        )
        parts = lax.dynamic_update_slice(parts, jnp.sum(t)[None], (owner,))
        return lax.ppermute(c, AXES, ring), lax.ppermute(t, AXES, ring), total, hits, parts

    start = (
        codes, token_loss, jnp.zeros((per_dev,), F32),
        jnp.zeros((per_dev,), jnp.int32), jnp.zeros((n,), F32),
    )
    _, _, code_loss, counts, parts = lax.fori_loop(0, n, add, start)
    probs = counts.astype(F32) / (rows * n)
    floor_prob = jnp.float32(1.0 / (rows * n))
    terms = jnp.where(counts > 0, probs * jnp.log(jnp.maximum(probs, floor_prob)), 0.0)

    def collect(step, carry):
        entropy, parts = carry
        owner = lax.rem(me - step + n, n)
        parts = lax.dynamic_update_slice(parts, entropy, (owner,))
        return lax.ppermute(entropy, AXES, ring), parts

    _, entropies = lax.fori_loop(0, n, collect, (jnp.sum(terms)[None], jnp.zeros((n,), F32)))
    commitment = 0.25 * jnp.sum(parts) / (rows * n)
    return quantized, token_loss, counts, code_loss, commitment, jnp.exp(-jnp.sum(entropies))


def kernel(
    n, cols, cap, spill, wide_spill,
    codes_hbm, tokens_hbm, book_hbm,
    quant_ref, tloss_ref, counts_ref, closs_ref, scal_ref,
    codes_ref, tokens_ref, book_ref, csend, crecv, hsend, hrecv, psend, precv, gsend, grecv, osend, orecv,
    dsend, drecv, lsend, lrecv, low1h, sel, spill1h, rank1h,
    in_sem, csem_s, csem_r, hsem_s, hsem_r, psem_s, psem_r,
    gsem_s, gsem_r, osem_s, osem_r, lsem_s, lsem_r, bsem, dsem,
):
    rows, width = tokens_hbm.shape
    per = book_hbm.shape[0]
    bits = per.bit_length() - 1
    total_tokens = rows * n
    chips, half = n // 2, cols // 2
    my_row, my_col = lax.axis_index("row"), lax.axis_index("col")
    core = lax.rem(my_col, 2)
    my_chip = lax.div(my_col, 2)
    me = my_row * half + my_chip
    inner = lax.rem(lax.div(my_row + 1, 2), 2)
    beside, across = my_row + 1 - 2 * lax.rem(my_row, 2), 3 - my_row
    near = inner * across + (1 - inner) * beside
    far = inner * beside + (1 - inner) * across
    rows_at = [my_row, near, lax.rem(my_row + 2, 4), far]
    chips_at = [
        my_chip, my_chip + 1 - 2 * lax.rem(my_chip, 2), lax.rem(my_chip + 2, 4), 3 - my_chip
    ]
    spots = [(rows_at[k // half], chips_at[k % half]) for k in range(chips)]
    at = [(r, 2 * c + core) for r, c in spots]
    mirror = [(r, 2 * c + 1 - core) for r, c in spots]
    peer = [r * half + c for r, c in spots]
    fetch_codes = pltpu.make_async_copy(codes_hbm, codes_ref, in_sem.at[0])
    own_book = book_ref.at[pl.ds(pl.multiple_of(core * per, per), per)]
    fetch_book = pltpu.make_async_copy(book_hbm, own_book, in_sem.at[1])
    fetch_tokens = pltpu.make_async_copy(tokens_hbm, tokens_ref, in_sem.at[2])
    fetch_codes.start()

    def remote(src, dst, ssem, rsem, to):
        return pltpu.make_async_remote_copy(
            src_ref=src,
            dst_ref=dst,
            send_sem=ssem,
            recv_sem=rsem,
            device_id=to,
            device_id_type=pl.DeviceIdType.MESH,
        )

    def put(send, recv, ssem, rsem, k):
        return remote(send.at[peer[k]], recv.at[me], ssem, rsem, at[k])

    def spill_put(d, c):
        r, to = rows_at[d], chips_at[c]
        return remote(gsend.at[r, to], grecv.at[r, my_chip], gsem_s, gsem_r.at[r], at[c])

    def joint_put(d):
        return remote(osend.at[rows_at[d]], orecv.at[my_row], osem_s, osem_r, at[d * half])

    def loss_put(k, other):
        to = mirror[k] if other else at[k]
        return remote(lsend.at[peer[k]], lrecv.at[other * chips + me], lsem_s, lsem_r, to)

    def all_in(ref, count, sem):
        part = ref.at[pl.ds(0, count)]
        remote(part, part, sem, sem, mirror[0]).wait_recv()

    def all_out(ref, count, sem):
        part = ref.at[pl.ds(0, count)]
        remote(part, part, sem, sem, mirror[0]).wait_send()

    ask_refs = (csend, crecv, csem_s, csem_r.at[my_row])
    count_refs = (hsend, hrecv, hsem_s, hsem_r)
    reply_refs = (psend, precv, psem_s, psem_r)
    partners = [k for d in ASK_ORDER for k in range(d * half, d * half + half) if k]
    everyone = [(k, other) for d in ASK_ORDER for k in range(d * half, d * half + half)
                for other in (0, 1) if k or other]
    share_book = remote(own_book, own_book, bsem.at[0], bsem.at[1], mirror[0])
    share_asks = remote(dsend, drecv, dsem.at[0], dsem.at[1], mirror[0])

    barrier = pltpu.get_barrier_semaphore()
    for k, other in everyone:
        pl.semaphore_signal(
            barrier, inc=1, device_id=mirror[k] if other else at[k],
            device_id_type=pl.DeviceIdType.MESH,
        )
    fetch_book.start()
    fetch_tokens.start()

    fetch_codes.wait()
    code_row = codes_ref[...].reshape(1, rows)
    hi_row = lax.shift_right_logical(code_row, bits)
    code_col = jnp.broadcast_to(code_row.astype(F32), (128, rows)).T.astype(jnp.int32)
    hi_col = lax.shift_right_logical(code_col, bits)
    lo_col = code_col & (per - 1)
    lane = lax.broadcasted_iota(jnp.int32, (rows, 128), 1)
    own_row = hi_row == lax.broadcasted_iota(jnp.int32, (n, rows), 0)
    for k in range(per // 128):
        low1h[:, k * 128 : (k + 1) * 128] = jnp.where(lo_col == lane + k * 128, 1.0, 0.0).astype(BF16)
    low = low1h[...]
    hist = jnp.dot(jnp.where(own_row, 1.0, 0.0).astype(BF16), low, preferred_element_type=F32)
    odd = (lax.broadcasted_iota(jnp.int32, (n, 128), 0) & 1) == 1

    def first_half(found):
        total = jnp.broadcast_to(jnp.sum(found, axis=1, keepdims=True), (n, 128))
        return total, jnp.where(odd, pltpu.roll(total, 1, 0), 0.0)

    wanted = jnp.where(hist > 0.5, 1.0, 0.0)
    total, ahead = first_half(wanted)
    both = total + ahead
    over = [jnp.where(odd, jnp.maximum(both - float(c), 0.0), 0.0) for c in (cap, 2 * cap)]
    over = jnp.minimum(jnp.concatenate(over, axis=1), 256.0).astype(BF16)
    line = lax.broadcasted_iota(jnp.int32, (2 * n, n), 0)
    source = lax.broadcasted_iota(jnp.int32, (2 * n, n), 1)
    line_of = lax.rem(line, n)
    same = lax.div(line_of, cols) == lax.div(source, cols)
    earlier = lax.div(source, 2) < lax.div(line_of, 2)
    reach = jnp.where(same & (earlier | (line >= n)), 1.0, 0.0).astype(BF16)
    over = jnp.dot(reach, over, preferred_element_type=F32)
    behind = over[:n, :1]
    worst = jnp.max(over[n:], axis=0, keepdims=True)
    heavy = jnp.max(jnp.max(hist, axis=0, keepdims=True), axis=1, keepdims=True) > 256.0
    most = jnp.where(worst[:, EXTRA:] > float(wide_spill), 2.0, 1.0)
    most = jnp.where(worst[:, :EXTRA] > float(spill), most, 0.0)
    most = jnp.where(heavy, 2.0, most)
    most_pair = jnp.broadcast_to(most, (2, EXTRA)).astype(BF16)
    before = lax.broadcasted_iota(jnp.int32, (per, per), 0) < lax.broadcasted_iota(jnp.int32, (per, per), 1)
    before = jnp.where(before, 1.0, 0.0).astype(BF16)
    rank = jnp.dot(wanted.astype(BF16), before, preferred_element_type=F32) + ahead[:, :1]
    rank = jnp.minimum(rank + jnp.where(rank > cap - 0.5, behind, 0.0), 255.0)
    order = jnp.where(wanted > 0.5, rank, -1.0).astype(BF16)
    for q in range(chips):
        csend[q, :, :per] = order[2 * q : 2 * q + 2, :]
        csend[q, :, per:] = most_pair
    crecv[pl.ds(me, 1)] = csend[pl.ds(me, 1)]

    pl.semaphore_wait(barrier, n - 1)
    for k in partners:
        put(*ask_refs, k).start()
    hist16 = jnp.minimum(hist, 256.0).astype(BF16)
    for q in range(chips):
        hsend[q] = hist16[2 * q : 2 * q + 2, :]
    hrecv[pl.ds(me, 1)] = hsend[pl.ds(me, 1)]
    fetch_book.wait()
    share_book.start()
    for k in partners:
        put(*count_refs, k).start()

    rank = rank.astype(BF16)
    hi1h = jnp.where(hi_col[:, :n] == lane[:, :n], 1.0, 0.0).astype(BF16)
    looked = jnp.dot(hi1h, rank, preferred_element_type=F32).astype(BF16) * low
    found = jnp.dot(looked, jnp.ones((per, 128), BF16), preferred_element_type=F32)
    found = found.astype(jnp.int32)
    rank1h[...] = jnp.where(found == lane, 1.0, 0.0).astype(BF16)
    chip_col = lax.shift_right_logical(hi_col, 1)
    slot = jnp.where(found < cap, chip_col * cap + found, -1)
    for k in range(chips * cap // 128):
        sel[:, k * 128 : (k + 1) * 128] = jnp.where(slot == lane + k * 128, 1.0, 0.0).astype(BF16)
    slot = jnp.where(found < cap, -1, lax.div(chip_col, half) * spill + (found - cap))
    planes = chips // half
    for k in range(0, planes * spill, 128):
        wide = min(128, planes * spill - k)
        spill1h[:, k : k + wide] = jnp.where(slot == lane + k, 1.0, 0.0).astype(BF16)[:, :wide]

    both_caps = cap + -(-spill // 16) * 16
    place = lax.broadcasted_iota(jnp.int32, (both_caps, per), 0).astype(F32)
    for i, d in enumerate(REPLY_ORDER):
        group = range(d * half, d * half + half)
        all_in(crecv, half if d else half - 1, csem_r.at[rows_at[d]])
        if i == 0:
            share_book.wait_recv()
        picks = []
        for k in group:
            pair = crecv[peer[k]][:, :per].astype(F32)
            picks.append(jnp.concatenate(
                [
                    jnp.where(jnp.broadcast_to(pair[h : h + 1], (both_caps, per)) == place, 1.0, 0.0).astype(BF16)
                    for h in (0, 1)
                ],
                axis=1,
            ))
        packed = jnp.dot(jnp.concatenate(picks, axis=0), book_ref[...], preferred_element_type=F32)
        packed = packed.astype(BF16)
        for j, k in enumerate(group):
            out = psend if k else precv
            start = j * both_caps
            out[peer[k]] = packed[start : start + cap]
            if j:
                gsend[rows_at[d], chips_at[j]] = packed[start + cap : start + cap + spill]
            else:
                grecv[rows_at[d], my_chip] = packed[start + cap : start + cap + spill]
        for c in range(1, half):
            spill_put(d, c).start()
        for k in group:
            if k:
                put(*reply_refs, k).start()

    for d in REPLY_ORDER:
        all_in(grecv.at[0], half - 1, gsem_r.at[rows_at[d]])
        joint = grecv[rows_at[d], 0].astype(F32)
        for c in range(1, half):
            joint = joint + grecv[rows_at[d], c].astype(F32)
        if d:
            osend[rows_at[d]] = joint.astype(BF16)
            joint_put(d).start()
        else:
            orecv[my_row] = joint.astype(BF16)

    all_in(hrecv, chips - 1, hsem_r)
    got = jnp.concatenate([crecv[q].astype(F32) for q in range(chips)], axis=0)
    asked = jnp.concatenate([hrecv[q].astype(F32) for q in range(chips)], axis=0)
    turn = lax.broadcasted_iota(jnp.int32, (n, n), 0)
    side = jnp.where(turn < chips, core, 1 - core)
    which = 2 * lax.rem(turn, chips) + side
    split = jnp.where(lax.broadcasted_iota(jnp.int32, (n, n), 1) == which, 1.0, 0.0).astype(BF16)
    both = jnp.concatenate([got[:, :per].astype(BF16), asked.astype(BF16)], axis=1)
    both = jnp.dot(split, both, preferred_element_type=F32)
    most_asked = jnp.max(got[:, per:], axis=0, keepdims=True)
    dsend[:, : 2 * per] = both[chips:]
    dsend[:, 2 * per :] = jnp.broadcast_to(most_asked, (chips, EXTRA))
    share_asks.start()
    share_asks.wait_recv()
    counts = jnp.sum(both[:chips, per:] + drecv[:, per : 2 * per], axis=0, keepdims=True)
    counts_ref[...] = counts.astype(jnp.int32)
    probs = counts / total_tokens
    terms = jnp.where(
        counts > 0.5, probs * jnp.log(jnp.maximum(probs, 1.0 / total_tokens)), 0.0
    )
    entropy = jnp.sum(terms, axis=1, keepdims=True)
    flag = jnp.maximum(most_asked, drecv[:1, 2 * per :])
    spots_of = [both[:chips, :per].astype(jnp.int32), drecv[:, :per].astype(jnp.int32)]

    all_in(precv, chips - 1, psem_r)
    fetch_tokens.wait()
    packs = precv[...].reshape(chips * cap, width)
    direct = jnp.dot(sel[...], packs, preferred_element_type=F32)
    all_in(orecv, planes - 1, osem_r)
    packs = orecv[...].reshape(planes * spill, width)
    quant = (direct + jnp.dot(spill1h[...], packs, preferred_element_type=F32)).astype(BF16)
    quant_ref[...] = quant
    diff = tokens_ref[...].astype(F32) - quant.astype(F32)
    square = diff * diff
    folded = square[:, :128]
    for k in range(1, width // 128):
        folded = folded + square[:, k * 128 : (k + 1) * 128]
    tloss = jnp.sum(folded.T, axis=0, keepdims=True) / width
    tloss_ref[...] = tloss
    part = jnp.sum(tloss, axis=1, keepdims=True)

    first = tloss.astype(BF16).astype(F32)
    second = (tloss - first).astype(BF16).astype(F32)
    third = tloss - first - second
    own_chip = lax.shift_right_logical(hi_row, 1) == lax.broadcasted_iota(jnp.int32, (chips, rows), 0)
    spread = jnp.concatenate(
        [jnp.where(own_chip, x, 0.0).astype(BF16) for x in (first, second, third)], axis=0
    )
    sums = jnp.dot(spread, rank1h[...], preferred_element_type=F32)
    sums = sums[:chips] + sums[chips : 2 * chips] + sums[2 * chips :]
    lane1 = lax.broadcasted_iota(jnp.int32, (chips, EXTRA), 1)
    sums = jnp.where(lane1 == EXTRA - 2, part, jnp.where(lane1 == EXTRA - 1, entropy, sums))
    for q in range(chips):
        lsend[q] = sums[q : q + 1, :]
    lrecv[pl.ds(me, 1)] = lsend[pl.ds(me, 1)]
    for k, other in everyone:
        loss_put(k, other).start()

    all_out(csend, chips - 1, csem_s)
    all_out(hsend, chips - 1, hsem_s)
    all_out(psend, chips - 1, psem_s)
    all_out(gsend, planes - 1, gsem_s)
    all_out(osend, planes - 1, osem_s)
    share_book.wait_send()
    share_asks.wait_send()
    all_in(lrecv, n - 1, lsem_r)
    added = jnp.zeros((chips, per), F32)
    ends = jnp.zeros((1, EXTRA), F32)
    for other in (0, 1):
        back = lrecv[other * chips : (other + 1) * chips, 0, :]
        spot = spots_of[other]
        parts = [
            jnp.take_along_axis(back, jnp.maximum(spot[:, j : j + 128], 0), axis=1)
            for j in range(0, per, 128)
        ]
        added = added + jnp.where(spot >= 0, jnp.concatenate(parts, axis=1), 0.0)
        ends = ends + jnp.sum(back, axis=0, keepdims=True)
    closs_ref[...] = jnp.sum(added, axis=0, keepdims=True)
    lane1 = lane1[:1]
    perp = jnp.exp(-ends[:, EXTRA - 1 :])
    commit = ends[:, EXTRA - 2 : EXTRA - 1] * (0.25 / total_tokens)
    scal_ref[...] = jnp.where(lane1 == 0, commit, jnp.where(lane1 == 1, perp, flag))
    all_out(lrecv, n - 1, lsem_s)


def exchange(n, cols, cap, spill, wide_spill, number, tokens, codebook, codes):
    rows, width = tokens.shape
    per = codebook.shape[0]
    chips, planes = n // 2, n // cols
    vmem = pl.BlockSpec(memory_space=pltpu.VMEM)
    dma = pltpu.SemaphoreType.DMA
    return pl.pallas_call(
        functools.partial(kernel, n, cols, cap, spill, wide_spill),
        out_shape=(
            pltpu.VMEM((rows, width), BF16),
            pltpu.VMEM((1, rows), F32),
            pltpu.VMEM((1, per), jnp.int32),
            pltpu.VMEM((1, per), F32),
            pltpu.VMEM((1, EXTRA), F32),
        ),
        in_specs=[pl.BlockSpec(memory_space=pltpu.HBM)] * 3,
        out_specs=(vmem,) * 5,
        scratch_shapes=[
            pltpu.VMEM(codes.shape, jnp.int32),
            pltpu.VMEM((rows, width), BF16),
            pltpu.VMEM((2 * per, width), BF16),
            pltpu.VMEM((chips, 2, per + EXTRA), BF16),
            pltpu.VMEM((chips, 2, per + EXTRA), BF16),
            pltpu.VMEM((chips, 2, per), BF16),
            pltpu.VMEM((chips, 2, per), BF16),
            pltpu.VMEM((chips, cap, width), BF16),
            pltpu.VMEM((chips, cap, width), BF16),
            pltpu.VMEM((planes, cols // 2, spill, width), BF16),
            pltpu.VMEM((planes, cols // 2, spill, width), BF16),
            pltpu.VMEM((planes, spill, width), BF16),
            pltpu.VMEM((planes, spill, width), BF16),
            pltpu.VMEM((chips, 2 * per + EXTRA), F32),
            pltpu.VMEM((chips, 2 * per + EXTRA), F32),
            pltpu.VMEM((chips, 1, EXTRA), F32),
            pltpu.VMEM((n, 1, EXTRA), F32),
            pltpu.VMEM((rows, per), BF16),
            pltpu.VMEM((rows, chips * cap), BF16),
            pltpu.VMEM((rows, planes * spill), BF16),
            pltpu.VMEM((rows, 128), BF16),
            dma((3,)),
            dma, dma((planes,)), *[dma] * 4,
            dma, dma((planes,)), *[dma] * 4,
            dma((2,)), dma((2,)),
        ],
        compiler_params=pltpu.CompilerParams(collective_id=number, has_side_effects=True),
    )(*[pltpu.with_memory_space_constraint(x, pltpu.HBM) for x in (codes, tokens, codebook)])


def finish_kernel(
    quant_ref, tloss_ref, counts_ref, closs_ref, scal_ref,
    quant_out, tloss_out, counts_out, closs_out, commit_out, perp_out, flag_out,
    tloss, counts, closs, commit, perp, sem,
):
    whole = pltpu.make_async_copy(quant_ref, quant_out, sem.at[0])
    whole.start()
    tloss[...] = tloss_ref[...].reshape(tloss.shape)
    counts[...] = counts_ref[...].reshape(counts.shape)
    closs[...] = closs_ref[...].reshape(closs.shape)
    commit[...] = scal_ref[:, :1]
    perp[...] = scal_ref[:, 1:2]
    small = [(tloss, tloss_out), (counts, counts_out), (closs, closs_out), (commit, commit_out), (perp, perp_out)]
    small = [pltpu.make_async_copy(src, dst, sem.at[1 + i]) for i, (src, dst) in enumerate(small)]
    for one in small:
        one.start()
    flag_out[0, 0] = jnp.max(scal_ref[:, 2:3]).astype(jnp.int32)
    for one in small:
        one.wait()
    whole.wait()


def finish(quantized, token_loss, counts, code_loss, scalars):
    rows, per = token_loss.shape[1], counts.shape[1]
    vmem = pl.BlockSpec(memory_space=pltpu.VMEM)
    hbm = pl.BlockSpec(memory_space=pltpu.HBM)
    q, t, k, c, m, p, f = pl.pallas_call(
        finish_kernel,
        out_shape=(
            jax.ShapeDtypeStruct(quantized.shape, BF16),
            jax.ShapeDtypeStruct((rows,), F32),
            jax.ShapeDtypeStruct((per,), jnp.int32),
            jax.ShapeDtypeStruct((per,), F32),
            jax.ShapeDtypeStruct((1, 1), F32),
            jax.ShapeDtypeStruct((1, 1), F32),
            pltpu.SMEM((1, 1), jnp.int32),
        ),
        in_specs=[vmem] * 5,
        out_specs=(hbm,) * 6 + (pl.BlockSpec(memory_space=pltpu.SMEM),),
        scratch_shapes=[
            pltpu.VMEM((rows,), F32),
            pltpu.VMEM((per,), jnp.int32),
            pltpu.VMEM((per,), F32),
            pltpu.VMEM((1, 1), F32),
            pltpu.VMEM((1, 1), F32),
            pltpu.SemaphoreType.DMA((6,)),
        ],
        compiler_params=pltpu.CompilerParams(vmem_limit_bytes=4 << 20),
    )(quantized, token_loss, counts, code_loss, scalars)
    return q, t, k, c, m[0, 0], p[0, 0], f


def held(x):
    def body(src, dst, sem):
        copy = pltpu.make_async_copy(src, dst, sem)
        copy.start()
        copy.wait()

    return pl.pallas_call(
        body,
        out_shape=jax.ShapeDtypeStruct(x.shape, x.dtype),
        in_specs=[pl.BlockSpec(memory_space=pltpu.HBM)],
        out_specs=pl.BlockSpec(memory_space=pltpu.VMEM),
        scratch_shapes=[pltpu.SemaphoreType.DMA],
    )(pltpu.with_memory_space_constraint(x, pltpu.HBM))


def asked_plan(n, cols, cap, spill, tokens, codebook, codes):
    wide = spill * 2
    outs = exchange(n, cols, cap, spill, wide, 0, tokens, codebook, codes)

    *done, flag = finish(*outs)

    def kept():
        return tuple(done)

    def wider():
        return finish(*exchange(n, cols, 2 * cap, wide, wide, 1, tokens, codebook, codes))[:-1]

    def ringed():
        return ring_plan(n, held(tokens), held(codebook), held(codes))

    def any_codes():
        return lax.cond(flag[0, 0] > 1, ringed, wider)

    return lax.cond(flag[0, 0] > 0, any_codes, kept)


def on_device(n, cols, tokens, codebook, codes):
    rows, width = tokens.shape
    per = codebook.shape[0]
    cap = -(-rows // (n * 16)) * 16
    spill = cap * 3 // 4
    fits = (
        per % 128 == 0
        and per & (per - 1) == 0
        and rows % 128 == 0
        and width % 128 == 0
        and n // 2 * cap % 128 == 0
        and spill % 8 == 0
        and cols == 8
        and n == 4 * cols
        and n <= 128
        and 2 * cap + 2 * spill < EXTRA - 1
    )
    if fits:
        return asked_plan(n, cols, cap, spill, tokens, codebook, codes)
    return dense_plan(tokens, codebook, codes)


def solution(mesh):
    n = mesh.shape["row"] * mesh.shape["col"]
    return jax.shard_map(
        functools.partial(on_device, n, mesh.shape["col"]),
        mesh=mesh,
        in_specs=(P(AXES, None), P(AXES, None), P(AXES)),
        out_specs=(P(AXES, None), P(AXES), P(AXES), P(AXES), P(), P()),
        check_vma=False,
    )
```

```python
import functools

import jax
import jax.numpy as jnp
from jax import lax
from jax.experimental import pallas as pl
from jax.experimental.pallas import tpu as pltpu
from jax.sharding import PartitionSpec as P

AXES = ("row", "col")
EXTRA = 128
ASK_ORDER = (3, 2, 1, 0)
REPLY_ORDER = (2, 3, 1, 0)
F32 = jnp.float32
BF16 = jnp.bfloat16


def dense_plan(tokens, codebook, codes):
    tok_rows = tokens.shape[0]
    width = tokens.shape[1]
    per_dev = codebook.shape[0]
    devices = lax.axis_size("row") * lax.axis_size("col")
    total_codes = per_dev * devices
    total_tokens = tok_rows * devices
    full_book = lax.all_gather(codebook, AXES, axis=0, tiled=True)
    quantized = jnp.take(full_book, codes, axis=0)
    diff = tokens.astype(F32) - quantized.astype(F32)
    token_loss = jnp.sum(diff * diff, axis=1) / width
    loss_part = jnp.sum(token_loss)
    local_counts = jax.ops.segment_sum(
        jnp.ones((tok_rows,), F32), codes, num_segments=total_codes
    )
    local_loss = jax.ops.segment_sum(token_loss, codes, num_segments=total_codes)
    floor_prob = jnp.float32(1.0 / total_tokens)
    totals, loss_totals = lax.psum((local_counts, local_loss), AXES)
    loss_sum = lax.psum(loss_part, AXES)
    probs = totals / total_tokens
    terms = jnp.where(
        totals > 0.5, probs * jnp.log(jnp.maximum(probs, floor_prob)), jnp.float32(0.0)
    )
    offset = lax.axis_index(AXES) * per_dev
    owned_counts = lax.dynamic_slice_in_dim(totals, offset, per_dev, 0)
    code_loss = lax.dynamic_slice_in_dim(loss_totals, offset, per_dev, 0)
    commitment = 0.25 * loss_sum / total_tokens
    return (
        quantized,
        token_loss,
        owned_counts.astype(jnp.int32),
        code_loss,
        commitment,
        jnp.exp(-jnp.sum(terms)),
    )


def ring_plan(n, tokens, codebook, codes):
    rows, width = tokens.shape
    per_dev = codebook.shape[0]
    me = lax.axis_index(AXES)
    ring = [(i, (i + 1) % n) for i in range(n)]
    hi = codes // per_dev
    lo = codes % per_dev

    def pick(step, carry):
        block, got = carry
        owner = lax.rem(me - step + n, n)
        got = jnp.where((hi == owner)[:, None], jnp.take(block, lo, axis=0), got)
        return lax.ppermute(block, AXES, ring), got

    _, quantized = lax.fori_loop(0, n, pick, (codebook, jnp.zeros_like(tokens)))
    diff = tokens.astype(F32) - quantized.astype(F32)
    token_loss = jnp.sum(diff * diff, axis=1) / width

    def add(step, carry):
        c, t, total, hits, parts = carry
        owner = lax.rem(me - step + n, n)
        mine = (c // per_dev) == me
        total = total + jax.ops.segment_sum(
            jnp.where(mine, t, 0.0), c % per_dev, num_segments=per_dev
        )
        hits = hits + jax.ops.segment_sum(
            mine.astype(jnp.int32), c % per_dev, num_segments=per_dev
        )
        parts = lax.dynamic_update_slice(parts, jnp.sum(t)[None], (owner,))
        return lax.ppermute(c, AXES, ring), lax.ppermute(t, AXES, ring), total, hits, parts

    start = (
        codes, token_loss, jnp.zeros((per_dev,), F32),
        jnp.zeros((per_dev,), jnp.int32), jnp.zeros((n,), F32),
    )
    _, _, code_loss, counts, parts = lax.fori_loop(0, n, add, start)
    probs = counts.astype(F32) / (rows * n)
    floor_prob = jnp.float32(1.0 / (rows * n))
    terms = jnp.where(counts > 0, probs * jnp.log(jnp.maximum(probs, floor_prob)), 0.0)

    def collect(step, carry):
        entropy, parts = carry
        owner = lax.rem(me - step + n, n)
        parts = lax.dynamic_update_slice(parts, entropy, (owner,))
        return lax.ppermute(entropy, AXES, ring), parts

    _, entropies = lax.fori_loop(0, n, collect, (jnp.sum(terms)[None], jnp.zeros((n,), F32)))
    commitment = 0.25 * jnp.sum(parts) / (rows * n)
    return quantized, token_loss, counts, code_loss, commitment, jnp.exp(-jnp.sum(entropies))


def kernel(
    n, cols, cap, spill, wide_spill,
    codes_hbm, tokens_hbm, book_hbm,
    quant_ref, tloss_ref, counts_ref, closs_ref, scal_ref,
    codes_ref, tokens_ref, book_ref, csend, crecv, hsend, hrecv, psend, precv, gsend, grecv, osend, orecv,
    dsend, drecv, lsend, lrecv, low1h, sel, spill1h, rank1h, direct,
    in_sem, csem_s, csem_r, hsem_s, hsem_r, psem_s, psem_r,
    gsem_s, gsem_r, osem_s, osem_r, lsem_s, lsem_r, bsem, dsem,
):
    rows, width = tokens_hbm.shape
    per = book_hbm.shape[0]
    bits = per.bit_length() - 1
    total_tokens = rows * n
    chips, half = n // 2, cols // 2
    my_row, my_col = lax.axis_index("row"), lax.axis_index("col")
    core = lax.rem(my_col, 2)
    my_chip = lax.div(my_col, 2)
    me = my_row * half + my_chip
    inner = lax.rem(lax.div(my_row + 1, 2), 2)
    beside, across = my_row + 1 - 2 * lax.rem(my_row, 2), 3 - my_row
    near = inner * across + (1 - inner) * beside
    far = inner * beside + (1 - inner) * across
    rows_at = [my_row, near, lax.rem(my_row + 2, 4), far]
    chips_at = [
        my_chip, my_chip + 1 - 2 * lax.rem(my_chip, 2), lax.rem(my_chip + 2, 4), 3 - my_chip
    ]
    spots = [(rows_at[k // half], chips_at[k % half]) for k in range(chips)]
    at = [(r, 2 * c + core) for r, c in spots]
    mirror = [(r, 2 * c + 1 - core) for r, c in spots]
    peer = [r * half + c for r, c in spots]
    fetch_codes = pltpu.make_async_copy(codes_hbm, codes_ref, in_sem.at[0])
    own_book = book_ref.at[pl.ds(pl.multiple_of(core * per, per), per)]
    fetch_book = pltpu.make_async_copy(book_hbm, own_book, in_sem.at[1])
    fetch_tokens = pltpu.make_async_copy(tokens_hbm, tokens_ref, in_sem.at[2])
    fetch_codes.start()

    def remote(src, dst, ssem, rsem, to):
        return pltpu.make_async_remote_copy(
            src_ref=src,
            dst_ref=dst,
            send_sem=ssem,
            recv_sem=rsem,
            device_id=to,
            device_id_type=pl.DeviceIdType.MESH,
        )

    def put(send, recv, ssem, rsem, k):
        return remote(send.at[peer[k]], recv.at[me], ssem, rsem, at[k])

    def spill_put(d, c):
        r, to = rows_at[d], chips_at[c]
        return remote(gsend.at[r, to], grecv.at[r, my_chip], gsem_s, gsem_r.at[r], at[c])

    def joint_put(d):
        return remote(osend.at[rows_at[d]], orecv.at[my_row], osem_s, osem_r, at[d * half])

    def loss_put(k, other):
        to = mirror[k] if other else at[k]
        return remote(lsend.at[peer[k]], lrecv.at[other * chips + me], lsem_s, lsem_r, to)

    def all_in(ref, count, sem):
        part = ref.at[pl.ds(0, count)]
        remote(part, part, sem, sem, mirror[0]).wait_recv()

    def all_out(ref, count, sem):
        part = ref.at[pl.ds(0, count)]
        remote(part, part, sem, sem, mirror[0]).wait_send()

    ask_refs = (csend, crecv, csem_s, csem_r.at[my_row])
    count_refs = (hsend, hrecv, hsem_s, hsem_r)
    reply_refs = (psend, precv, psem_s, psem_r)
    partners = [k for d in ASK_ORDER for k in range(d * half, d * half + half) if k]
    everyone = [(k, other) for d in ASK_ORDER for k in range(d * half, d * half + half)
                for other in (0, 1) if k or other]
    share_book = remote(own_book, own_book, bsem.at[0], bsem.at[1], mirror[0])
    share_asks = remote(dsend, drecv, dsem.at[0], dsem.at[1], mirror[0])

    barrier = pltpu.get_barrier_semaphore()
    for k, other in everyone:
        pl.semaphore_signal(
            barrier, inc=1, device_id=mirror[k] if other else at[k],
            device_id_type=pl.DeviceIdType.MESH,
        )
    fetch_book.start()
    fetch_tokens.start()

    fetch_codes.wait()
    code_row = codes_ref[...].reshape(1, rows)
    hi_row = lax.shift_right_logical(code_row, bits)
    code_col = jnp.broadcast_to(code_row.astype(F32), (128, rows)).T.astype(jnp.int32)
    hi_col = lax.shift_right_logical(code_col, bits)
    lo_col = code_col & (per - 1)
    lane = lax.broadcasted_iota(jnp.int32, (rows, 128), 1)
    own_row = hi_row == lax.broadcasted_iota(jnp.int32, (n, rows), 0)
    for k in range(per // 128):
        low1h[:, k * 128 : (k + 1) * 128] = jnp.where(lo_col == lane + k * 128, 1.0, 0.0).astype(BF16)
    low = low1h[...]
    hist = jnp.dot(jnp.where(own_row, 1.0, 0.0).astype(BF16), low, preferred_element_type=F32)
    odd = (lax.broadcasted_iota(jnp.int32, (n, 128), 0) & 1) == 1

    def first_half(found):
        total = jnp.broadcast_to(jnp.sum(found, axis=1, keepdims=True), (n, 128))
        return total, jnp.where(odd, pltpu.roll(total, 1, 0), 0.0)

    wanted = jnp.where(hist > 0.5, 1.0, 0.0)
    total, ahead = first_half(wanted)
    both = total + ahead
    over = [jnp.where(odd, jnp.maximum(both - float(c), 0.0), 0.0) for c in (cap, 2 * cap)]
    over = jnp.minimum(jnp.concatenate(over, axis=1), 256.0).astype(BF16)
    line = lax.broadcasted_iota(jnp.int32, (2 * n, n), 0)
    source = lax.broadcasted_iota(jnp.int32, (2 * n, n), 1)
    line_of = lax.rem(line, n)
    same = lax.div(line_of, cols) == lax.div(source, cols)
    earlier = lax.div(source, 2) < lax.div(line_of, 2)
    reach = jnp.where(same & (earlier | (line >= n)), 1.0, 0.0).astype(BF16)
    over = jnp.dot(reach, over, preferred_element_type=F32)
    behind = over[:n, :1]
    worst = jnp.max(over[n:], axis=0, keepdims=True)
    heavy = jnp.max(jnp.max(hist, axis=0, keepdims=True), axis=1, keepdims=True) > 256.0
    most = jnp.where(worst[:, EXTRA:] > float(wide_spill), 2.0, 1.0)
    most = jnp.where(worst[:, :EXTRA] > float(spill), most, 0.0)
    most = jnp.where(heavy, 2.0, most)
    most_pair = jnp.broadcast_to(most, (2, EXTRA)).astype(BF16)
    before = lax.broadcasted_iota(jnp.int32, (per, per), 0) < lax.broadcasted_iota(jnp.int32, (per, per), 1)
    before = jnp.where(before, 1.0, 0.0).astype(BF16)
    rank = jnp.dot(wanted.astype(BF16), before, preferred_element_type=F32) + ahead[:, :1]
    rank = jnp.minimum(rank + jnp.where(rank > cap - 0.5, behind, 0.0), 255.0)
    order = jnp.where(wanted > 0.5, rank, -1.0).astype(BF16)
    for q in range(chips):
        csend[q, :, :per] = order[2 * q : 2 * q + 2, :]
        csend[q, :, per:] = most_pair
    crecv[pl.ds(me, 1)] = csend[pl.ds(me, 1)]

    pl.semaphore_wait(barrier, n - 1)
    for k in partners:
        put(*ask_refs, k).start()
    hist16 = jnp.minimum(hist, 256.0).astype(BF16)
    for q in range(chips):
        hsend[q] = hist16[2 * q : 2 * q + 2, :]
    hrecv[pl.ds(me, 1)] = hsend[pl.ds(me, 1)]
    fetch_book.wait()
    share_book.start()
    for k in partners:
        put(*count_refs, k).start()

    rank = rank.astype(BF16)
    hi1h = jnp.where(hi_col[:, :n] == lane[:, :n], 1.0, 0.0).astype(BF16)
    looked = jnp.dot(hi1h, rank, preferred_element_type=F32).astype(BF16) * low
    found = jnp.dot(looked, jnp.ones((per, 128), BF16), preferred_element_type=F32)
    found = found.astype(jnp.int32)
    rank1h[...] = jnp.where(found == lane, 1.0, 0.0).astype(BF16)
    chip_col = lax.shift_right_logical(hi_col, 1)
    slot = jnp.where(found < cap, chip_col * cap + found, -1)
    for k in range(chips * cap // 128):
        sel[:, k * 128 : (k + 1) * 128] = jnp.where(slot == lane + k * 128, 1.0, 0.0).astype(BF16)
    slot = jnp.where(found < cap, -1, lax.div(chip_col, half) * spill + (found - cap))
    planes = chips // half
    for k in range(0, planes * spill, 128):
        wide = min(128, planes * spill - k)
        spill1h[:, k : k + wide] = jnp.where(slot == lane + k, 1.0, 0.0).astype(BF16)[:, :wide]

    both_caps = cap + -(-spill // 16) * 16
    place = lax.broadcasted_iota(jnp.int32, (both_caps, per), 0).astype(F32).astype(BF16)
    one, none = jnp.ones((), BF16), jnp.zeros((), BF16)
    for i, d in enumerate(REPLY_ORDER):
        group = range(d * half, d * half + half)
        all_in(crecv, half if d else half - 1, csem_r.at[rows_at[d]])
        if i == 0:
            share_book.wait_recv()
        picks = []
        for k in group:
            pair = crecv[peer[k]][:, :per].astype(F32)
            picks.append(jnp.concatenate(
                [
                    jnp.where(jnp.broadcast_to(pair[h : h + 1], (both_caps, per)).astype(BF16) == place, one, none)
                    for h in (0, 1)
                ],
                axis=1,
            ))
        packed = jnp.dot(jnp.concatenate(picks, axis=0), book_ref[...], preferred_element_type=F32)
        packed = packed.astype(BF16)
        for j, k in enumerate(group):
            out = psend if k else precv
            start = j * both_caps
            out[peer[k]] = packed[start : start + cap]
            if j:
                gsend[rows_at[d], chips_at[j]] = packed[start + cap : start + cap + spill]
            else:
                grecv[rows_at[d], my_chip] = packed[start + cap : start + cap + spill]
        for c in range(1, half):
            spill_put(d, c).start()
        for k in group:
            if k:
                put(*reply_refs, k).start()

    for d in REPLY_ORDER:
        all_in(grecv.at[0], half - 1, gsem_r.at[rows_at[d]])
        joint = grecv[rows_at[d], 0].astype(F32)
        for c in range(1, half):
            joint = joint + grecv[rows_at[d], c].astype(F32)
        if d:
            osend[rows_at[d]] = joint.astype(BF16)
            joint_put(d).start()
        else:
            orecv[my_row] = joint.astype(BF16)

    all_in(hrecv, chips - 1, hsem_r)
    got = jnp.concatenate([crecv[q].astype(F32) for q in range(chips)], axis=0)
    asked = jnp.concatenate([hrecv[q].astype(F32) for q in range(chips)], axis=0)
    turn = lax.broadcasted_iota(jnp.int32, (n, n), 0)
    side = jnp.where(turn < chips, core, 1 - core)
    which = 2 * lax.rem(turn, chips) + side
    split = jnp.where(lax.broadcasted_iota(jnp.int32, (n, n), 1) == which, 1.0, 0.0).astype(BF16)
    both = jnp.concatenate([got[:, :per].astype(BF16), asked.astype(BF16)], axis=1)
    both = jnp.dot(split, both, preferred_element_type=F32)
    most_asked = jnp.max(got[:, per:], axis=0, keepdims=True)
    dsend[:, : 2 * per] = both[chips:]
    dsend[:, 2 * per :] = jnp.broadcast_to(most_asked, (chips, EXTRA))
    share_asks.start()
    share_asks.wait_recv()
    counts = jnp.sum(both[:chips, per:] + drecv[:, per : 2 * per], axis=0, keepdims=True)
    counts_ref[...] = counts.astype(jnp.int32)
    probs = counts / total_tokens
    terms = jnp.where(
        counts > 0.5, probs * jnp.log(jnp.maximum(probs, 1.0 / total_tokens)), 0.0
    )
    entropy = jnp.sum(terms, axis=1, keepdims=True)
    flag = jnp.maximum(most_asked, drecv[:1, 2 * per :])
    spots_of = [both[:chips, :per].astype(jnp.int32), drecv[:, :per].astype(jnp.int32)]

    all_in(precv, chips - 1, psem_r)
    fetch_tokens.wait()
    packs = precv[...].reshape(chips * cap, width)
    direct[...] = jnp.dot(sel[...], packs, preferred_element_type=F32)
    all_in(orecv, planes - 1, osem_r)
    packs = orecv[...].reshape(planes * spill, width)
    quant = (direct[...] + jnp.dot(spill1h[...], packs, preferred_element_type=F32)).astype(BF16)
    quant_ref[...] = quant
    diff = tokens_ref[...].astype(F32) - quant.astype(F32)
    square = diff * diff
    folded = square[:, :128]
    for k in range(1, width // 128):
        folded = folded + square[:, k * 128 : (k + 1) * 128]
    tloss = jnp.sum(folded.T, axis=0, keepdims=True) / width
    tloss_ref[...] = tloss
    part = jnp.sum(tloss, axis=1, keepdims=True)

    first = tloss.astype(BF16).astype(F32)
    second = (tloss - first).astype(BF16).astype(F32)
    third = tloss - first - second
    own_chip = lax.shift_right_logical(hi_row, 1) == lax.broadcasted_iota(jnp.int32, (chips, rows), 0)
    spread = jnp.concatenate(
        [jnp.where(own_chip, x, 0.0).astype(BF16) for x in (first, second, third)], axis=0
    )
    sums = jnp.dot(spread, rank1h[...], preferred_element_type=F32)
    sums = sums[:chips] + sums[chips : 2 * chips] + sums[2 * chips :]
    lane1 = lax.broadcasted_iota(jnp.int32, (chips, EXTRA), 1)
    sums = jnp.where(lane1 == EXTRA - 2, part, jnp.where(lane1 == EXTRA - 1, entropy, sums))
    for q in range(chips):
        lsend[q] = sums[q : q + 1, :]
    lrecv[pl.ds(me, 1)] = lsend[pl.ds(me, 1)]
    for k, other in everyone:
        loss_put(k, other).start()

    all_out(csend, chips - 1, csem_s)
    all_out(hsend, chips - 1, hsem_s)
    all_out(psend, chips - 1, psem_s)
    all_out(gsend, planes - 1, gsem_s)
    all_out(osend, planes - 1, osem_s)
    share_book.wait_send()
    share_asks.wait_send()
    all_in(lrecv, n - 1, lsem_r)
    added = jnp.zeros((chips, per), F32)
    ends = jnp.zeros((1, EXTRA), F32)
    for other in (0, 1):
        back = lrecv[other * chips : (other + 1) * chips, 0, :]
        spot = spots_of[other]
        parts = [
            jnp.take_along_axis(back, jnp.maximum(spot[:, j : j + 128], 0), axis=1)
            for j in range(0, per, 128)
        ]
        added = added + jnp.where(spot >= 0, jnp.concatenate(parts, axis=1), 0.0)
        ends = ends + jnp.sum(back, axis=0, keepdims=True)
    closs_ref[...] = jnp.sum(added, axis=0, keepdims=True)
    lane1 = lane1[:1]
    perp = jnp.exp(-ends[:, EXTRA - 1 :])
    commit = ends[:, EXTRA - 2 : EXTRA - 1] * (0.25 / total_tokens)
    scal_ref[...] = jnp.where(lane1 == 0, commit, jnp.where(lane1 == 1, perp, flag))
    all_out(lrecv, n - 1, lsem_s)


def exchange(n, cols, cap, spill, wide_spill, number, tokens, codebook, codes):
    rows, width = tokens.shape
    per = codebook.shape[0]
    chips, planes = n // 2, n // cols
    vmem = pl.BlockSpec(memory_space=pltpu.VMEM)
    dma = pltpu.SemaphoreType.DMA
    return pl.pallas_call(
        functools.partial(kernel, n, cols, cap, spill, wide_spill),
        out_shape=(
            pltpu.VMEM((rows, width), BF16),
            pltpu.VMEM((1, rows), F32),
            pltpu.VMEM((1, per), jnp.int32),
            pltpu.VMEM((1, per), F32),
            pltpu.VMEM((1, EXTRA), F32),
        ),
        in_specs=[pl.BlockSpec(memory_space=pltpu.HBM)] * 3,
        out_specs=(vmem,) * 5,
        scratch_shapes=[
            pltpu.VMEM(codes.shape, jnp.int32),
            pltpu.VMEM((rows, width), BF16),
            pltpu.VMEM((2 * per, width), BF16),
            pltpu.VMEM((chips, 2, per + EXTRA), BF16),
            pltpu.VMEM((chips, 2, per + EXTRA), BF16),
            pltpu.VMEM((chips, 2, per), BF16),
            pltpu.VMEM((chips, 2, per), BF16),
            pltpu.VMEM((chips, cap, width), BF16),
            pltpu.VMEM((chips, cap, width), BF16),
            pltpu.VMEM((planes, cols // 2, spill, width), BF16),
            pltpu.VMEM((planes, cols // 2, spill, width), BF16),
            pltpu.VMEM((planes, spill, width), BF16),
            pltpu.VMEM((planes, spill, width), BF16),
            pltpu.VMEM((chips, 2 * per + EXTRA), F32),
            pltpu.VMEM((chips, 2 * per + EXTRA), F32),
            pltpu.VMEM((chips, 1, EXTRA), F32),
            pltpu.VMEM((n, 1, EXTRA), F32),
            pltpu.VMEM((rows, per), BF16),
            pltpu.VMEM((rows, chips * cap), BF16),
            pltpu.VMEM((rows, planes * spill), BF16),
            pltpu.VMEM((rows, 128), BF16),
            pltpu.VMEM((rows, width), F32),
            dma((3,)),
            dma, dma((planes,)), *[dma] * 4,
            dma, dma((planes,)), *[dma] * 4,
            dma((2,)), dma((2,)),
        ],
        compiler_params=pltpu.CompilerParams(collective_id=number, has_side_effects=True),
    )(*[pltpu.with_memory_space_constraint(x, pltpu.HBM) for x in (codes, tokens, codebook)])


def finish_kernel(
    quant_ref, tloss_ref, counts_ref, closs_ref, scal_ref,
    quant_out, tloss_out, counts_out, closs_out, commit_out, perp_out, flag_out,
    tloss, counts, closs, commit, perp, sem,
):
    whole = pltpu.make_async_copy(quant_ref, quant_out, sem.at[0])
    whole.start()
    tloss[...] = tloss_ref[...].reshape(tloss.shape)
    counts[...] = counts_ref[...].reshape(counts.shape)
    closs[...] = closs_ref[...].reshape(closs.shape)
    commit[...] = scal_ref[:, :1]
    perp[...] = scal_ref[:, 1:2]
    small = [(tloss, tloss_out), (counts, counts_out), (closs, closs_out), (commit, commit_out), (perp, perp_out)]
    small = [pltpu.make_async_copy(src, dst, sem.at[1 + i]) for i, (src, dst) in enumerate(small)]
    for one in small:
        one.start()
    flag_out[0, 0] = jnp.max(scal_ref[:, 2:3]).astype(jnp.int32)
    for one in small:
        one.wait()
    whole.wait()


def finish(quantized, token_loss, counts, code_loss, scalars):
    rows, per = token_loss.shape[1], counts.shape[1]
    vmem = pl.BlockSpec(memory_space=pltpu.VMEM)
    hbm = pl.BlockSpec(memory_space=pltpu.HBM)
    q, t, k, c, m, p, f = pl.pallas_call(
        finish_kernel,
        out_shape=(
            jax.ShapeDtypeStruct(quantized.shape, BF16),
            jax.ShapeDtypeStruct((rows,), F32),
            jax.ShapeDtypeStruct((per,), jnp.int32),
            jax.ShapeDtypeStruct((per,), F32),
            jax.ShapeDtypeStruct((1, 1), F32),
            jax.ShapeDtypeStruct((1, 1), F32),
            pltpu.SMEM((1, 1), jnp.int32),
        ),
        in_specs=[vmem] * 5,
        out_specs=(hbm,) * 6 + (pl.BlockSpec(memory_space=pltpu.SMEM),),
        scratch_shapes=[
            pltpu.VMEM((rows,), F32),
            pltpu.VMEM((per,), jnp.int32),
            pltpu.VMEM((per,), F32),
            pltpu.VMEM((1, 1), F32),
            pltpu.VMEM((1, 1), F32),
            pltpu.SemaphoreType.DMA((6,)),
        ],
        compiler_params=pltpu.CompilerParams(vmem_limit_bytes=4 << 20),
    )(quantized, token_loss, counts, code_loss, scalars)
    return q, t, k, c, m[0, 0], p[0, 0], f


def held(x):
    def body(src, dst, sem):
        copy = pltpu.make_async_copy(src, dst, sem)
        copy.start()
        copy.wait()

    return pl.pallas_call(
        body,
        out_shape=jax.ShapeDtypeStruct(x.shape, x.dtype),
        in_specs=[pl.BlockSpec(memory_space=pltpu.HBM)],
        out_specs=pl.BlockSpec(memory_space=pltpu.VMEM),
        scratch_shapes=[pltpu.SemaphoreType.DMA],
    )(pltpu.with_memory_space_constraint(x, pltpu.HBM))


def asked_plan(n, cols, cap, spill, tokens, codebook, codes):
    wide = spill * 2
    outs = exchange(n, cols, cap, spill, wide, 0, tokens, codebook, codes)

    *done, flag = finish(*outs)

    def kept():
        return tuple(done)

    def wider():
        return finish(*exchange(n, cols, 2 * cap, wide, wide, 1, tokens, codebook, codes))[:-1]

    def ringed():
        return ring_plan(n, held(tokens), held(codebook), held(codes))

    def any_codes():
        return lax.cond(flag[0, 0] > 1, ringed, wider)

    return lax.cond(flag[0, 0] > 0, any_codes, kept)


def on_device(n, cols, tokens, codebook, codes):
    rows, width = tokens.shape
    per = codebook.shape[0]
    cap = -(-rows // (n * 16)) * 16
    spill = cap * 3 // 4
    fits = (
        per % 128 == 0
        and per & (per - 1) == 0
        and rows % 128 == 0
        and width % 128 == 0
        and n // 2 * cap % 128 == 0
        and spill % 8 == 0
        and cols == 8
        and n == 4 * cols
        and n <= 128
        and 2 * cap + 2 * spill < EXTRA - 1
    )
    if fits:
        return asked_plan(n, cols, cap, spill, tokens, codebook, codes)
    return dense_plan(tokens, codebook, codes)


def solution(mesh):
    n = mesh.shape["row"] * mesh.shape["col"]
    return jax.shard_map(
        functools.partial(on_device, n, mesh.shape["col"]),
        mesh=mesh,
        in_specs=(P(AXES, None), P(AXES, None), P(AXES)),
        out_specs=(P(AXES, None), P(AXES), P(AXES), P(AXES), P(), P()),
        check_vma=False,
    )
```

```python
import functools

import jax
import jax.numpy as jnp
from jax import lax
from jax.experimental import pallas as pl
from jax.experimental.pallas import tpu as pltpu
from jax.sharding import PartitionSpec as P

AXES = ("row", "col")
EXTRA = 128
ASK_ORDER = (2, 3, 1, 0)
REPLY_ORDER = (2, 3, 1, 0)
F32 = jnp.float32
BF16 = jnp.bfloat16


def dense_plan(tokens, codebook, codes):
    tok_rows = tokens.shape[0]
    width = tokens.shape[1]
    per_dev = codebook.shape[0]
    devices = lax.axis_size("row") * lax.axis_size("col")
    total_codes = per_dev * devices
    total_tokens = tok_rows * devices
    full_book = lax.all_gather(codebook, AXES, axis=0, tiled=True)
    quantized = jnp.take(full_book, codes, axis=0)
    diff = tokens.astype(F32) - quantized.astype(F32)
    token_loss = jnp.sum(diff * diff, axis=1) / width
    loss_part = jnp.sum(token_loss)
    local_counts = jax.ops.segment_sum(
        jnp.ones((tok_rows,), F32), codes, num_segments=total_codes
    )
    local_loss = jax.ops.segment_sum(token_loss, codes, num_segments=total_codes)
    floor_prob = jnp.float32(1.0 / total_tokens)
    totals, loss_totals = lax.psum((local_counts, local_loss), AXES)
    loss_sum = lax.psum(loss_part, AXES)
    probs = totals / total_tokens
    terms = jnp.where(
        totals > 0.5, probs * jnp.log(jnp.maximum(probs, floor_prob)), jnp.float32(0.0)
    )
    offset = lax.axis_index(AXES) * per_dev
    owned_counts = lax.dynamic_slice_in_dim(totals, offset, per_dev, 0)
    code_loss = lax.dynamic_slice_in_dim(loss_totals, offset, per_dev, 0)
    commitment = 0.25 * loss_sum / total_tokens
    return (
        quantized,
        token_loss,
        owned_counts.astype(jnp.int32),
        code_loss,
        commitment,
        jnp.exp(-jnp.sum(terms)),
    )


def ring_plan(n, tokens, codebook, codes):
    rows, width = tokens.shape
    per_dev = codebook.shape[0]
    me = lax.axis_index(AXES)
    ring = [(i, (i + 1) % n) for i in range(n)]
    hi = codes // per_dev
    lo = codes % per_dev

    def pick(step, carry):
        block, got = carry
        owner = lax.rem(me - step + n, n)
        got = jnp.where((hi == owner)[:, None], jnp.take(block, lo, axis=0), got)
        return lax.ppermute(block, AXES, ring), got

    _, quantized = lax.fori_loop(0, n, pick, (codebook, jnp.zeros_like(tokens)))
    diff = tokens.astype(F32) - quantized.astype(F32)
    token_loss = jnp.sum(diff * diff, axis=1) / width

    def add(step, carry):
        c, t, total, hits, parts = carry
        owner = lax.rem(me - step + n, n)
        mine = (c // per_dev) == me
        total = total + jax.ops.segment_sum(
            jnp.where(mine, t, 0.0), c % per_dev, num_segments=per_dev
        )
        hits = hits + jax.ops.segment_sum(
            mine.astype(jnp.int32), c % per_dev, num_segments=per_dev
        )
        parts = lax.dynamic_update_slice(parts, jnp.sum(t)[None], (owner,))
        return lax.ppermute(c, AXES, ring), lax.ppermute(t, AXES, ring), total, hits, parts

    start = (
        codes, token_loss, jnp.zeros((per_dev,), F32),
        jnp.zeros((per_dev,), jnp.int32), jnp.zeros((n,), F32),
    )
    _, _, code_loss, counts, parts = lax.fori_loop(0, n, add, start)
    probs = counts.astype(F32) / (rows * n)
    floor_prob = jnp.float32(1.0 / (rows * n))
    terms = jnp.where(counts > 0, probs * jnp.log(jnp.maximum(probs, floor_prob)), 0.0)

    def collect(step, carry):
        entropy, parts = carry
        owner = lax.rem(me - step + n, n)
        parts = lax.dynamic_update_slice(parts, entropy, (owner,))
        return lax.ppermute(entropy, AXES, ring), parts

    _, entropies = lax.fori_loop(0, n, collect, (jnp.sum(terms)[None], jnp.zeros((n,), F32)))
    commitment = 0.25 * jnp.sum(parts) / (rows * n)
    return quantized, token_loss, counts, code_loss, commitment, jnp.exp(-jnp.sum(entropies))


def kernel(
    n, cols, cap, spill, wide_spill,
    codes_hbm, tokens_hbm, book_hbm,
    quant_ref, tloss_ref, counts_ref, closs_ref, scal_ref,
    codes_ref, tokens_ref, book_ref, csend, crecv, hsend, hrecv, psend, precv, gsend, grecv, osend, orecv,
    dsend, drecv, lsend, lrecv, low1h, sel, spill1h, rank1h, direct,
    in_sem, csem_s, csem_r, hsem_s, hsem_r, psem_s, psem_r,
    gsem_s, gsem_r, osem_s, osem_r, lsem_s, lsem_r, bsem, dsem,
):
    rows, width = tokens_hbm.shape
    per = book_hbm.shape[0]
    bits = per.bit_length() - 1
    total_tokens = rows * n
    chips, half = n // 2, cols // 2
    my_row, my_col = lax.axis_index("row"), lax.axis_index("col")
    core = lax.rem(my_col, 2)
    my_chip = lax.div(my_col, 2)
    me = my_row * half + my_chip
    inner = lax.rem(lax.div(my_row + 1, 2), 2)
    beside, across = my_row + 1 - 2 * lax.rem(my_row, 2), 3 - my_row
    near = inner * across + (1 - inner) * beside
    far = inner * beside + (1 - inner) * across
    rows_at = [my_row, near, lax.rem(my_row + 2, 4), far]
    chips_at = [
        my_chip, my_chip + 1 - 2 * lax.rem(my_chip, 2), lax.rem(my_chip + 2, 4), 3 - my_chip
    ]
    spots = [(rows_at[k // half], chips_at[k % half]) for k in range(chips)]
    at = [(r, 2 * c + core) for r, c in spots]
    mirror = [(r, 2 * c + 1 - core) for r, c in spots]
    peer = [r * half + c for r, c in spots]
    fetch_codes = pltpu.make_async_copy(codes_hbm, codes_ref, in_sem.at[0])
    own_book = book_ref.at[pl.ds(pl.multiple_of(core * per, per), per)]
    fetch_book = pltpu.make_async_copy(book_hbm, own_book, in_sem.at[1])
    fetch_tokens = pltpu.make_async_copy(tokens_hbm, tokens_ref, in_sem.at[2])
    fetch_codes.start()

    def remote(src, dst, ssem, rsem, to):
        return pltpu.make_async_remote_copy(
            src_ref=src,
            dst_ref=dst,
            send_sem=ssem,
            recv_sem=rsem,
            device_id=to,
            device_id_type=pl.DeviceIdType.MESH,
        )

    def put(send, recv, ssem, rsem, k):
        return remote(send.at[peer[k]], recv.at[me], ssem, rsem, at[k])

    def spill_put(d, c):
        r, to = rows_at[d], chips_at[c]
        return remote(gsend.at[r, to], grecv.at[r, my_chip], gsem_s, gsem_r.at[r], at[c])

    def joint_put(d):
        return remote(osend.at[rows_at[d]], orecv.at[my_row], osem_s, osem_r, at[d * half])

    def loss_put(k, other):
        to = mirror[k] if other else at[k]
        return remote(lsend.at[peer[k]], lrecv.at[other * chips + me], lsem_s, lsem_r, to)

    def all_in(ref, count, sem):
        part = ref.at[pl.ds(0, count)]
        remote(part, part, sem, sem, mirror[0]).wait_recv()

    def all_out(ref, count, sem):
        part = ref.at[pl.ds(0, count)]
        remote(part, part, sem, sem, mirror[0]).wait_send()

    ask_refs = (csend, crecv, csem_s, csem_r.at[my_row])
    count_refs = (hsend, hrecv, hsem_s, hsem_r)
    reply_refs = (psend, precv, psem_s, psem_r)
    partners = [k for d in ASK_ORDER for k in range(d * half, d * half + half) if k]
    everyone = [(k, other) for d in ASK_ORDER for k in range(d * half, d * half + half)
                for other in (0, 1) if k or other]
    share_book = remote(own_book, own_book, bsem.at[0], bsem.at[1], mirror[0])
    share_asks = remote(dsend, drecv, dsem.at[0], dsem.at[1], mirror[0])

    barrier = pltpu.get_barrier_semaphore()
    for k, other in everyone:
        pl.semaphore_signal(
            barrier, inc=1, device_id=mirror[k] if other else at[k],
            device_id_type=pl.DeviceIdType.MESH,
        )
    fetch_book.start()
    fetch_tokens.start()

    fetch_codes.wait()
    code_row = codes_ref[...].reshape(1, rows)
    hi_row = lax.shift_right_logical(code_row, bits)
    code_col = jnp.broadcast_to(code_row.astype(F32), (128, rows)).T.astype(jnp.int32)
    hi_col = lax.shift_right_logical(code_col, bits)
    lo_col = code_col & (per - 1)
    lane = lax.broadcasted_iota(jnp.int32, (rows, 128), 1)
    own_row = hi_row == lax.broadcasted_iota(jnp.int32, (n, rows), 0)
    for k in range(per // 128):
        low1h[:, k * 128 : (k + 1) * 128] = jnp.where(lo_col == lane + k * 128, 1.0, 0.0).astype(BF16)
    low = low1h[...]
    hist = jnp.dot(jnp.where(own_row, 1.0, 0.0).astype(BF16), low, preferred_element_type=F32)
    odd = (lax.broadcasted_iota(jnp.int32, (n, 128), 0) & 1) == 1

    def first_half(found):
        total = jnp.broadcast_to(jnp.sum(found, axis=1, keepdims=True), (n, 128))
        return total, jnp.where(odd, pltpu.roll(total, 1, 0), 0.0)

    wanted = jnp.where(hist > 0.5, 1.0, 0.0)
    total, ahead = first_half(wanted)
    both = total + ahead
    over = [jnp.where(odd, jnp.maximum(both - float(c), 0.0), 0.0) for c in (cap, 2 * cap)]
    over = jnp.minimum(jnp.concatenate(over, axis=1), 256.0).astype(BF16)
    line = lax.broadcasted_iota(jnp.int32, (2 * n, n), 0)
    source = lax.broadcasted_iota(jnp.int32, (2 * n, n), 1)
    line_of = lax.rem(line, n)
    same = lax.div(line_of, cols) == lax.div(source, cols)
    earlier = lax.div(source, 2) < lax.div(line_of, 2)
    reach = jnp.where(same & (earlier | (line >= n)), 1.0, 0.0).astype(BF16)
    over = jnp.dot(reach, over, preferred_element_type=F32)
    behind = over[:n, :1]
    worst = jnp.max(over[n:], axis=0, keepdims=True)
    heavy = jnp.max(jnp.max(hist, axis=0, keepdims=True), axis=1, keepdims=True) > 256.0
    most = jnp.where(worst[:, EXTRA:] > float(wide_spill), 2.0, 1.0)
    most = jnp.where(worst[:, :EXTRA] > float(spill), most, 0.0)
    most = jnp.where(heavy, 2.0, most)
    most_pair = jnp.broadcast_to(most, (2, EXTRA)).astype(BF16)
    before = lax.broadcasted_iota(jnp.int32, (per, per), 0) < lax.broadcasted_iota(jnp.int32, (per, per), 1)
    before = jnp.where(before, 1.0, 0.0).astype(BF16)
    rank = jnp.dot(wanted.astype(BF16), before, preferred_element_type=F32) + ahead[:, :1]
    rank = jnp.minimum(rank + jnp.where(rank > cap - 0.5, behind, 0.0), 255.0)
    order = jnp.where(wanted > 0.5, rank, -1.0).astype(BF16)
    for q in range(chips):
        csend[q] = order[2 * q : 2 * q + 2, :]
    crecv[pl.ds(me, 1)] = csend[pl.ds(me, 1)]

    pl.semaphore_wait(barrier, n - 1)
    for k in partners:
        put(*ask_refs, k).start()
    hist16 = jnp.minimum(hist, 256.0).astype(BF16)
    for q in range(chips):
        hsend[q, :, :per] = hist16[2 * q : 2 * q + 2, :]
        hsend[q, :, per:] = most_pair
    hrecv[pl.ds(me, 1)] = hsend[pl.ds(me, 1)]
    fetch_book.wait()
    share_book.start()
    for k in partners:
        put(*count_refs, k).start()

    rank = rank.astype(BF16)
    hi1h = jnp.where(hi_col[:, :n] == lane[:, :n], 1.0, 0.0).astype(BF16)
    looked = jnp.dot(hi1h, rank, preferred_element_type=F32).astype(BF16) * low
    found = jnp.dot(looked, jnp.ones((per, 128), BF16), preferred_element_type=F32)
    found = found.astype(jnp.int32)
    rank1h[...] = jnp.where(found == lane, 1.0, 0.0).astype(BF16)
    chip_col = lax.shift_right_logical(hi_col, 1)
    slot = jnp.where(found < cap, chip_col * cap + found, -1)
    for k in range(chips * cap // 128):
        sel[:, k * 128 : (k + 1) * 128] = jnp.where(slot == lane + k * 128, 1.0, 0.0).astype(BF16)
    slot = jnp.where(found < cap, -1, lax.div(chip_col, half) * spill + (found - cap))
    planes = chips // half
    for k in range(0, planes * spill, 128):
        wide = min(128, planes * spill - k)
        spill1h[:, k : k + wide] = jnp.where(slot == lane + k, 1.0, 0.0).astype(BF16)[:, :wide]

    both_caps = cap + -(-spill // 16) * 16
    place = lax.broadcasted_iota(jnp.int32, (both_caps, per), 0).astype(F32).astype(BF16)
    one, none = jnp.ones((), BF16), jnp.zeros((), BF16)
    for i, d in enumerate(REPLY_ORDER):
        group = range(d * half, d * half + half)
        all_in(crecv, half if d else half - 1, csem_r.at[rows_at[d]])
        if i == 0:
            share_book.wait_recv()
        picks = []
        for k in group:
            pair = crecv[peer[k]].astype(F32)
            picks.append(jnp.concatenate(
                [
                    jnp.where(jnp.broadcast_to(pair[h : h + 1], (both_caps, per)).astype(BF16) == place, one, none)
                    for h in (0, 1)
                ],
                axis=1,
            ))
        packed = jnp.dot(jnp.concatenate(picks, axis=0), book_ref[...], preferred_element_type=F32)
        packed = packed.astype(BF16)
        for j, k in enumerate(group):
            out = psend if k else precv
            start = j * both_caps
            out[peer[k]] = packed[start : start + cap]
            if j:
                gsend[rows_at[d], chips_at[j]] = packed[start + cap : start + cap + spill]
            else:
                grecv[rows_at[d], my_chip] = packed[start + cap : start + cap + spill]
        for c in range(1, half):
            spill_put(d, c).start()
        for k in group:
            if k:
                put(*reply_refs, k).start()

    for d in REPLY_ORDER:
        all_in(grecv.at[0], half - 1, gsem_r.at[rows_at[d]])
        joint = grecv[rows_at[d], 0].astype(F32)
        for c in range(1, half):
            joint = joint + grecv[rows_at[d], c].astype(F32)
        if d:
            osend[rows_at[d]] = joint.astype(BF16)
            joint_put(d).start()
        else:
            orecv[my_row] = joint.astype(BF16)

    all_in(hrecv, chips - 1, hsem_r)
    got = jnp.concatenate([crecv[q].astype(F32) for q in range(chips)], axis=0)
    asked = jnp.concatenate([hrecv[q].astype(F32) for q in range(chips)], axis=0)
    turn = lax.broadcasted_iota(jnp.int32, (n, n), 0)
    side = jnp.where(turn < chips, core, 1 - core)
    which = 2 * lax.rem(turn, chips) + side
    split = jnp.where(lax.broadcasted_iota(jnp.int32, (n, n), 1) == which, 1.0, 0.0).astype(BF16)
    both = jnp.concatenate([got.astype(BF16), asked[:, :per].astype(BF16)], axis=1)
    both = jnp.dot(split, both, preferred_element_type=F32)
    most_asked = jnp.max(asked[:, per:], axis=0, keepdims=True)
    dsend[:, : 2 * per] = both[chips:]
    dsend[:, 2 * per :] = jnp.broadcast_to(most_asked, (chips, EXTRA))
    share_asks.start()
    share_asks.wait_recv()
    counts = jnp.sum(both[:chips, per:] + drecv[:, per : 2 * per], axis=0, keepdims=True)
    counts_ref[...] = counts.astype(jnp.int32)
    probs = counts / total_tokens
    terms = jnp.where(
        counts > 0.5, probs * jnp.log(jnp.maximum(probs, 1.0 / total_tokens)), 0.0
    )
    entropy = jnp.sum(terms, axis=1, keepdims=True)
    flag = jnp.maximum(most_asked, drecv[:1, 2 * per :])
    spots_of = [both[:chips, :per].astype(jnp.int32), drecv[:, :per].astype(jnp.int32)]

    all_in(precv, chips - 1, psem_r)
    fetch_tokens.wait()
    packs = precv[...].reshape(chips * cap, width)
    direct[...] = jnp.dot(sel[...], packs, preferred_element_type=F32)
    all_in(orecv, planes - 1, osem_r)
    packs = orecv[...].reshape(planes * spill, width)
    quant = (direct[...] + jnp.dot(spill1h[...], packs, preferred_element_type=F32)).astype(BF16)
    quant_ref[...] = quant
    diff = tokens_ref[...].astype(F32) - quant.astype(F32)
    square = diff * diff
    folded = square[:, :128]
    for k in range(1, width // 128):
        folded = folded + square[:, k * 128 : (k + 1) * 128]
    tloss = jnp.sum(folded.T, axis=0, keepdims=True) / width
    tloss_ref[...] = tloss
    part = jnp.sum(tloss, axis=1, keepdims=True)

    first = tloss.astype(BF16).astype(F32)
    second = (tloss - first).astype(BF16).astype(F32)
    third = tloss - first - second
    own_chip = lax.shift_right_logical(hi_row, 1) == lax.broadcasted_iota(jnp.int32, (chips, rows), 0)
    spread = jnp.concatenate(
        [jnp.where(own_chip, x, 0.0).astype(BF16) for x in (first, second, third)], axis=0
    )
    sums = jnp.dot(spread, rank1h[...], preferred_element_type=F32)
    sums = sums[:chips] + sums[chips : 2 * chips] + sums[2 * chips :]
    lane1 = lax.broadcasted_iota(jnp.int32, (chips, EXTRA), 1)
    sums = jnp.where(lane1 == EXTRA - 2, part, jnp.where(lane1 == EXTRA - 1, entropy, sums))
    for q in range(chips):
        lsend[q] = sums[q : q + 1, :]
    lrecv[pl.ds(me, 1)] = lsend[pl.ds(me, 1)]
    for k, other in everyone:
        loss_put(k, other).start()

    all_out(csend, chips - 1, csem_s)
    all_out(hsend, chips - 1, hsem_s)
    all_out(psend, chips - 1, psem_s)
    all_out(gsend, planes - 1, gsem_s)
    all_out(osend, planes - 1, osem_s)
    share_book.wait_send()
    share_asks.wait_send()
    all_in(lrecv, n - 1, lsem_r)
    added = jnp.zeros((chips, per), F32)
    ends = jnp.zeros((1, EXTRA), F32)
    for other in (0, 1):
        back = lrecv[other * chips : (other + 1) * chips, 0, :]
        spot = spots_of[other]
        parts = [
            jnp.take_along_axis(back, jnp.maximum(spot[:, j : j + 128], 0), axis=1)
            for j in range(0, per, 128)
        ]
        added = added + jnp.where(spot >= 0, jnp.concatenate(parts, axis=1), 0.0)
        ends = ends + jnp.sum(back, axis=0, keepdims=True)
    closs_ref[...] = jnp.sum(added, axis=0, keepdims=True)
    lane1 = lane1[:1]
    perp = jnp.exp(-ends[:, EXTRA - 1 :])
    commit = ends[:, EXTRA - 2 : EXTRA - 1] * (0.25 / total_tokens)
    scal_ref[...] = jnp.where(lane1 == 0, commit, jnp.where(lane1 == 1, perp, flag))
    all_out(lrecv, n - 1, lsem_s)


def exchange(n, cols, cap, spill, wide_spill, number, tokens, codebook, codes):
    rows, width = tokens.shape
    per = codebook.shape[0]
    chips, planes = n // 2, n // cols
    vmem = pl.BlockSpec(memory_space=pltpu.VMEM)
    dma = pltpu.SemaphoreType.DMA
    return pl.pallas_call(
        functools.partial(kernel, n, cols, cap, spill, wide_spill),
        out_shape=(
            pltpu.VMEM((rows, width), BF16),
            pltpu.VMEM((1, rows), F32),
            pltpu.VMEM((1, per), jnp.int32),
            pltpu.VMEM((1, per), F32),
            pltpu.VMEM((1, EXTRA), F32),
        ),
        in_specs=[pl.BlockSpec(memory_space=pltpu.HBM)] * 3,
        out_specs=(vmem,) * 5,
        scratch_shapes=[
            pltpu.VMEM(codes.shape, jnp.int32),
            pltpu.VMEM((rows, width), BF16),
            pltpu.VMEM((2 * per, width), BF16),
            pltpu.VMEM((chips, 2, per), BF16),
            pltpu.VMEM((chips, 2, per), BF16),
            pltpu.VMEM((chips, 2, per + EXTRA), BF16),
            pltpu.VMEM((chips, 2, per + EXTRA), BF16),
            pltpu.VMEM((chips, cap, width), BF16),
            pltpu.VMEM((chips, cap, width), BF16),
            pltpu.VMEM((planes, cols // 2, spill, width), BF16),
            pltpu.VMEM((planes, cols // 2, spill, width), BF16),
            pltpu.VMEM((planes, spill, width), BF16),
            pltpu.VMEM((planes, spill, width), BF16),
            pltpu.VMEM((chips, 2 * per + EXTRA), F32),
            pltpu.VMEM((chips, 2 * per + EXTRA), F32),
            pltpu.VMEM((chips, 1, EXTRA), F32),
            pltpu.VMEM((n, 1, EXTRA), F32),
            pltpu.VMEM((rows, per), BF16),
            pltpu.VMEM((rows, chips * cap), BF16),
            pltpu.VMEM((rows, planes * spill), BF16),
            pltpu.VMEM((rows, 128), BF16),
            pltpu.VMEM((rows, width), F32),
            dma((3,)),
            dma, dma((planes,)), *[dma] * 4,
            dma, dma((planes,)), *[dma] * 4,
            dma((2,)), dma((2,)),
        ],
        compiler_params=pltpu.CompilerParams(collective_id=number, has_side_effects=True),
    )(*[pltpu.with_memory_space_constraint(x, pltpu.HBM) for x in (codes, tokens, codebook)])


def finish_kernel(
    quant_ref, tloss_ref, counts_ref, closs_ref, scal_ref,
    quant_out, tloss_out, counts_out, closs_out, commit_out, perp_out, flag_out,
    tloss, counts, closs, commit, perp, sem,
):
    whole = pltpu.make_async_copy(quant_ref, quant_out, sem.at[0])
    whole.start()
    tloss[...] = tloss_ref[...].reshape(tloss.shape)
    counts[...] = counts_ref[...].reshape(counts.shape)
    closs[...] = closs_ref[...].reshape(closs.shape)
    commit[...] = scal_ref[:, :1]
    perp[...] = scal_ref[:, 1:2]
    small = [(tloss, tloss_out), (counts, counts_out), (closs, closs_out), (commit, commit_out), (perp, perp_out)]
    small = [pltpu.make_async_copy(src, dst, sem.at[1 + i]) for i, (src, dst) in enumerate(small)]
    for one in small:
        one.start()
    flag_out[0, 0] = jnp.max(scal_ref[:, 2:3]).astype(jnp.int32)
    for one in small:
        one.wait()
    whole.wait()


def finish(quantized, token_loss, counts, code_loss, scalars):
    rows, per = token_loss.shape[1], counts.shape[1]
    vmem = pl.BlockSpec(memory_space=pltpu.VMEM)
    hbm = pl.BlockSpec(memory_space=pltpu.HBM)
    q, t, k, c, m, p, f = pl.pallas_call(
        finish_kernel,
        out_shape=(
            jax.ShapeDtypeStruct(quantized.shape, BF16),
            jax.ShapeDtypeStruct((rows,), F32),
            jax.ShapeDtypeStruct((per,), jnp.int32),
            jax.ShapeDtypeStruct((per,), F32),
            jax.ShapeDtypeStruct((1, 1), F32),
            jax.ShapeDtypeStruct((1, 1), F32),
            pltpu.SMEM((1, 1), jnp.int32),
        ),
        in_specs=[vmem] * 5,
        out_specs=(hbm,) * 6 + (pl.BlockSpec(memory_space=pltpu.SMEM),),
        scratch_shapes=[
            pltpu.VMEM((rows,), F32),
            pltpu.VMEM((per,), jnp.int32),
            pltpu.VMEM((per,), F32),
            pltpu.VMEM((1, 1), F32),
            pltpu.VMEM((1, 1), F32),
            pltpu.SemaphoreType.DMA((6,)),
        ],
        compiler_params=pltpu.CompilerParams(vmem_limit_bytes=4 << 20),
    )(quantized, token_loss, counts, code_loss, scalars)
    return q, t, k, c, m[0, 0], p[0, 0], f


def held(x):
    def body(src, dst, sem):
        copy = pltpu.make_async_copy(src, dst, sem)
        copy.start()
        copy.wait()

    return pl.pallas_call(
        body,
        out_shape=jax.ShapeDtypeStruct(x.shape, x.dtype),
        in_specs=[pl.BlockSpec(memory_space=pltpu.HBM)],
        out_specs=pl.BlockSpec(memory_space=pltpu.VMEM),
        scratch_shapes=[pltpu.SemaphoreType.DMA],
    )(pltpu.with_memory_space_constraint(x, pltpu.HBM))


def asked_plan(n, cols, cap, spill, tokens, codebook, codes):
    wide = spill * 2
    outs = exchange(n, cols, cap, spill, wide, 0, tokens, codebook, codes)

    *done, flag = finish(*outs)

    def kept():
        return tuple(done)

    def wider():
        return finish(*exchange(n, cols, 2 * cap, wide, wide, 1, tokens, codebook, codes))[:-1]

    def ringed():
        return ring_plan(n, held(tokens), held(codebook), held(codes))

    def any_codes():
        return lax.cond(flag[0, 0] > 1, ringed, wider)

    return lax.cond(flag[0, 0] > 0, any_codes, kept)


def on_device(n, cols, tokens, codebook, codes):
    rows, width = tokens.shape
    per = codebook.shape[0]
    cap = -(-rows // (n * 16)) * 16
    spill = cap * 3 // 4
    fits = (
        per % 128 == 0
        and per & (per - 1) == 0
        and rows % 128 == 0
        and width % 128 == 0
        and n // 2 * cap % 128 == 0
        and spill % 8 == 0
        and cols == 8
        and n == 4 * cols
        and n <= 128
        and 2 * cap + 2 * spill < EXTRA - 1
    )
    if fits:
        return asked_plan(n, cols, cap, spill, tokens, codebook, codes)
    return dense_plan(tokens, codebook, codes)


def solution(mesh):
    n = mesh.shape["row"] * mesh.shape["col"]
    return jax.shard_map(
        functools.partial(on_device, n, mesh.shape["col"]),
        mesh=mesh,
        in_specs=(P(AXES, None), P(AXES, None), P(AXES)),
        out_specs=(P(AXES, None), P(AXES), P(AXES), P(AXES), P(), P()),
        check_vma=False,
    )
```

```python
import functools

import jax
import jax.numpy as jnp
from jax import lax
from jax.experimental import pallas as pl
from jax.experimental.pallas import tpu as pltpu
from jax.sharding import PartitionSpec as P

AXES = ("row", "col")
EXTRA = 128
ASK_ORDER = (2, 3, 1, 0)
REPLY_ORDER = (2, 3, 1, 0)
F32 = jnp.float32
BF16 = jnp.bfloat16


def dense_plan(tokens, codebook, codes):
    tok_rows = tokens.shape[0]
    width = tokens.shape[1]
    per_dev = codebook.shape[0]
    devices = lax.axis_size("row") * lax.axis_size("col")
    total_codes = per_dev * devices
    total_tokens = tok_rows * devices
    full_book = lax.all_gather(codebook, AXES, axis=0, tiled=True)
    quantized = jnp.take(full_book, codes, axis=0)
    diff = tokens.astype(F32) - quantized.astype(F32)
    token_loss = jnp.sum(diff * diff, axis=1) / width
    loss_part = jnp.sum(token_loss)
    local_counts = jax.ops.segment_sum(
        jnp.ones((tok_rows,), F32), codes, num_segments=total_codes
    )
    local_loss = jax.ops.segment_sum(token_loss, codes, num_segments=total_codes)
    floor_prob = jnp.float32(1.0 / total_tokens)
    totals, loss_totals = lax.psum((local_counts, local_loss), AXES)
    loss_sum = lax.psum(loss_part, AXES)
    probs = totals / total_tokens
    terms = jnp.where(
        totals > 0.5, probs * jnp.log(jnp.maximum(probs, floor_prob)), jnp.float32(0.0)
    )
    offset = lax.axis_index(AXES) * per_dev
    owned_counts = lax.dynamic_slice_in_dim(totals, offset, per_dev, 0)
    code_loss = lax.dynamic_slice_in_dim(loss_totals, offset, per_dev, 0)
    commitment = 0.25 * loss_sum / total_tokens
    return (
        quantized,
        token_loss,
        owned_counts.astype(jnp.int32),
        code_loss,
        commitment,
        jnp.exp(-jnp.sum(terms)),
    )


def ring_plan(n, tokens, codebook, codes):
    rows, width = tokens.shape
    per_dev = codebook.shape[0]
    me = lax.axis_index(AXES)
    ring = [(i, (i + 1) % n) for i in range(n)]
    hi = codes // per_dev
    lo = codes % per_dev

    def pick(step, carry):
        block, got = carry
        owner = lax.rem(me - step + n, n)
        got = jnp.where((hi == owner)[:, None], jnp.take(block, lo, axis=0), got)
        return lax.ppermute(block, AXES, ring), got

    _, quantized = lax.fori_loop(0, n, pick, (codebook, jnp.zeros_like(tokens)))
    diff = tokens.astype(F32) - quantized.astype(F32)
    token_loss = jnp.sum(diff * diff, axis=1) / width

    def add(step, carry):
        c, t, total, hits, parts = carry
        owner = lax.rem(me - step + n, n)
        mine = (c // per_dev) == me
        total = total + jax.ops.segment_sum(
            jnp.where(mine, t, 0.0), c % per_dev, num_segments=per_dev
        )
        hits = hits + jax.ops.segment_sum(
            mine.astype(jnp.int32), c % per_dev, num_segments=per_dev
        )
        parts = lax.dynamic_update_slice(parts, jnp.sum(t)[None], (owner,))
        return lax.ppermute(c, AXES, ring), lax.ppermute(t, AXES, ring), total, hits, parts

    start = (
        codes, token_loss, jnp.zeros((per_dev,), F32),
        jnp.zeros((per_dev,), jnp.int32), jnp.zeros((n,), F32),
    )
    _, _, code_loss, counts, parts = lax.fori_loop(0, n, add, start)
    probs = counts.astype(F32) / (rows * n)
    floor_prob = jnp.float32(1.0 / (rows * n))
    terms = jnp.where(counts > 0, probs * jnp.log(jnp.maximum(probs, floor_prob)), 0.0)

    def collect(step, carry):
        entropy, parts = carry
        owner = lax.rem(me - step + n, n)
        parts = lax.dynamic_update_slice(parts, entropy, (owner,))
        return lax.ppermute(entropy, AXES, ring), parts

    _, entropies = lax.fori_loop(0, n, collect, (jnp.sum(terms)[None], jnp.zeros((n,), F32)))
    commitment = 0.25 * jnp.sum(parts) / (rows * n)
    return quantized, token_loss, counts, code_loss, commitment, jnp.exp(-jnp.sum(entropies))


def kernel(
    n, cols, cap, spill, wide_spill,
    codes_hbm, tokens_hbm, book_hbm,
    quant_ref, tloss_ref, counts_ref, closs_ref, scal_ref,
    codes_ref, tokens_ref, book_ref, csend, crecv, hsend, hrecv, psend, precv, gsend, grecv, osend, orecv,
    dsend, drecv, lsend, lrecv, low1h, sel, spill1h, rank1h, direct,
    in_sem, csem_s, csem_r, hsem_s, hsem_r, psem_s, psem_r,
    gsem_s, gsem_r, osem_s, osem_r, lsem_s, lsem_r, bsem, dsem,
):
    rows, width = tokens_hbm.shape
    per = book_hbm.shape[0]
    bits = per.bit_length() - 1
    total_tokens = rows * n
    chips, half = n // 2, cols // 2
    my_row, my_col = lax.axis_index("row"), lax.axis_index("col")
    core = lax.rem(my_col, 2)
    my_chip = lax.div(my_col, 2)
    me = my_row * half + my_chip
    inner = lax.rem(lax.div(my_row + 1, 2), 2)
    beside, across = my_row + 1 - 2 * lax.rem(my_row, 2), 3 - my_row
    skip, late = lax.rem(my_row + 2, 4), lax.div(my_row, 2)
    near = inner * across + (1 - inner) * beside
    far = inner * beside + (1 - inner) * across
    first = late * beside + (1 - late) * skip
    then = late * skip + (1 - late) * far
    last = late * across + (1 - late) * near
    rows_at = [my_row, last, first, then]
    chips_at = [
        my_chip, my_chip + 1 - 2 * lax.rem(my_chip, 2), lax.rem(my_chip + 2, 4), 3 - my_chip
    ]
    spots = [(rows_at[k // half], chips_at[k % half]) for k in range(chips)]
    at = [(r, 2 * c + core) for r, c in spots]
    mirror = [(r, 2 * c + 1 - core) for r, c in spots]
    peer = [r * half + c for r, c in spots]
    fetch_codes = pltpu.make_async_copy(codes_hbm, codes_ref, in_sem.at[0])
    own_book = book_ref.at[pl.ds(pl.multiple_of(core * per, per), per)]
    fetch_book = pltpu.make_async_copy(book_hbm, own_book, in_sem.at[1])
    fetch_tokens = pltpu.make_async_copy(tokens_hbm, tokens_ref, in_sem.at[2])
    fetch_codes.start()

    def remote(src, dst, ssem, rsem, to):
        return pltpu.make_async_remote_copy(
            src_ref=src,
            dst_ref=dst,
            send_sem=ssem,
            recv_sem=rsem,
            device_id=to,
            device_id_type=pl.DeviceIdType.MESH,
        )

    def put(send, recv, ssem, rsem, k):
        return remote(send.at[peer[k]], recv.at[me], ssem, rsem, at[k])

    def spill_put(d, c):
        r, to = rows_at[d], chips_at[c]
        return remote(gsend.at[r, to], grecv.at[r, my_chip], gsem_s, gsem_r.at[r], at[c])

    def joint_put(d):
        return remote(osend.at[rows_at[d]], orecv.at[my_row], osem_s, osem_r, at[d * half])

    def loss_put(k, other):
        to = mirror[k] if other else at[k]
        return remote(lsend.at[peer[k]], lrecv.at[other * chips + me], lsem_s, lsem_r, to)

    def all_in(ref, count, sem):
        part = ref.at[pl.ds(0, count)]
        remote(part, part, sem, sem, mirror[0]).wait_recv()

    def all_out(ref, count, sem):
        part = ref.at[pl.ds(0, count)]
        remote(part, part, sem, sem, mirror[0]).wait_send()

    ask_refs = (csend, crecv, csem_s, csem_r.at[my_row])
    count_refs = (hsend, hrecv, hsem_s, hsem_r)
    reply_refs = (psend, precv, psem_s, psem_r)
    partners = [k for d in ASK_ORDER for k in range(d * half, d * half + half) if k]
    everyone = [(k, other) for d in ASK_ORDER for k in range(d * half, d * half + half)
                for other in (0, 1) if k or other]
    share_book = remote(own_book, own_book, bsem.at[0], bsem.at[1], mirror[0])
    share_asks = remote(dsend, drecv, dsem.at[0], dsem.at[1], mirror[0])

    barrier = pltpu.get_barrier_semaphore()
    for k, other in everyone:
        pl.semaphore_signal(
            barrier, inc=1, device_id=mirror[k] if other else at[k],
            device_id_type=pl.DeviceIdType.MESH,
        )
    fetch_book.start()
    fetch_tokens.start()

    fetch_codes.wait()
    code_row = codes_ref[...].reshape(1, rows)
    hi_row = lax.shift_right_logical(code_row, bits)
    code_col = jnp.broadcast_to(code_row.astype(F32), (128, rows)).T.astype(jnp.int32)
    hi_col = lax.shift_right_logical(code_col, bits)
    lo_col = code_col & (per - 1)
    lane = lax.broadcasted_iota(jnp.int32, (rows, 128), 1)
    own_row = hi_row == lax.broadcasted_iota(jnp.int32, (n, rows), 0)
    for k in range(per // 128):
        low1h[:, k * 128 : (k + 1) * 128] = jnp.where(lo_col == lane + k * 128, 1.0, 0.0).astype(BF16)
    low = low1h[...]
    hist = jnp.dot(jnp.where(own_row, 1.0, 0.0).astype(BF16), low, preferred_element_type=F32)
    odd = (lax.broadcasted_iota(jnp.int32, (n, 128), 0) & 1) == 1

    def first_half(found):
        total = jnp.broadcast_to(jnp.sum(found, axis=1, keepdims=True), (n, 128))
        return total, jnp.where(odd, pltpu.roll(total, 1, 0), 0.0)

    wanted = jnp.where(hist > 0.5, 1.0, 0.0)
    total, ahead = first_half(wanted)
    both = total + ahead
    over = [jnp.where(odd, jnp.maximum(both - float(c), 0.0), 0.0) for c in (cap, 2 * cap)]
    over = jnp.minimum(jnp.concatenate(over, axis=1), 256.0).astype(BF16)
    line = lax.broadcasted_iota(jnp.int32, (2 * n, n), 0)
    source = lax.broadcasted_iota(jnp.int32, (2 * n, n), 1)
    line_of = lax.rem(line, n)
    same = lax.div(line_of, cols) == lax.div(source, cols)
    earlier = lax.div(source, 2) < lax.div(line_of, 2)
    reach = jnp.where(same & (earlier | (line >= n)), 1.0, 0.0).astype(BF16)
    over = jnp.dot(reach, over, preferred_element_type=F32)
    behind = over[:n, :1]
    worst = jnp.max(over[n:], axis=0, keepdims=True)
    heavy = jnp.max(jnp.max(hist, axis=0, keepdims=True), axis=1, keepdims=True) > 256.0
    most = jnp.where(worst[:, EXTRA:] > float(wide_spill), 2.0, 1.0)
    most = jnp.where(worst[:, :EXTRA] > float(spill), most, 0.0)
    most = jnp.where(heavy, 2.0, most)
    most_pair = jnp.broadcast_to(most, (2, EXTRA)).astype(BF16)
    before = lax.broadcasted_iota(jnp.int32, (per, per), 0) < lax.broadcasted_iota(jnp.int32, (per, per), 1)
    before = jnp.where(before, 1.0, 0.0).astype(BF16)
    rank = jnp.dot(wanted.astype(BF16), before, preferred_element_type=F32) + ahead[:, :1]
    rank = jnp.minimum(rank + jnp.where(rank > cap - 0.5, behind, 0.0), 255.0)
    order = jnp.where(wanted > 0.5, rank, -1.0).astype(BF16)
    for q in range(chips):
        csend[q] = order[2 * q : 2 * q + 2, :]
    crecv[pl.ds(me, 1)] = csend[pl.ds(me, 1)]

    pl.semaphore_wait(barrier, n - 1)
    for k in partners:
        put(*ask_refs, k).start()
    hist16 = jnp.minimum(hist, 256.0).astype(BF16)
    for q in range(chips):
        hsend[q, :, :per] = hist16[2 * q : 2 * q + 2, :]
        hsend[q, :, per:] = most_pair
    hrecv[pl.ds(me, 1)] = hsend[pl.ds(me, 1)]
    fetch_book.wait()
    share_book.start()
    for k in partners:
        put(*count_refs, k).start()

    rank = rank.astype(BF16)
    hi1h = jnp.where(hi_col[:, :n] == lane[:, :n], 1.0, 0.0).astype(BF16)
    looked = jnp.dot(hi1h, rank, preferred_element_type=F32).astype(BF16) * low
    found = jnp.dot(looked, jnp.ones((per, 128), BF16), preferred_element_type=F32)
    found = found.astype(jnp.int32)
    rank1h[...] = jnp.where(found == lane, 1.0, 0.0).astype(BF16)
    chip_col = lax.shift_right_logical(hi_col, 1)
    slot = jnp.where(found < cap, chip_col * cap + found, -1)
    for k in range(chips * cap // 128):
        sel[:, k * 128 : (k + 1) * 128] = jnp.where(slot == lane + k * 128, 1.0, 0.0).astype(BF16)
    slot = jnp.where(found < cap, -1, lax.div(chip_col, half) * spill + (found - cap))
    planes = chips // half
    for k in range(0, planes * spill, 128):
        wide = min(128, planes * spill - k)
        spill1h[:, k : k + wide] = jnp.where(slot == lane + k, 1.0, 0.0).astype(BF16)[:, :wide]

    both_caps = cap + -(-spill // 16) * 16
    place = lax.broadcasted_iota(jnp.int32, (both_caps, per), 0).astype(F32).astype(BF16)
    one, none = jnp.ones((), BF16), jnp.zeros((), BF16)
    for i, d in enumerate(REPLY_ORDER):
        group = range(d * half, d * half + half)
        all_in(crecv, half if d else half - 1, csem_r.at[rows_at[d]])
        if i == 0:
            share_book.wait_recv()
        for first in range(0, half, 2):
            picks = []
            for k in group[first : first + 2]:
                pair = crecv[peer[k]].astype(F32)
                picks.append(jnp.concatenate(
                    [
                        jnp.where(jnp.broadcast_to(pair[h : h + 1], (both_caps, per)).astype(BF16) == place, one, none)
                        for h in (0, 1)
                    ],
                    axis=1,
                ))
            packed = jnp.dot(jnp.concatenate(picks, axis=0), book_ref[...], preferred_element_type=F32)
            packed = packed.astype(BF16)
            for j, k in enumerate(group[first : first + 2]):
                c = first + j
                out = psend if k else precv
                start = j * both_caps
                out[peer[k]] = packed[start : start + cap]
                if c:
                    gsend[rows_at[d], chips_at[c]] = packed[start + cap : start + cap + spill]
                    spill_put(d, c).start()
                else:
                    grecv[rows_at[d], my_chip] = packed[start + cap : start + cap + spill]
            for k in group[first : first + 2]:
                if k:
                    put(*reply_refs, k).start()

    for d in REPLY_ORDER:
        all_in(grecv.at[0], half - 1, gsem_r.at[rows_at[d]])
        joint = grecv[rows_at[d], 0].astype(F32)
        for c in range(1, half):
            joint = joint + grecv[rows_at[d], c].astype(F32)
        if d:
            osend[rows_at[d]] = joint.astype(BF16)
            joint_put(d).start()
        else:
            orecv[my_row] = joint.astype(BF16)

    all_in(hrecv, chips - 1, hsem_r)
    got = jnp.concatenate([crecv[q].astype(F32) for q in range(chips)], axis=0)
    asked = jnp.concatenate([hrecv[q].astype(F32) for q in range(chips)], axis=0)
    turn = lax.broadcasted_iota(jnp.int32, (n, n), 0)
    side = jnp.where(turn < chips, core, 1 - core)
    which = 2 * lax.rem(turn, chips) + side
    split = jnp.where(lax.broadcasted_iota(jnp.int32, (n, n), 1) == which, 1.0, 0.0).astype(BF16)
    both = jnp.concatenate([got.astype(BF16), asked[:, :per].astype(BF16)], axis=1)
    both = jnp.dot(split, both, preferred_element_type=F32)
    most_asked = jnp.max(asked[:, per:], axis=0, keepdims=True)
    dsend[:, : 2 * per] = both[chips:]
    dsend[:, 2 * per :] = jnp.broadcast_to(most_asked, (chips, EXTRA))
    share_asks.start()
    share_asks.wait_recv()
    counts = jnp.sum(both[:chips, per:] + drecv[:, per : 2 * per], axis=0, keepdims=True)
    counts_ref[...] = counts.astype(jnp.int32)
    probs = counts / total_tokens
    terms = jnp.where(
        counts > 0.5, probs * jnp.log(jnp.maximum(probs, 1.0 / total_tokens)), 0.0
    )
    entropy = jnp.sum(terms, axis=1, keepdims=True)
    flag = jnp.maximum(most_asked, drecv[:1, 2 * per :])
    spots_of = [both[:chips, :per].astype(jnp.int32), drecv[:, :per].astype(jnp.int32)]

    all_in(precv, chips - 1, psem_r)
    fetch_tokens.wait()
    packs = precv[...].reshape(chips * cap, width)
    direct[...] = jnp.dot(sel[...], packs, preferred_element_type=F32)
    all_in(orecv, planes - 1, osem_r)
    packs = orecv[...].reshape(planes * spill, width)
    quant = (direct[...] + jnp.dot(spill1h[...], packs, preferred_element_type=F32)).astype(BF16)
    quant_ref[...] = quant
    diff = tokens_ref[...].astype(F32) - quant.astype(F32)
    square = diff * diff
    folded = square[:, :128]
    for k in range(1, width // 128):
        folded = folded + square[:, k * 128 : (k + 1) * 128]
    tloss = jnp.sum(folded.T, axis=0, keepdims=True) / width
    tloss_ref[...] = tloss
    part = jnp.sum(tloss, axis=1, keepdims=True)

    first = tloss.astype(BF16).astype(F32)
    second = (tloss - first).astype(BF16).astype(F32)
    third = tloss - first - second
    own_chip = lax.shift_right_logical(hi_row, 1) == lax.broadcasted_iota(jnp.int32, (chips, rows), 0)
    spread = jnp.concatenate(
        [jnp.where(own_chip, x, 0.0).astype(BF16) for x in (first, second, third)], axis=0
    )
    sums = jnp.dot(spread, rank1h[...], preferred_element_type=F32)
    sums = sums[:chips] + sums[chips : 2 * chips] + sums[2 * chips :]
    lane1 = lax.broadcasted_iota(jnp.int32, (chips, EXTRA), 1)
    sums = jnp.where(lane1 == EXTRA - 2, part, jnp.where(lane1 == EXTRA - 1, entropy, sums))
    for q in range(chips):
        lsend[q] = sums[q : q + 1, :]
    lrecv[pl.ds(me, 1)] = lsend[pl.ds(me, 1)]
    for k, other in everyone:
        loss_put(k, other).start()

    all_out(csend, chips - 1, csem_s)
    all_out(hsend, chips - 1, hsem_s)
    all_out(psend, chips - 1, psem_s)
    all_out(gsend, planes - 1, gsem_s)
    all_out(osend, planes - 1, osem_s)
    share_book.wait_send()
    share_asks.wait_send()
    all_in(lrecv, n - 1, lsem_r)
    added = jnp.zeros((chips, per), F32)
    ends = jnp.zeros((1, EXTRA), F32)
    for other in (0, 1):
        back = lrecv[other * chips : (other + 1) * chips, 0, :]
        spot = spots_of[other]
        parts = [
            jnp.take_along_axis(back, jnp.maximum(spot[:, j : j + 128], 0), axis=1)
            for j in range(0, per, 128)
        ]
        added = added + jnp.where(spot >= 0, jnp.concatenate(parts, axis=1), 0.0)
        ends = ends + jnp.sum(back, axis=0, keepdims=True)
    closs_ref[...] = jnp.sum(added, axis=0, keepdims=True)
    lane1 = lane1[:1]
    perp = jnp.exp(-ends[:, EXTRA - 1 :])
    commit = ends[:, EXTRA - 2 : EXTRA - 1] * (0.25 / total_tokens)
    scal_ref[...] = jnp.where(lane1 == 0, commit, jnp.where(lane1 == 1, perp, flag))
    all_out(lrecv, n - 1, lsem_s)


def exchange(n, cols, cap, spill, wide_spill, number, tokens, codebook, codes):
    rows, width = tokens.shape
    per = codebook.shape[0]
    chips, planes = n // 2, n // cols
    vmem = pl.BlockSpec(memory_space=pltpu.VMEM)
    dma = pltpu.SemaphoreType.DMA
    return pl.pallas_call(
        functools.partial(kernel, n, cols, cap, spill, wide_spill),
        out_shape=(
            pltpu.VMEM((rows, width), BF16),
            pltpu.VMEM((1, rows), F32),
            pltpu.VMEM((1, per), jnp.int32),
            pltpu.VMEM((1, per), F32),
            pltpu.VMEM((1, EXTRA), F32),
        ),
        in_specs=[pl.BlockSpec(memory_space=pltpu.HBM)] * 3,
        out_specs=(vmem,) * 5,
        scratch_shapes=[
            pltpu.VMEM(codes.shape, jnp.int32),
            pltpu.VMEM((rows, width), BF16),
            pltpu.VMEM((2 * per, width), BF16),
            pltpu.VMEM((chips, 2, per), BF16),
            pltpu.VMEM((chips, 2, per), BF16),
            pltpu.VMEM((chips, 2, per + EXTRA), BF16),
            pltpu.VMEM((chips, 2, per + EXTRA), BF16),
            pltpu.VMEM((chips, cap, width), BF16),
            pltpu.VMEM((chips, cap, width), BF16),
            pltpu.VMEM((planes, cols // 2, spill, width), BF16),
            pltpu.VMEM((planes, cols // 2, spill, width), BF16),
            pltpu.VMEM((planes, spill, width), BF16),
            pltpu.VMEM((planes, spill, width), BF16),
            pltpu.VMEM((chips, 2 * per + EXTRA), F32),
            pltpu.VMEM((chips, 2 * per + EXTRA), F32),
            pltpu.VMEM((chips, 1, EXTRA), F32),
            pltpu.VMEM((n, 1, EXTRA), F32),
            pltpu.VMEM((rows, per), BF16),
            pltpu.VMEM((rows, chips * cap), BF16),
            pltpu.VMEM((rows, planes * spill), BF16),
            pltpu.VMEM((rows, 128), BF16),
            pltpu.VMEM((rows, width), F32),
            dma((3,)),
            dma, dma((planes,)), *[dma] * 4,
            dma, dma((planes,)), *[dma] * 4,
            dma((2,)), dma((2,)),
        ],
        compiler_params=pltpu.CompilerParams(collective_id=number, has_side_effects=True),
    )(*[pltpu.with_memory_space_constraint(x, pltpu.HBM) for x in (codes, tokens, codebook)])


def finish_kernel(
    quant_ref, tloss_ref, counts_ref, closs_ref, scal_ref,
    quant_out, tloss_out, counts_out, closs_out, commit_out, perp_out, flag_out,
    tloss, counts, closs, commit, perp, sem,
):
    whole = pltpu.make_async_copy(quant_ref, quant_out, sem.at[0])
    whole.start()
    tloss[...] = tloss_ref[...].reshape(tloss.shape)
    counts[...] = counts_ref[...].reshape(counts.shape)
    closs[...] = closs_ref[...].reshape(closs.shape)
    commit[...] = scal_ref[:, :1]
    perp[...] = scal_ref[:, 1:2]
    small = [(tloss, tloss_out), (counts, counts_out), (closs, closs_out), (commit, commit_out), (perp, perp_out)]
    small = [pltpu.make_async_copy(src, dst, sem.at[1 + i]) for i, (src, dst) in enumerate(small)]
    for one in small:
        one.start()
    flag_out[0, 0] = jnp.max(scal_ref[:, 2:3]).astype(jnp.int32)
    for one in small:
        one.wait()
    whole.wait()


def finish(quantized, token_loss, counts, code_loss, scalars):
    rows, per = token_loss.shape[1], counts.shape[1]
    vmem = pl.BlockSpec(memory_space=pltpu.VMEM)
    hbm = pl.BlockSpec(memory_space=pltpu.HBM)
    q, t, k, c, m, p, f = pl.pallas_call(
        finish_kernel,
        out_shape=(
            jax.ShapeDtypeStruct(quantized.shape, BF16),
            jax.ShapeDtypeStruct((rows,), F32),
            jax.ShapeDtypeStruct((per,), jnp.int32),
            jax.ShapeDtypeStruct((per,), F32),
            jax.ShapeDtypeStruct((1, 1), F32),
            jax.ShapeDtypeStruct((1, 1), F32),
            pltpu.SMEM((1, 1), jnp.int32),
        ),
        in_specs=[vmem] * 5,
        out_specs=(hbm,) * 6 + (pl.BlockSpec(memory_space=pltpu.SMEM),),
        scratch_shapes=[
            pltpu.VMEM((rows,), F32),
            pltpu.VMEM((per,), jnp.int32),
            pltpu.VMEM((per,), F32),
            pltpu.VMEM((1, 1), F32),
            pltpu.VMEM((1, 1), F32),
            pltpu.SemaphoreType.DMA((6,)),
        ],
        compiler_params=pltpu.CompilerParams(vmem_limit_bytes=4 << 20),
    )(quantized, token_loss, counts, code_loss, scalars)
    return q, t, k, c, m[0, 0], p[0, 0], f


def held(x):
    def body(src, dst, sem):
        copy = pltpu.make_async_copy(src, dst, sem)
        copy.start()
        copy.wait()

    return pl.pallas_call(
        body,
        out_shape=jax.ShapeDtypeStruct(x.shape, x.dtype),
        in_specs=[pl.BlockSpec(memory_space=pltpu.HBM)],
        out_specs=pl.BlockSpec(memory_space=pltpu.VMEM),
        scratch_shapes=[pltpu.SemaphoreType.DMA],
    )(pltpu.with_memory_space_constraint(x, pltpu.HBM))


def asked_plan(n, cols, cap, spill, tokens, codebook, codes):
    wide = spill * 2
    outs = exchange(n, cols, cap, spill, wide, 0, tokens, codebook, codes)

    *done, flag = finish(*outs)

    def kept():
        return tuple(done)

    def wider():
        return finish(*exchange(n, cols, 2 * cap, wide, wide, 1, tokens, codebook, codes))[:-1]

    def ringed():
        return ring_plan(n, held(tokens), held(codebook), held(codes))

    def any_codes():
        return lax.cond(flag[0, 0] > 1, ringed, wider)

    return lax.cond(flag[0, 0] > 0, any_codes, kept)


def on_device(n, cols, tokens, codebook, codes):
    rows, width = tokens.shape
    per = codebook.shape[0]
    cap = -(-rows // (n * 16)) * 16
    spill = cap * 3 // 4
    fits = (
        per % 128 == 0
        and per & (per - 1) == 0
        and rows % 128 == 0
        and width % 128 == 0
        and n // 2 * cap % 128 == 0
        and spill % 8 == 0
        and cols == 8
        and n == 4 * cols
        and n <= 128
        and 2 * cap + 2 * spill < EXTRA - 1
    )
    if fits:
        return asked_plan(n, cols, cap, spill, tokens, codebook, codes)
    return dense_plan(tokens, codebook, codes)


def solution(mesh):
    n = mesh.shape["row"] * mesh.shape["col"]
    return jax.shard_map(
        functools.partial(on_device, n, mesh.shape["col"]),
        mesh=mesh,
        in_specs=(P(AXES, None), P(AXES, None), P(AXES)),
        out_specs=(P(AXES, None), P(AXES), P(AXES), P(AXES), P(), P()),
        check_vma=False,
    )
```

```python
import functools

import jax
import jax.numpy as jnp
from jax import lax
from jax.experimental import pallas as pl
from jax.experimental.pallas import tpu as pltpu
from jax.sharding import PartitionSpec as P

AXES = ("row", "col")
EXTRA = 128
ASK_ORDER = (2, 3, 1, 0)
REPLY_ORDER = (2, 3, 1, 0)
F32 = jnp.float32
BF16 = jnp.bfloat16


def dense_plan(tokens, codebook, codes):
    tok_rows = tokens.shape[0]
    width = tokens.shape[1]
    per_dev = codebook.shape[0]
    devices = lax.axis_size("row") * lax.axis_size("col")
    total_codes = per_dev * devices
    total_tokens = tok_rows * devices
    full_book = lax.all_gather(codebook, AXES, axis=0, tiled=True)
    quantized = jnp.take(full_book, codes, axis=0)
    diff = tokens.astype(F32) - quantized.astype(F32)
    token_loss = jnp.sum(diff * diff, axis=1) / width
    loss_part = jnp.sum(token_loss)
    local_counts = jax.ops.segment_sum(
        jnp.ones((tok_rows,), F32), codes, num_segments=total_codes
    )
    local_loss = jax.ops.segment_sum(token_loss, codes, num_segments=total_codes)
    floor_prob = jnp.float32(1.0 / total_tokens)
    totals, loss_totals = lax.psum((local_counts, local_loss), AXES)
    loss_sum = lax.psum(loss_part, AXES)
    probs = totals / total_tokens
    terms = jnp.where(
        totals > 0.5, probs * jnp.log(jnp.maximum(probs, floor_prob)), jnp.float32(0.0)
    )
    offset = lax.axis_index(AXES) * per_dev
    owned_counts = lax.dynamic_slice_in_dim(totals, offset, per_dev, 0)
    code_loss = lax.dynamic_slice_in_dim(loss_totals, offset, per_dev, 0)
    commitment = 0.25 * loss_sum / total_tokens
    return (
        quantized,
        token_loss,
        owned_counts.astype(jnp.int32),
        code_loss,
        commitment,
        jnp.exp(-jnp.sum(terms)),
    )


def ring_plan(n, tokens, codebook, codes):
    rows, width = tokens.shape
    per_dev = codebook.shape[0]
    me = lax.axis_index(AXES)
    ring = [(i, (i + 1) % n) for i in range(n)]
    hi = codes // per_dev
    lo = codes % per_dev

    def pick(step, carry):
        block, got = carry
        owner = lax.rem(me - step + n, n)
        got = jnp.where((hi == owner)[:, None], jnp.take(block, lo, axis=0), got)
        return lax.ppermute(block, AXES, ring), got

    _, quantized = lax.fori_loop(0, n, pick, (codebook, jnp.zeros_like(tokens)))
    diff = tokens.astype(F32) - quantized.astype(F32)
    token_loss = jnp.sum(diff * diff, axis=1) / width

    def add(step, carry):
        c, t, total, hits, parts = carry
        owner = lax.rem(me - step + n, n)
        mine = (c // per_dev) == me
        total = total + jax.ops.segment_sum(
            jnp.where(mine, t, 0.0), c % per_dev, num_segments=per_dev
        )
        hits = hits + jax.ops.segment_sum(
            mine.astype(jnp.int32), c % per_dev, num_segments=per_dev
        )
        parts = lax.dynamic_update_slice(parts, jnp.sum(t)[None], (owner,))
        return lax.ppermute(c, AXES, ring), lax.ppermute(t, AXES, ring), total, hits, parts

    start = (
        codes, token_loss, jnp.zeros((per_dev,), F32),
        jnp.zeros((per_dev,), jnp.int32), jnp.zeros((n,), F32),
    )
    _, _, code_loss, counts, parts = lax.fori_loop(0, n, add, start)
    probs = counts.astype(F32) / (rows * n)
    floor_prob = jnp.float32(1.0 / (rows * n))
    terms = jnp.where(counts > 0, probs * jnp.log(jnp.maximum(probs, floor_prob)), 0.0)

    def collect(step, carry):
        entropy, parts = carry
        owner = lax.rem(me - step + n, n)
        parts = lax.dynamic_update_slice(parts, entropy, (owner,))
        return lax.ppermute(entropy, AXES, ring), parts

    _, entropies = lax.fori_loop(0, n, collect, (jnp.sum(terms)[None], jnp.zeros((n,), F32)))
    commitment = 0.25 * jnp.sum(parts) / (rows * n)
    return quantized, token_loss, counts, code_loss, commitment, jnp.exp(-jnp.sum(entropies))


def kernel(
    n, cols, cap, spill, wide_spill,
    codes_hbm, tokens_hbm, book_hbm,
    quant_ref, tloss_ref, counts_ref, closs_ref, scal_ref,
    codes_ref, tokens_ref, book_ref, csend, crecv, hsend, hrecv, psend, precv, gsend, grecv, osend, orecv,
    dsend, drecv, lsend, lrecv, low1h, sel, spill1h, rank1h, direct,
    in_sem, csem_s, csem_r, hsem_s, hsem_r, psem_s, psem_r,
    gsem_s, gsem_r, osem_s, osem_r, lsem_s, lsem_r, bsem, dsem,
):
    rows, width = tokens_hbm.shape
    per = book_hbm.shape[0]
    bits = per.bit_length() - 1
    total_tokens = rows * n
    chips, half = n // 2, cols // 2
    my_row, my_col = lax.axis_index("row"), lax.axis_index("col")
    core = lax.rem(my_col, 2)
    my_chip = lax.div(my_col, 2)
    me = my_row * half + my_chip
    inner = lax.rem(lax.div(my_row + 1, 2), 2)
    beside, across = my_row + 1 - 2 * lax.rem(my_row, 2), 3 - my_row
    skip, late = lax.rem(my_row + 2, 4), lax.div(my_row, 2)
    near = inner * across + (1 - inner) * beside
    far = inner * beside + (1 - inner) * across
    first = late * beside + (1 - late) * skip
    then = late * skip + (1 - late) * far
    last = late * across + (1 - late) * near
    rows_at = [my_row, last, first, then]
    chips_at = [
        my_chip, my_chip + 1 - 2 * lax.rem(my_chip, 2), lax.rem(my_chip + 2, 4), 3 - my_chip
    ]
    spots = [(rows_at[k // half], chips_at[k % half]) for k in range(chips)]
    at = [(r, 2 * c + core) for r, c in spots]
    mirror = [(r, 2 * c + 1 - core) for r, c in spots]
    peer = [r * half + c for r, c in spots]
    fetch_codes = pltpu.make_async_copy(codes_hbm, codes_ref, in_sem.at[0])
    own_book = book_ref.at[pl.ds(pl.multiple_of(core * per, per), per)]
    fetch_book = pltpu.make_async_copy(book_hbm, own_book, in_sem.at[1])
    fetch_tokens = pltpu.make_async_copy(tokens_hbm, tokens_ref, in_sem.at[2])
    fetch_codes.start()

    def remote(src, dst, ssem, rsem, to):
        return pltpu.make_async_remote_copy(
            src_ref=src,
            dst_ref=dst,
            send_sem=ssem,
            recv_sem=rsem,
            device_id=to,
            device_id_type=pl.DeviceIdType.MESH,
        )

    def put(send, recv, ssem, rsem, k):
        return remote(send.at[peer[k]], recv.at[me], ssem, rsem, at[k])

    def spill_put(d, c):
        r, to = rows_at[d], chips_at[c]
        return remote(gsend.at[r, to], grecv.at[r, my_chip], gsem_s, gsem_r.at[r], at[c])

    def joint_put(d):
        return remote(osend.at[rows_at[d]], orecv.at[my_row], osem_s, osem_r, at[d * half])

    def loss_put(k, other):
        to = mirror[k] if other else at[k]
        return remote(lsend.at[peer[k]], lrecv.at[other * chips + me], lsem_s, lsem_r, to)

    def all_in(ref, count, sem):
        part = ref.at[pl.ds(0, count)]
        remote(part, part, sem, sem, mirror[0]).wait_recv()

    def all_out(ref, count, sem):
        part = ref.at[pl.ds(0, count)]
        remote(part, part, sem, sem, mirror[0]).wait_send()

    ask_refs = (csend, crecv, csem_s, csem_r.at[my_row])
    count_refs = (hsend, hrecv, hsem_s, hsem_r)
    reply_refs = (psend, precv, psem_s, psem_r)
    partners = [k for d in ASK_ORDER for k in range(d * half, d * half + half) if k]
    everyone = [(k, other) for d in ASK_ORDER for k in range(d * half, d * half + half)
                for other in (0, 1) if k or other]
    share_book = remote(own_book, own_book, bsem.at[0], bsem.at[1], mirror[0])
    share_asks = remote(dsend, drecv, dsem.at[0], dsem.at[1], mirror[0])

    barrier = pltpu.get_barrier_semaphore()
    for k, other in everyone:
        pl.semaphore_signal(
            barrier, inc=1, device_id=mirror[k] if other else at[k],
            device_id_type=pl.DeviceIdType.MESH,
        )
    fetch_book.start()
    fetch_tokens.start()

    fetch_codes.wait()
    code_row = codes_ref[...].reshape(1, rows)
    hi_row = lax.shift_right_logical(code_row, bits)
    code_col = jnp.broadcast_to(code_row.astype(F32), (128, rows)).T.astype(jnp.int32)
    hi_col = lax.shift_right_logical(code_col, bits)
    lo_col = code_col & (per - 1)
    lane = lax.broadcasted_iota(jnp.int32, (rows, 128), 1)
    own_row = hi_row == lax.broadcasted_iota(jnp.int32, (n, rows), 0)
    for k in range(per // 128):
        low1h[:, k * 128 : (k + 1) * 128] = jnp.where(lo_col == lane + k * 128, 1.0, 0.0).astype(BF16)
    low = low1h[...]
    hist = jnp.dot(jnp.where(own_row, 1.0, 0.0).astype(BF16), low, preferred_element_type=F32)
    odd = (lax.broadcasted_iota(jnp.int32, (n, 128), 0) & 1) == 1

    def first_half(found):
        total = jnp.broadcast_to(jnp.sum(found, axis=1, keepdims=True), (n, 128))
        return total, jnp.where(odd, pltpu.roll(total, 1, 0), 0.0)

    wanted = jnp.where(hist > 0.5, 1.0, 0.0)
    total, ahead = first_half(wanted)
    both = total + ahead
    over = [jnp.where(odd, jnp.maximum(both - float(c), 0.0), 0.0) for c in (cap, 2 * cap)]
    over = jnp.minimum(jnp.concatenate(over, axis=1), 256.0).astype(BF16)
    line = lax.broadcasted_iota(jnp.int32, (2 * n, n), 0)
    source = lax.broadcasted_iota(jnp.int32, (2 * n, n), 1)
    line_of = lax.rem(line, n)
    same = lax.div(line_of, cols) == lax.div(source, cols)
    earlier = lax.div(source, 2) < lax.div(line_of, 2)
    reach = jnp.where(same & (earlier | (line >= n)), 1.0, 0.0).astype(BF16)
    over = jnp.dot(reach, over, preferred_element_type=F32)
    behind = over[:n, :1]
    worst = jnp.max(over[n:], axis=0, keepdims=True)
    heavy = jnp.max(jnp.max(hist, axis=0, keepdims=True), axis=1, keepdims=True) > 256.0
    most = jnp.where(worst[:, EXTRA:] > float(wide_spill), 2.0, 1.0)
    most = jnp.where(worst[:, :EXTRA] > float(spill), most, 0.0)
    most = jnp.where(heavy, 2.0, most)
    most_pair = jnp.broadcast_to(most, (2, EXTRA)).astype(BF16)
    before = lax.broadcasted_iota(jnp.int32, (per, per), 0) < lax.broadcasted_iota(jnp.int32, (per, per), 1)
    before = jnp.where(before, 1.0, 0.0).astype(BF16)
    rank = jnp.dot(wanted.astype(BF16), before, preferred_element_type=F32) + ahead[:, :1]
    rank = jnp.minimum(rank + jnp.where(rank > cap - 0.5, behind, 0.0), 255.0)
    order = jnp.where(wanted > 0.5, rank, -1.0).astype(BF16)
    for q in range(chips):
        csend[q] = order[2 * q : 2 * q + 2, :]
    crecv[pl.ds(me, 1)] = csend[pl.ds(me, 1)]

    pl.semaphore_wait(barrier, n - 1)
    for k in partners:
        put(*ask_refs, k).start()
    hist16 = jnp.minimum(hist, 256.0).astype(BF16)
    for q in range(chips):
        hsend[q, :, :per] = hist16[2 * q : 2 * q + 2, :]
        hsend[q, :, per:] = most_pair
    hrecv[pl.ds(me, 1)] = hsend[pl.ds(me, 1)]
    fetch_book.wait()
    share_book.start()
    for k in partners:
        put(*count_refs, k).start()

    rank = rank.astype(BF16)
    hi1h = jnp.where(hi_col[:, :n] == lane[:, :n], 1.0, 0.0).astype(BF16)
    looked = jnp.dot(hi1h, rank, preferred_element_type=F32).astype(BF16) * low
    found = jnp.dot(looked, jnp.ones((per, 128), BF16), preferred_element_type=F32)
    found = found.astype(jnp.int32)
    rank1h[...] = jnp.where(found == lane, 1.0, 0.0).astype(BF16)
    chip_col = lax.shift_right_logical(hi_col, 1)
    slot = jnp.where(found < cap, chip_col * cap + found, -1)
    for k in range(chips * cap // 128):
        sel[:, k * 128 : (k + 1) * 128] = jnp.where(slot == lane + k * 128, 1.0, 0.0).astype(BF16)
    slot = jnp.where(found < cap, -1, lax.div(chip_col, half) * spill + (found - cap))
    planes = chips // half
    for k in range(0, planes * spill, 128):
        wide = min(128, planes * spill - k)
        spill1h[:, k : k + wide] = jnp.where(slot == lane + k, 1.0, 0.0).astype(BF16)[:, :wide]

    both_caps = cap + -(-spill // 16) * 16
    place = lax.broadcasted_iota(jnp.int32, (both_caps, per), 0).astype(F32).astype(BF16)
    one, none = jnp.ones((), BF16), jnp.zeros((), BF16)
    for i, d in enumerate(REPLY_ORDER):
        group = range(d * half, d * half + half)
        all_in(crecv, half if d else half - 1, csem_r.at[rows_at[d]])
        if i == 0:
            share_book.wait_recv()
        step = half if i else 2
        for first in range(0, half, step):
            picks = []
            for k in group[first : first + step]:
                pair = crecv[peer[k]].astype(F32)
                picks.append(jnp.concatenate(
                    [
                        jnp.where(jnp.broadcast_to(pair[h : h + 1], (both_caps, per)).astype(BF16) == place, one, none)
                        for h in (0, 1)
                    ],
                    axis=1,
                ))
            packed = jnp.dot(jnp.concatenate(picks, axis=0), book_ref[...], preferred_element_type=F32)
            packed = packed.astype(BF16)
            for j, k in enumerate(group[first : first + step]):
                c = first + j
                out = psend if k else precv
                start = j * both_caps
                out[peer[k]] = packed[start : start + cap]
                if c:
                    gsend[rows_at[d], chips_at[c]] = packed[start + cap : start + cap + spill]
                    spill_put(d, c).start()
                else:
                    grecv[rows_at[d], my_chip] = packed[start + cap : start + cap + spill]
            for k in group[first : first + step]:
                if k:
                    put(*reply_refs, k).start()

    for d in REPLY_ORDER:
        all_in(grecv.at[0], half - 1, gsem_r.at[rows_at[d]])
        joint = grecv[rows_at[d], 0].astype(F32)
        for c in range(1, half):
            joint = joint + grecv[rows_at[d], c].astype(F32)
        if d:
            osend[rows_at[d]] = joint.astype(BF16)
            joint_put(d).start()
        else:
            orecv[my_row] = joint.astype(BF16)

    all_in(hrecv, chips - 1, hsem_r)
    got = jnp.concatenate([crecv[q].astype(F32) for q in range(chips)], axis=0)
    asked = jnp.concatenate([hrecv[q].astype(F32) for q in range(chips)], axis=0)
    turn = lax.broadcasted_iota(jnp.int32, (n, n), 0)
    side = jnp.where(turn < chips, core, 1 - core)
    which = 2 * lax.rem(turn, chips) + side
    split = jnp.where(lax.broadcasted_iota(jnp.int32, (n, n), 1) == which, 1.0, 0.0).astype(BF16)
    both = jnp.concatenate([got.astype(BF16), asked[:, :per].astype(BF16)], axis=1)
    both = jnp.dot(split, both, preferred_element_type=F32)
    most_asked = jnp.max(asked[:, per:], axis=0, keepdims=True)
    dsend[:, : 2 * per] = both[chips:]
    dsend[:, 2 * per :] = jnp.broadcast_to(most_asked, (chips, EXTRA))
    share_asks.start()
    share_asks.wait_recv()
    counts = jnp.sum(both[:chips, per:] + drecv[:, per : 2 * per], axis=0, keepdims=True)
    counts_ref[...] = counts.astype(jnp.int32)
    probs = counts / total_tokens
    terms = jnp.where(
        counts > 0.5, probs * jnp.log(jnp.maximum(probs, 1.0 / total_tokens)), 0.0
    )
    entropy = jnp.sum(terms, axis=1, keepdims=True)
    flag = jnp.maximum(most_asked, drecv[:1, 2 * per :])
    spots_of = [both[:chips, :per].astype(jnp.int32), drecv[:, :per].astype(jnp.int32)]

    all_in(precv, chips - 1, psem_r)
    fetch_tokens.wait()
    packs = precv[...].reshape(chips * cap, width)
    direct[...] = jnp.dot(sel[...], packs, preferred_element_type=F32)
    all_in(orecv, planes - 1, osem_r)
    packs = orecv[...].reshape(planes * spill, width)
    quant = (direct[...] + jnp.dot(spill1h[...], packs, preferred_element_type=F32)).astype(BF16)
    quant_ref[...] = quant
    diff = tokens_ref[...].astype(F32) - quant.astype(F32)
    square = diff * diff
    folded = square[:, :128]
    for k in range(1, width // 128):
        folded = folded + square[:, k * 128 : (k + 1) * 128]
    tloss = jnp.sum(folded.T, axis=0, keepdims=True) / width
    tloss_ref[...] = tloss
    part = jnp.sum(tloss, axis=1, keepdims=True)

    first = tloss.astype(BF16).astype(F32)
    second = (tloss - first).astype(BF16).astype(F32)
    third = tloss - first - second
    own_chip = lax.shift_right_logical(hi_row, 1) == lax.broadcasted_iota(jnp.int32, (chips, rows), 0)
    spread = jnp.concatenate(
        [jnp.where(own_chip, x, 0.0).astype(BF16) for x in (first, second, third)], axis=0
    )
    sums = jnp.dot(spread, rank1h[...], preferred_element_type=F32)
    sums = sums[:chips] + sums[chips : 2 * chips] + sums[2 * chips :]
    lane1 = lax.broadcasted_iota(jnp.int32, (chips, EXTRA), 1)
    sums = jnp.where(lane1 == EXTRA - 2, part, jnp.where(lane1 == EXTRA - 1, entropy, sums))
    for q in range(chips):
        lsend[q] = sums[q : q + 1, :]
    lrecv[pl.ds(me, 1)] = lsend[pl.ds(me, 1)]
    for k, other in everyone:
        loss_put(k, other).start()

    all_out(csend, chips - 1, csem_s)
    all_out(hsend, chips - 1, hsem_s)
    all_out(psend, chips - 1, psem_s)
    all_out(gsend, planes - 1, gsem_s)
    all_out(osend, planes - 1, osem_s)
    share_book.wait_send()
    share_asks.wait_send()
    all_in(lrecv, n - 1, lsem_r)
    added = jnp.zeros((chips, per), F32)
    ends = jnp.zeros((1, EXTRA), F32)
    for other in (0, 1):
        back = lrecv[other * chips : (other + 1) * chips, 0, :]
        spot = spots_of[other]
        parts = [
            jnp.take_along_axis(back, jnp.maximum(spot[:, j : j + 128], 0), axis=1)
            for j in range(0, per, 128)
        ]
        added = added + jnp.where(spot >= 0, jnp.concatenate(parts, axis=1), 0.0)
        ends = ends + jnp.sum(back, axis=0, keepdims=True)
    closs_ref[...] = jnp.sum(added, axis=0, keepdims=True)
    lane1 = lane1[:1]
    perp = jnp.exp(-ends[:, EXTRA - 1 :])
    commit = ends[:, EXTRA - 2 : EXTRA - 1] * (0.25 / total_tokens)
    scal_ref[...] = jnp.where(lane1 == 0, commit, jnp.where(lane1 == 1, perp, flag))
    all_out(lrecv, n - 1, lsem_s)


def exchange(n, cols, cap, spill, wide_spill, number, tokens, codebook, codes):
    rows, width = tokens.shape
    per = codebook.shape[0]
    chips, planes = n // 2, n // cols
    vmem = pl.BlockSpec(memory_space=pltpu.VMEM)
    dma = pltpu.SemaphoreType.DMA
    return pl.pallas_call(
        functools.partial(kernel, n, cols, cap, spill, wide_spill),
        out_shape=(
            pltpu.VMEM((rows, width), BF16),
            pltpu.VMEM((1, rows), F32),
            pltpu.VMEM((1, per), jnp.int32),
            pltpu.VMEM((1, per), F32),
            pltpu.VMEM((1, EXTRA), F32),
        ),
        in_specs=[pl.BlockSpec(memory_space=pltpu.HBM)] * 3,
        out_specs=(vmem,) * 5,
        scratch_shapes=[
            pltpu.VMEM(codes.shape, jnp.int32),
            pltpu.VMEM((rows, width), BF16),
            pltpu.VMEM((2 * per, width), BF16),
            pltpu.VMEM((chips, 2, per), BF16),
            pltpu.VMEM((chips, 2, per), BF16),
            pltpu.VMEM((chips, 2, per + EXTRA), BF16),
            pltpu.VMEM((chips, 2, per + EXTRA), BF16),
            pltpu.VMEM((chips, cap, width), BF16),
            pltpu.VMEM((chips, cap, width), BF16),
            pltpu.VMEM((planes, cols // 2, spill, width), BF16),
            pltpu.VMEM((planes, cols // 2, spill, width), BF16),
            pltpu.VMEM((planes, spill, width), BF16),
            pltpu.VMEM((planes, spill, width), BF16),
            pltpu.VMEM((chips, 2 * per + EXTRA), F32),
            pltpu.VMEM((chips, 2 * per + EXTRA), F32),
            pltpu.VMEM((chips, 1, EXTRA), F32),
            pltpu.VMEM((n, 1, EXTRA), F32),
            pltpu.VMEM((rows, per), BF16),
            pltpu.VMEM((rows, chips * cap), BF16),
            pltpu.VMEM((rows, planes * spill), BF16),
            pltpu.VMEM((rows, 128), BF16),
            pltpu.VMEM((rows, width), F32),
            dma((3,)),
            dma, dma((planes,)), *[dma] * 4,
            dma, dma((planes,)), *[dma] * 4,
            dma((2,)), dma((2,)),
        ],
        compiler_params=pltpu.CompilerParams(collective_id=number, has_side_effects=True),
    )(*[pltpu.with_memory_space_constraint(x, pltpu.HBM) for x in (codes, tokens, codebook)])


def finish_kernel(
    quant_ref, tloss_ref, counts_ref, closs_ref, scal_ref,
    quant_out, tloss_out, counts_out, closs_out, commit_out, perp_out, flag_out,
    tloss, counts, closs, commit, perp, sem,
):
    whole = pltpu.make_async_copy(quant_ref, quant_out, sem.at[0])
    whole.start()
    tloss[...] = tloss_ref[...].reshape(tloss.shape)
    counts[...] = counts_ref[...].reshape(counts.shape)
    closs[...] = closs_ref[...].reshape(closs.shape)
    commit[...] = scal_ref[:, :1]
    perp[...] = scal_ref[:, 1:2]
    small = [(tloss, tloss_out), (counts, counts_out), (closs, closs_out), (commit, commit_out), (perp, perp_out)]
    small = [pltpu.make_async_copy(src, dst, sem.at[1 + i]) for i, (src, dst) in enumerate(small)]
    for one in small:
        one.start()
    flag_out[0, 0] = jnp.max(scal_ref[:, 2:3]).astype(jnp.int32)
    for one in small:
        one.wait()
    whole.wait()


def finish(quantized, token_loss, counts, code_loss, scalars):
    rows, per = token_loss.shape[1], counts.shape[1]
    vmem = pl.BlockSpec(memory_space=pltpu.VMEM)
    hbm = pl.BlockSpec(memory_space=pltpu.HBM)
    q, t, k, c, m, p, f = pl.pallas_call(
        finish_kernel,
        out_shape=(
            jax.ShapeDtypeStruct(quantized.shape, BF16),
            jax.ShapeDtypeStruct((rows,), F32),
            jax.ShapeDtypeStruct((per,), jnp.int32),
            jax.ShapeDtypeStruct((per,), F32),
            jax.ShapeDtypeStruct((1, 1), F32),
            jax.ShapeDtypeStruct((1, 1), F32),
            pltpu.SMEM((1, 1), jnp.int32),
        ),
        in_specs=[vmem] * 5,
        out_specs=(hbm,) * 6 + (pl.BlockSpec(memory_space=pltpu.SMEM),),
        scratch_shapes=[
            pltpu.VMEM((rows,), F32),
            pltpu.VMEM((per,), jnp.int32),
            pltpu.VMEM((per,), F32),
            pltpu.VMEM((1, 1), F32),
            pltpu.VMEM((1, 1), F32),
            pltpu.SemaphoreType.DMA((6,)),
        ],
        compiler_params=pltpu.CompilerParams(vmem_limit_bytes=4 << 20),
    )(quantized, token_loss, counts, code_loss, scalars)
    return q, t, k, c, m[0, 0], p[0, 0], f


def held(x):
    def body(src, dst, sem):
        copy = pltpu.make_async_copy(src, dst, sem)
        copy.start()
        copy.wait()

    return pl.pallas_call(
        body,
        out_shape=jax.ShapeDtypeStruct(x.shape, x.dtype),
        in_specs=[pl.BlockSpec(memory_space=pltpu.HBM)],
        out_specs=pl.BlockSpec(memory_space=pltpu.VMEM),
        scratch_shapes=[pltpu.SemaphoreType.DMA],
    )(pltpu.with_memory_space_constraint(x, pltpu.HBM))


def asked_plan(n, cols, cap, spill, tokens, codebook, codes):
    wide = spill * 2
    outs = exchange(n, cols, cap, spill, wide, 0, tokens, codebook, codes)

    *done, flag = finish(*outs)

    def kept():
        return tuple(done)

    def wider():
        return finish(*exchange(n, cols, 2 * cap, wide, wide, 1, tokens, codebook, codes))[:-1]

    def ringed():
        return ring_plan(n, held(tokens), held(codebook), held(codes))

    def any_codes():
        return lax.cond(flag[0, 0] > 1, ringed, wider)

    return lax.cond(flag[0, 0] > 0, any_codes, kept)


def on_device(n, cols, tokens, codebook, codes):
    rows, width = tokens.shape
    per = codebook.shape[0]
    cap = -(-rows // (n * 16)) * 16
    spill = cap * 3 // 4
    fits = (
        per % 128 == 0
        and per & (per - 1) == 0
        and rows % 128 == 0
        and width % 128 == 0
        and n // 2 * cap % 128 == 0
        and spill % 8 == 0
        and cols == 8
        and n == 4 * cols
        and n <= 128
        and 2 * cap + 2 * spill < EXTRA - 1
    )
    if fits:
        return asked_plan(n, cols, cap, spill, tokens, codebook, codes)
    return dense_plan(tokens, codebook, codes)


def solution(mesh):
    n = mesh.shape["row"] * mesh.shape["col"]
    return jax.shard_map(
        functools.partial(on_device, n, mesh.shape["col"]),
        mesh=mesh,
        in_specs=(P(AXES, None), P(AXES, None), P(AXES)),
        out_specs=(P(AXES, None), P(AXES), P(AXES), P(AXES), P(), P()),
        check_vma=False,
    )
```
